32 devices in a mesh: row: 8 (over z, y), col: 4 (over x, core).
Axes of the slice: x: 2, y: 2, z: 4, core: 2. Of those that a mesh axis runs over, the one named last changes fastest.
Arguments:
- inputs: bfloat16 [4, 12288, 227], P(None, ('row', 'col')), may hold values from -6 to 6
- targets: bfloat16 [4, 12288, 83], P(None, ('row', 'col')), may hold values from -6 to 6
- cell_area: float32 [12288], P(('row', 'col')), may hold values from 0.1 to 1
- cell_count: int32 [32], P(('row', 'col')), may hold values from 128 to 384, as said below
- cell_node: int32 [12288], P(('row', 'col')), may hold values from 0 to 63
- edge_senders: int32 [32768], P(('row', 'col')), may hold values from 0 to 511
- edge_receivers: int32 [32768], P(('row', 'col')), may hold values from 0 to 255
- weight_input: float32 [227, 512], P(None, 'col'), may hold values from -0.375 to 0.375
- weight_latent: float32 [6, 512, 512], P(None, 'col'), may hold values from -0.25 to 0.25
- weight_output: float32 [512, 83], P('col'), may hold values from -0.25 to 0.25
- mean_input: float32 [227, 512], P(None, 'col'), may hold values from -0.00024414062 to 0.00024414062
- mean_latent: float32 [6, 512, 512], P(None, 'col'), may hold values from -0.00024414062 to 0.00024414062
- mean_output: float32 [512, 83], P('col'), may hold values from -0.00024414062 to 0.00024414062
- square_input: float32 [227, 512], P(None, 'col'), as said below
- square_latent: float32 [6, 512, 512], P(None, 'col'), as said below
- square_output: float32 [512, 83], P('col'), as said below
Outputs:
- loss_value: float32 [], replicated
- gradient_input: float32 [227, 512], P(None, 'col')
- gradient_latent: float32 [6, 512, 512], P(None, 'col')
- gradient_output: float32 [512, 83], P('col')
- first_input: float32 [227, 512], P(None, 'col')
- first_latent: float32 [6, 512, 512], P(None, 'col')
- first_output: float32 [512, 83], P('col')
- second_input: float32 [227, 512], P(None, 'col')
- second_latent: float32 [6, 512, 512], P(None, 'col')
- second_output: float32 [512, 83], P('col')
- master_input: float32 [227, 512], P(None, 'col')
- master_latent: float32 [6, 512, 512], P(None, 'col')
- master_output: float32 [512, 83], P('col')
- copy_input: bfloat16 [227, 512], P(None, 'col')
- copy_latent: bfloat16 [6, 512, 512], P(None, 'col')
- copy_output: bfloat16 [512, 83], P('col')
- trust_norms: float32 [2, 8], replicated
The draws below stay inside these ranges and needn't reach their ends.
Inputs may be any that keep to these rules, and one draw needn't show every extreme that they name: `cell_count`: used cell slots of a device; some device uses all 384. `cell_node`: A node of the cell's own device. `edge_senders`: index into the block's column of nodes. `edge_receivers`: index into the block's row of nodes. `square_input`: Positive. `square_latent`: Positive. `square_output`: Positive.
All inputs are finite; a program needn't handle non-finite values.
Results may differ from the reference program's by a relative error of at most 0.0035.
The reference program's roundings to bfloat16 on the way count: a program that leaves them out, or rounds other values in their place, can miss the bound.
Values may be sent and summed in bfloat16 or wider, within the bound.
A program may use at most 192 MiB of HBM per device.

```python
import math
import jax
import jax.numpy as jnp
from jax import lax

D = 512
C_IN = 227
C_OUT = 83
DEG = 16
SAMPLES = 4
CAP = 384
MESH_DEV = 64
E_DEV = 1024
CELLS = 12288
MESH = 2048
EDGES = 32768
N_ROW = 8
N_COL = 4


def draw_cell_count(key, part):
    device_total = N_ROW * N_COL
    first_key, second_key = jax.random.split(key)
    counts = jax.random.randint(first_key, (device_total,), CAP // 3, CAP + 1, dtype=jnp.int32)
    chosen = jax.random.randint(second_key, (), 0, device_total, dtype=jnp.int32)
    return jnp.where(jnp.arange(device_total, dtype=jnp.int32) == chosen, CAP, counts).astype(jnp.int32)


def second_moment(key, shape):
    base = 0.0001 / (SAMPLES * CAP * N_ROW * N_COL)
    factor = jax.random.uniform(key, shape, jnp.float32, 0.25, 4.0)
    return (base * factor).astype(jnp.float32)


def draw_square_input(key, part):
    return second_moment(jax.random.fold_in(key, 11), (C_IN, D))


def draw_square_latent(key, part):
    return second_moment(jax.random.fold_in(key, 12), (6, D, D))


def draw_square_output(key, part):
    return second_moment(jax.random.fold_in(key, 13), (D, C_OUT))


def plant(drawn, rng, low, top_value):
    dims = drawn.shape
    index_at = [jax.random.randint(jax.random.fold_in(rng, axis), (), 0, dims[axis]) for axis in range(len(dims))]
    drawn = drawn.at[tuple(index_at)].set(low)
    longest = dims.index(max(dims))
    index_at[longest] = (index_at[longest] + 1) % dims[longest]
    return drawn.at[tuple(index_at)].set(top_value)


def shard_levels(rng, dims, shards, smallest, top_value):
    factor_of = 1.0
    for position, shards_of in shards:
        steps = jax.random.uniform(jax.random.fold_in(jax.random.fold_in(rng, 6), position), (shards_of,), jnp.float32, smallest / len(shards), top_value / len(shards))
        factor_of = factor_of * jnp.repeat(jnp.exp(steps), dims[position] // shards_of).reshape((-1,) + (1,) * (len(dims) - 1 - position))
    return factor_of


def centred(key, shape, deviation, limit, cuts=(), kind=jnp.bfloat16):
    values = jax.random.normal(key, shape, jnp.float32) * deviation
    if len(cuts) > 0:
        values = shard_levels(key, shape, cuts, -0.22, 0.18) * values
    return jnp.clip(values, min=-limit, max=limit).astype(kind)


def setup_inputs(seed: int = 0) -> dict:
    key_of = jax.random.split(jax.random.key(seed), 17)
    return {
        "inputs": centred(key_of[0], (SAMPLES, CELLS, C_IN), 1.0, 6.0, ((1, 32),)),
        "targets": centred(key_of[1], (SAMPLES, CELLS, C_OUT), 1.0, 6.0, ((1, 32),)),
        "cell_area": jnp.clip(jnp.exp(math.log(1.0) - 2.3025851 * jax.random.uniform(key_of[2], (CELLS,), jnp.float32) ** shard_levels(key_of[2], (CELLS,), ((0, 32),), -0.2, 0.2)), 0.1, 1.0),
        "cell_count": draw_cell_count(jax.random.fold_in(key_of[16], 71), 0),
        "cell_node": plant(jax.random.randint(key_of[4], (CELLS,), 0, MESH_DEV), jax.random.fold_in(key_of[4], 1), 0, MESH_DEV - 1).astype(jnp.int32),
        "edge_senders": plant(jax.random.randint(key_of[5], (EDGES,), 0, N_ROW * MESH_DEV), jax.random.fold_in(key_of[5], 1), 0, (N_ROW * MESH_DEV) - 1).astype(jnp.int32),
        "edge_receivers": plant(jax.random.randint(key_of[6], (EDGES,), 0, N_COL * MESH_DEV), jax.random.fold_in(key_of[6], 1), 0, (N_COL * MESH_DEV) - 1).astype(jnp.int32),
        "weight_input": centred(key_of[7], (C_IN, D), C_IN ** -0.5, 0.375, ((1, 4),), jnp.float32),
        "weight_latent": centred(key_of[8], (6, D, D), D ** -0.5, 0.25, ((1, 4),), jnp.float32),
        "weight_output": centred(key_of[9], (D, C_OUT), D ** -0.5, 0.25, ((0, 4),), jnp.float32),
        "mean_input": centred(key_of[10], (C_IN, D), (10000 * SAMPLES * CAP * N_ROW * N_COL) ** -0.5, 0.00024414062, ((1, 4),), jnp.float32),
        "mean_latent": centred(key_of[11], (6, D, D), (10000 * SAMPLES * CAP * N_ROW * N_COL) ** -0.5, 0.00024414062, ((1, 4),), jnp.float32),
        "mean_output": centred(key_of[12], (D, C_OUT), (10000 * SAMPLES * CAP * N_ROW * N_COL) ** -0.5, 0.00024414062, ((0, 4),), jnp.float32),
        "square_input": draw_square_input(jax.random.fold_in(key_of[16], 71), 0),
        "square_latent": draw_square_latent(jax.random.fold_in(key_of[16], 71), 0),
        "square_output": draw_square_output(jax.random.fold_in(key_of[16], 71), 0),
    }


@jax.custom_vjp
def reduced_precision(v):
    return lax.optimization_barrier(v.astype(jnp.bfloat16)).astype(jnp.float32)

@jax.custom_vjp
def reduced_backward(v):
    return v

def low_keep(v):
    return (reduced_precision(v), None)

def low_pass(kept, grad):
    return (grad,)

def back_keep(v):
    return (v, None)

def back_low(kept, grad):
    return (reduced_precision(grad),)
reduced_precision.defvjp(low_keep, low_pass)
reduced_backward.defvjp(back_keep, back_low)
highest = lax.Precision.HIGHEST
beta_first = 0.5
beta_second = 0.5
adam_epsilon = 1e-08
trust_epsilon = 1e-06
weight_decay = 0.01
learn_rate = 0.1

def einsum_result(form, left, right):
    return jnp.einsum(form, left, right, precision=highest)

def segment_rows(values, segment_ids, count):
    return jax.vmap(lambda rows: jax.ops.segment_sum(rows, segment_ids, num_segments=count))(values)

def forward(weight_input, weight_latent, weight_output, inputs, targets, cell_weight, valid, node_global, sender_global, receiver_global):
    first_pre = reduced_backward(einsum_result('sci,id->scd', inputs, reduced_precision(weight_input)))
    grid_latent = reduced_precision(jax.nn.silu(first_pre))
    node_sum = segment_rows(grid_latent * valid[None, :, None], node_global, MESH)
    node_count = jax.ops.segment_sum(valid, node_global, num_segments=MESH)
    node_average = node_sum / jnp.maximum(node_count, 1.0)[None, :, None]
    latent_reduced = reduced_precision(weight_latent)
    second_activation_input = reduced_backward(einsum_result('kaj,jz->kaz', reduced_precision(node_average), latent_reduced[0]))
    mesh_latent = jax.nn.silu(second_activation_input)
    mesh_state_reduced = reduced_precision(mesh_latent)
    sender_projected = reduced_backward(einsum_result('kaj,jz->kaz', mesh_state_reduced, latent_reduced[1]))
    receiver_projected = reduced_backward(einsum_result('kaj,jz->kaz', mesh_state_reduced, latent_reduced[2]))
    edge_pre = sender_projected[:, sender_global] + receiver_projected[:, receiver_global]
    summed = segment_rows(jax.nn.silu(edge_pre), receiver_global, MESH)
    message_total = reduced_backward(summed / DEG)
    residual_branch = reduced_backward(einsum_result('kaj,jz->kaz', reduced_precision(message_total), latent_reduced[3]))
    mesh_next = mesh_latent + residual_branch
    decode_rows = reduced_precision(mesh_next)[:, node_global]
    third_pre = reduced_backward(einsum_result('scd,de->sce', decode_rows, latent_reduced[4]) + einsum_result('scd,de->sce', grid_latent, latent_reduced[5]))
    grid_out = reduced_precision(jax.nn.silu(third_pre))
    predict = reduced_backward(einsum_result('scd,do->sco', grid_out, reduced_precision(weight_output)))
    error = predict - targets
    return jnp.sum(cell_weight[None, :, None] * error * error) / (C_OUT * SAMPLES * jnp.sum(cell_weight))

def adam_parts(weight, gradient, first, second):
    new_first = beta_first * first + (1.0 - beta_first) * gradient
    new_second = beta_second * second + (1.0 - beta_second) * gradient * gradient
    update = new_first / (jnp.sqrt(new_second) + adam_epsilon) + weight_decay * weight
    return (new_first, new_second, update)

def reference(inputs, targets, cell_area, cell_count, cell_node, edge_senders, edge_receivers, weight_input, weight_latent, weight_output, mean_input, mean_latent, mean_output, square_input, square_latent, square_output):
    devices = N_ROW * N_COL
    slots = jnp.arange(CAP, dtype=jnp.int32)
    valid = (slots[None, :] < cell_count[:, None]).reshape(-1).astype(jnp.float32)
    cell_weight = cell_area * valid
    cell_device = jnp.arange(CAP * devices, dtype=jnp.int32) // CAP
    node_global = (cell_device * MESH_DEV + cell_node).astype(jnp.int32)
    edge_device = jnp.arange(E_DEV * devices, dtype=jnp.int32) // E_DEV
    edge_row = edge_device // N_COL
    edge_col = edge_device % N_COL
    sender_global = ((edge_senders // MESH_DEV * N_COL + edge_col) * MESH_DEV + edge_senders % MESH_DEV).astype(jnp.int32)
    receiver_global = (edge_row * (N_COL * MESH_DEV) + edge_receivers).astype(jnp.int32)
    inputs_wide = inputs.astype(jnp.float32)
    targets_wide = targets.astype(jnp.float32)

    def loss_of(first_weight, middle_weight, last_weight):
        return forward(first_weight, middle_weight, last_weight, inputs_wide, targets_wide, cell_weight, valid, node_global, sender_global, receiver_global)
    loss_value, pullback = jax.vjp(loss_of, weight_input, weight_latent, weight_output)
    gradient_input, gradient_latent, gradient_output = pullback(jnp.ones((), jnp.float32))
    first_input, second_input, update_input = adam_parts(weight_input, gradient_input, mean_input, square_input)
    first_latent, second_latent, update_latent = adam_parts(weight_latent, gradient_latent, mean_latent, square_latent)
    first_output, second_output, update_output = adam_parts(weight_output, gradient_output, mean_output, square_output)
    weight_sums = jnp.concatenate([jnp.sum(weight_input * weight_input)[None], lax.optimization_barrier(jnp.sum(weight_latent * weight_latent, axis=(1, 2))), jnp.sum(weight_output * weight_output)[None]])
    update_sums = jnp.concatenate([jnp.sum(update_input * update_input)[None], lax.optimization_barrier(jnp.sum(update_latent * update_latent, axis=(1, 2))), jnp.sum(update_output * update_output)[None]])
    trust_norms = jnp.sqrt(jnp.stack([weight_sums, update_sums]))
    ratio = trust_norms[0] / (trust_norms[1] + trust_epsilon)
    master_input = weight_input - learn_rate * ratio[0] * update_input
    master_latent = weight_latent - learn_rate * ratio[1:7][:, None, None] * update_latent
    master_output = weight_output - learn_rate * ratio[7] * update_output
    return (loss_value, gradient_input, gradient_latent, gradient_output, first_input, first_latent, first_output, second_input, second_latent, second_output, master_input, master_latent, master_output, master_input.astype(jnp.bfloat16), master_latent.astype(jnp.bfloat16), master_output.astype(jnp.bfloat16), trust_norms)
```

```python
import functools
import types

import jax
import jax.numpy as jnp
from jax import lax
from jax.experimental import pallas as pl
from jax.experimental.pallas import tpu as pltpu
from jax.sharding import PartitionSpec as P

C_OUT = 83
DEG = 16
MESH_DEV = 64


highest = lax.Precision.HIGHEST
beta_first = 0.5
beta_second = 0.5
adam_epsilon = 1e-08
trust_epsilon = 1e-06
weight_decay = 0.01
learn_rate = 0.1


def silu_grad(pre_act, grad_out):
    sigma = jax.nn.sigmoid(pre_act)
    return grad_out * sigma * (1.0 + pre_act * (1.0 - sigma))


def reduced_matmul(form, left, right):
    return jnp.einsum(form, left, right, preferred_element_type=jnp.float32)


def split_parts(values):
    upper = values.astype(jnp.bfloat16)
    rest = values - upper.astype(jnp.float32)
    middle = rest.astype(jnp.bfloat16)
    lower = (rest - middle.astype(jnp.float32)).astype(jnp.bfloat16)
    return (upper, middle, lower)


def pick_rows(match, values):
    upper, middle, lower = split_parts(values)
    total = reduced_matmul("es,ksd->ked", match, upper)
    total = total + reduced_matmul("es,ksd->ked", match, middle)
    return total + reduced_matmul("es,ksd->ked", match, lower)


def add_into_rows(match, values):
    upper, middle, lower = split_parts(values)
    total = reduced_matmul("es,ked->ksd", match, upper)
    total = total + reduced_matmul("es,ked->ksd", match, middle)
    return total + reduced_matmul("es,ked->ksd", match, lower)


def one_hot_table(indices, count):
    return (indices[:, None] == jnp.arange(count, dtype=jnp.int32)[None, :]).astype(jnp.bfloat16)


def adam_parts(weight, gradient, first, second):
    new_first = beta_first * first + (1.0 - beta_first) * gradient
    new_second = beta_second * second + (1.0 - beta_second) * gradient * gradient
    update = new_first / (jnp.sqrt(new_second) + adam_epsilon) + weight_decay * weight
    return (new_first, new_second, update)


MESH = pl.DeviceIdType.MESH
bf16 = jnp.bfloat16
f32 = jnp.float32
VMEM_ROOM = 63 * 2**20
N_IN = 256
N_OUT = 128
WIRE = ("in", 0, 1, 2, 5, 3, 4, "out")


def sizes_of(n_row, n_col):
    X = n_col // 2
    Y = X if n_row % X == 0 else 1
    return X, Y, n_row // Y


class Place:
    def __init__(self, n_row, n_col):
        self.K = 2
        self.X, self.Y, self.Z = sizes_of(n_row, n_col)
        self.row, self.col = lax.axis_index("row"), lax.axis_index("col")
        self.z, self.y = self.row // self.Y, self.row % self.Y
        self.x, self.k = self.col // 2, self.col % 2

    def to(self, axis, d):
        n = getattr(self, axis.upper())
        return (getattr(self, axis) + d) % n

    def peer(self, axis, d):
        at = {a: getattr(self, a) for a in "zyxk"}
        at[axis] = self.to(axis, d)
        return (at["z"] * self.Y + at["y"], at["x"] * 2 + at["k"])

    def barrier(self):
        sem = pltpu.get_barrier_semaphore()
        peers = [self.peer(a, d) for a in "kxyz" for d in range(1, getattr(self, a.upper()))]
        for peer in peers:
            pl.semaphore_signal(sem, inc=1, device_id=peer, device_id_type=MESH)
        pl.semaphore_wait(sem, len(peers))


def remote(src, dst, send_sem, recv_sem, device):
    return pltpu.make_async_remote_copy(
        src_ref=src,
        dst_ref=dst,
        send_sem=send_sem,
        recv_sem=recv_sem,
        device_id=device,
        device_id_type=MESH,
    )


def ds(start, size):
    if isinstance(start, int):
        return pl.ds(start, size)
    return pl.ds(pl.multiple_of(start, size if size % 128 else 128), size)


def by_rows(count, step, todo):
    def one(i, carry):
        todo(pl.multiple_of(i * step, step))
        return carry

    lax.fori_loop(0, count // step, one, 0)


def mm(a, b):
    return jnp.dot(a, b, preferred_element_type=f32)


def mm_nt(a, b):
    return lax.dot_general(a, b, (((1,), (1,)), ((), ())), preferred_element_type=f32)


def mm_tn(a, b):
    return lax.dot_general(a, b, (((0,), (0,)), ((), ())), preferred_element_type=f32)


def sigmoid(v):
    return 0.5 * jnp.tanh(0.5 * v) + 0.5


def silu(v):
    return v * sigmoid(v)


def silu_slope(v):
    s = sigmoid(v)
    return s * (1.0 + v * (1.0 - s))


def high_low(v):
    high = v.astype(bf16)
    return high, (v - high.astype(f32)).astype(bf16)


class Total:
    AXES = "kxyz"

    @staticmethod
    def scratch(X, Y, Z):
        many = 1 + X - 1 + Y - 1 + Z - 1
        return [pltpu.VMEM((n, 8, 128), f32) for n in (2, X, Y, Z)] + [
            pltpu.VMEM((8, 128), f32),
            pltpu.SemaphoreType.DMA((many,)),
            pltpu.SemaphoreType.DMA((many,)),
        ]

    def __init__(self, place, refs):
        self.p, self.bufs, (self.value, self.ss, self.rs) = place, dict(zip("kxyz", refs[:4])), refs[4:]

    def _copies(self, axis):
        p, buf = self.p, self.bufs[axis]
        base = sum(getattr(p, a.upper()) - 1 for a in self.AXES[: self.AXES.index(axis)])
        here = buf.at[getattr(p, axis)]
        for d in range(1, getattr(p, axis.upper())):
            i = base + d - 1
            yield remote(here, here, self.ss.at[i], self.rs.at[i], p.peer(axis, d))

    def start(self, axis):
        self.bufs[axis][getattr(self.p, axis)] = self.value[...]
        for copy in self._copies(axis):
            copy.start()

    def finish(self, axis):
        for copy in self._copies(axis):
            copy.wait_recv()
        buf = self.bufs[axis]
        value = buf[0]
        for i in range(1, getattr(self.p, axis.upper())):
            value = value + buf[i]
        self.value[...] = value

    def drain(self):
        for axis in self.AXES:
            for copy in self._copies(axis):
                copy.wait_send()


class Reduce:
    def __init__(self, grid, dim, n_col, width, late):
        self.X, self.Y, self.Z = grid
        self.dim, self.shard, self.late = dim, dim // n_col, late
        self.ry = self.shard // self.Y
        self.zr = min(self.ry // 16, self.Z)
        self.zl = self.Z // self.zr
        self.rz = self.ry // self.zr
        self.w = -(-width // (128 * self.zl)) * 128 * self.zl
        self.wz = self.w // self.zl

    def scratch(self):
        X, Y, Z, w = self.X, self.Y, self.Z, self.w
        many = X + (X - 1) + 2 * (Y - 1) + 2 * (Z - 1)
        return [
            pltpu.VMEM((self.dim, w), f32),
            pltpu.VMEM((X, self.shard, w), f32),
            pltpu.VMEM((X - 1, self.shard, w), bf16),
            pltpu.VMEM((X - 1, self.shard, w), bf16),
            pltpu.VMEM((Y - 1, self.ry, w), bf16),
            pltpu.VMEM((Y - 1, self.ry, w), bf16),
            pltpu.VMEM((Z - 1, self.rz, self.wz), self.late),
            pltpu.VMEM((Z - 1, self.rz, self.wz), self.late),
            pltpu.VMEM((self.rz, self.wz), f32),
            pltpu.VMEM((self.shard, w), self.late),
            pltpu.SemaphoreType.DMA((many,)),
            pltpu.SemaphoreType.DMA((many,)),
        ]

    def bind(self, place, refs):
        (self.full, self.cr, self.xs, self.xr, self.ys, self.yr, self.zs, self.zin, self.piece, self.out, self.ss, self.rs) = refs
        self.p = place
        self.copies = []

    def rows_of(self, x, k):
        return (2 * x + k) * self.shard

    def piece_at(self, z):
        rows = pl.multiple_of((z // self.zl) * self.rz, 16)
        if self.zl == 1:
            return rows, pl.ds(0, self.wz)
        return rows, pl.ds(pl.multiple_of((z % self.zl) * self.wz, 128), self.wz)

    def _send(self, i, src, dst, device):
        copy = remote(src, dst, self.ss.at[i], self.rs.at[i], device)
        copy.start()
        self.copies.append(copy)
        return copy

    def stage(self, s):
        p, X, Y, Z = self.p, self.X, self.Y, self.Z
        if s == 0:
            self.core = [
                self._send(x, self.full.at[ds(self.rows_of(x, 1 - p.k), self.shard), :], self.cr.at[x], p.peer("k", 1))
                for x in range(X)
            ]
        elif s == 1:
            for copy in self.core:
                copy.wait_recv()
            self.xc = []
            for d in range(1, X):
                to = p.to("x", d)

                def one(at, to=to, d=d):
                    mine = self.full[pl.ds(pl.multiple_of(self.rows_of(to, p.k) + at, 16), 16), :]
                    self.xs[d - 1, pl.ds(at, 16), :] = (mine + self.cr[to, pl.ds(at, 16), :]).astype(bf16)

                by_rows(self.shard, 16, one)
                self.xc.append(self._send(X + d - 1, self.xs.at[d - 1], self.xr.at[d - 1], p.peer("x", d)))
        elif s == 2:
            for copy in self.xc:
                copy.wait_recv()

            def total(at, n=16):
                value = self.full[pl.ds(pl.multiple_of(self.rows_of(p.x, p.k) + at, 16), n), :]
                value = value + self.cr[p.x, pl.ds(at, n), :]
                for d in range(1, X):
                    value = value + self.xr[d - 1, pl.ds(at, n), :].astype(f32)
                return value

            self.yc = []
            for d in range(1, Y):
                base = p.to("y", d) * self.ry

                def one(at, base=base, d=d):
                    self.ys[d - 1, pl.ds(at, 16), :] = total(pl.multiple_of(base + at, 16)).astype(bf16)

                by_rows(self.ry, 16, one)
                self.yc.append(self._send(2 * X - 2 + d, self.ys.at[d - 1], self.yr.at[d - 1], p.peer("y", d)))

            def mine(at):
                at = pl.multiple_of(p.y * self.ry + at, 16)
                self.cr[p.x, pl.ds(at, 16), :] = total(at)

            by_rows(self.ry, 16, mine)
        elif s == 3:
            for copy in self.yc:
                copy.wait_recv()

            def total(z):
                rows, lanes = self.piece_at(z)
                value = self.cr[p.x, pl.ds(pl.multiple_of(p.y * self.ry + rows, 16), self.rz), lanes]
                for d in range(1, Y):
                    value = value + self.yr[d - 1, pl.ds(rows, self.rz), lanes].astype(f32)
                return value

            self.zc = []
            base = 2 * X - 1 + Y - 1
            for d in range(1, Z):
                self.zs[d - 1] = total(p.to("z", d)).astype(self.late)
                self.zc.append(self._send(base + d - 1, self.zs.at[d - 1], self.zin.at[d - 1], p.peer("z", d)))
            self.piece[...] = total(p.z)
        elif s == 4:
            for copy in self.zc:
                copy.wait_recv()
            value = self.piece[...]
            for d in range(1, Z):
                value = value + self.zin[d - 1].astype(f32)
            self.piece[...] = value
            rows, lanes = self.piece_at(p.z)
            here = self.out.at[pl.ds(pl.multiple_of(p.y * self.ry + rows, 16), self.rz), lanes]
            here[...] = value.astype(self.late)
            base = 2 * X - 1 + Y - 1 + Z - 1
            self.gz = [self._send(base + d - 1, here, here, p.peer("z", d)) for d in range(1, Z)]
        elif s == 5:
            for copy in self.gz:
                copy.wait_recv()
            here = self.out.at[pl.ds(pl.multiple_of(p.y * self.ry, 16), self.ry), :]
            base = 2 * X - 1 + Y - 1 + 2 * (Z - 1)
            self.gy = [self._send(base + d - 1, here, here, p.peer("y", d)) for d in range(1, Y)]
        elif s == 6:
            for copy in self.gy:
                copy.wait_recv()

    def drain(self):
        for copy in self.copies:
            copy.wait_send()


STAGES = 7


class Step:
    def __init__(self, mesh, samples, slots, dim, edges, c_in):
        self.n_row, self.n_col = mesh.shape["row"], mesh.shape["col"]
        self.grid = sizes_of(self.n_row, self.n_col)
        self.S, self.C, self.D, self.E, self.c_in = samples, slots, dim, edges, c_in
        self.N = MESH_DEV
        self.SH = dim // self.n_col
        self.R, self.Q = self.n_row * self.N, self.n_col * self.N
        chunk = lambda width, late: Reduce(self.grid, dim, self.n_col, width, late)
        self.chunks = [
            chunk(dim + N_OUT, f32),
            chunk(2 * dim, bf16),
            chunk(2 * dim, bf16),
            chunk(dim, bf16),
            chunk(N_IN, f32),
        ]
        X, Y, Z = self.grid
        S, C, D, E, N, R, Q = self.S, self.C, self.D, self.E, self.N, self.R, self.Q
        vm = pltpu.VMEM
        dma = lambda *shape: pltpu.SemaphoreType.DMA(shape)
        self.shapes = dict(
            wib=vm((D, N_IN), bf16),
            wlb=vm((6, D, D), bf16),
            wob=vm((D, N_OUT), bf16),
            nm=vm((N, C), bf16),
            nv=vm((N, C), bf16),
            cm=vm((C, N), bf16),
            cmv=vm((C, N), bf16),
            cw=vm((C, 128), f32),
            cnt=vm((N, 128), f32),
            fp=vm((S * C, D), f32),
            gl=vm((S * C, D), bf16),
            tp=vm((S * C, D), f32),
            go=vm((S * C, D), bf16),
            dp=vm((S * C, N_OUT), bf16),
            dt=vm((S * C, D), bf16),
            av=vm((S * N, D), bf16),
            sp=vm((S * N, D), f32),
            ml=vm((S * N, D), f32),
            mlb=vm((S * N, D), bf16),
            agb=vm((S * N, D), bf16),
            mnb=vm((S * N, D), bf16),
            sg=vm((S * N, D), f32),
            dmn=vm((S * N, D), f32),
            dbb=vm((S * N, D), bf16),
            dsb=vm((S * N, D), bf16),
            drb=vm((S * N, D), bf16),
            d2b=vm((S * N, D), bf16),
            sr=vm((S, R + Q, D), bf16),
            oh=vm((E, R + Q), bf16),
            oht=vm((R + Q, E), bf16),
            ep=vm((S, E, D), f32),
            ac=vm((E, D), bf16),
            tmp=vm((R + Q, D), f32),
            part=vm((S, Q, D), f32),
            pcr=vm((S, X, N, D), f32),
            pxs=vm((S, X - 1, N, D), bf16),
            pxr=vm((S, X - 1, N, D), bf16),
            da=vm((S, Q, D), bf16),
            down=vm((S, Z, N, D), f32),
            dys=vm((S, Y - 1, Z, N, D), bf16),
            dyr=vm((S, Y - 1, Z, N, D), bf16),
            dzs=vm((S, Z - 1, N, D), bf16),
            dzr=vm((S, Z - 1, N, D), bf16),
            loss=vm((8, 128), f32),
            l_sem=dma(6),
            w_ss=dma(8, 1 + 2 * (X - 1)),
            w_rs=dma(8, 1 + 2 * (X - 1)),
            mz_ss=dma(S, Z - 1),
            mz_rs=dma(S, Z - 1),
            my_ss=dma(S, Y - 1, Z),
            my_rs=dma(S, Y - 1, Z),
            mr_ss=dma(S, 1 + 2 * (X - 1)),
            mr_rs=dma(S, 1 + 2 * (X - 1)),
            pk_ss=dma(2, S, X),
            pk_rs=dma(2, S, X),
            px_ss=dma(2, S, X - 1),
            px_rs=dma(2, S, X - 1),
            a_ss=dma(S, 1 + 2 * (X - 1)),
            a_rs=dma(S, 1 + 2 * (X - 1)),
            dy_ss=dma(S, Y - 1),
            dy_rs=dma(S, Y - 1),
            dz_ss=dma(S, Z - 1),
            dz_rs=dma(S, Z - 1),
        )

    def vmem_bytes(self):
        total = 0
        for s in [*self.shapes.values(), *[s for c in self.chunks for s in c.scratch()]]:
            dtype = getattr(s, "dtype", None)
            if dtype in (jnp.dtype(f32), jnp.dtype(bf16)):
                size = jnp.dtype(dtype).itemsize
                for n in s.shape[:-1]:
                    size *= n
                total += size * -(-s.shape[-1] // 128) * 128
        return total

    def scratch(self):
        total = Total.scratch(*self.grid)
        return [*self.shapes.values(), *total, *total, *[s for c in self.chunks for s in c.scratch()]]

    def kernel(self, count, x, tgt, area, node, snd, rcv, wit, wl, wo, *refs):
        S, C, D, E, N, R, Q, SH = self.S, self.C, self.D, self.E, self.N, self.R, self.Q, self.SH
        X, Y, Z = self.grid
        outs, stats, refs = refs[:5], refs[5], refs[6:]
        v = types.SimpleNamespace(**dict(zip(self.shapes, refs)))
        refs = refs[len(self.shapes) :]
        p = Place(self.n_row, self.n_col)
        area_sum, loss_sum = Total(p, refs[:7]), Total(p, refs[7:14])
        refs = refs[14:]
        for chunk in self.chunks:
            many = len(chunk.scratch())
            chunk.bind(p, refs[:many])
            refs = refs[many:]

        def weight_rows(i, col):
            which = WIRE[i]
            whole = v.wib if which == "in" else v.wob if which == "out" else v.wlb.at[which]
            return whole.at[ds(col * SH, SH), :]

        def w_copy(i, j, d=0):
            rows = weight_rows(i, 2 * p.to("x", -d) + p.k if j == 2 else p.col)
            at = (0, d, X - 1 + d)[j]
            device = p.peer("x", d) if j == 1 else p.peer("k", 1)
            return remote(rows, rows, v.w_ss.at[i, at], v.w_rs.at[i, at], device)

        hops = range(1, X)

        def w_forward(i):
            for d in hops:
                w_copy(i, 1, d).wait_recv()
                w_copy(i, 2, d).start()

        def w_get(i):
            w_copy(i, 0).wait_recv()
            for d in hops:
                w_copy(i, 2, d).wait_recv()

        W = lambda which: v.wlb[which]
        own = ds(p.col * SH, SH)
        v.wib[own, :] = wit[...]
        loads = [pltpu.make_async_copy(wl.at[m], v.fp.at[m * SH : (m + 1) * SH, :], v.l_sem.at[m]) for m in range(6)]
        for load in loads:
            load.start()
        for m, load in enumerate(loads):
            load.wait()
            v.wlb[m, own, :] = v.fp[m * SH : (m + 1) * SH, :].astype(bf16)
        v.wob[own, :] = jnp.zeros((SH, N_OUT), bf16)
        v.wob[own, 0:C_OUT] = wo[...].astype(bf16)
        p.barrier()
        for i in range(8):
            w_copy(i, 0).start()
            for d in hops:
                w_copy(i, 1, d).start()

        used = count[0]
        node_row = node[...]
        match = (lax.broadcasted_iota(jnp.int32, (N, C), 0) == node_row).astype(f32)
        v.nm[...] = match.astype(bf16)
        match = match * (lax.broadcasted_iota(jnp.int32, (N, C), 1) < used).astype(f32)
        v.nv[...] = match.astype(bf16)
        v.cnt[...] = jnp.broadcast_to(jnp.maximum(jnp.sum(match, axis=1, keepdims=True), 1.0), (N, 128))
        node_col = jnp.transpose(jnp.broadcast_to(node_row, (128, C)))
        area_row = area[...] * (lax.broadcasted_iota(jnp.int32, (1, C), 1) < used).astype(f32)
        v.cw[...] = jnp.transpose(jnp.broadcast_to(area_row, (128, C)))
        match = (lax.broadcasted_iota(jnp.int32, (C, 128), 1) == node_col).astype(f32)
        v.cm[...] = match[:, :N].astype(bf16)
        match = match * (lax.broadcasted_iota(jnp.int32, (C, 128), 0) < used).astype(f32)
        v.cmv[...] = match[:, :N].astype(bf16)
        area_sum.value[...] = jnp.broadcast_to(jnp.sum(area_row), (8, 128))
        area_sum.start("k")

        w_forward(0)
        w_get(0)

        def encode(s, carry):
            at = ds(s * C, C)
            pre = mm_nt(x[s], v.wib[:, : self.c_in])
            v.fp[at, :] = pre
            v.gl[at, :] = silu(pre).astype(bf16)
            here = ds(s * N, N)
            v.av[here, :] = (mm(v.nv[...], v.gl[at, :]) / v.cnt[:, 0:1]).astype(bf16)
            return carry

        lax.fori_loop(0, S, encode, 0)
        area_sum.finish("k")
        area_sum.start("x")
        w_forward(1)
        w_get(1)
        pre = mm(v.av[...], W(0))
        v.sp[...] = pre
        v.ml[...] = silu(pre)
        v.mlb[...] = v.ml[...].astype(bf16)
        w_forward(2)
        w_get(2)
        v.tmp[0 : S * N, :] = mm(v.mlb[...], W(1))
        for s in range(S):
            v.sr[s, ds(p.row * N, N), :] = v.tmp[s * N : (s + 1) * N, :].astype(bf16)
        w_forward(3)
        w_get(3)

        def mz(s, d):
            rows = v.sr.at[s, ds(p.row * N, N), :]
            return remote(rows, rows, v.mz_ss.at[s, d - 1], v.mz_rs.at[s, d - 1], p.peer("z", d))

        def my(s, d, e):
            rows = v.sr.at[s, ds((p.to("z", -e) * Y + p.y) * N, N), :]
            return remote(rows, rows, v.my_ss.at[s, d - 1, e], v.my_rs.at[s, d - 1, e], p.peer("y", d))

        def mr(s, j, d=0):
            col = 2 * p.to("x", -d) + p.k if j == 2 else p.col
            rows = v.sr.at[s, ds(R + col * N, N), :]
            at = (0, d, X - 1 + d)[j]
            return remote(rows, rows, v.mr_ss.at[s, at], v.mr_rs.at[s, at], p.peer("x", d) if j == 1 else p.peer("k", 1))

        for s in range(S):
            for d in range(1, Z):
                mz(s, d).start()
            for d in range(1, Y):
                my(s, d, 0).start()
        v.tmp[0 : S * N, :] = mm(v.mlb[...], W(2))
        for s in range(S):
            v.sr[s, ds(R + p.col * N, N), :] = v.tmp[s * N : (s + 1) * N, :].astype(bf16)
        for s in range(S):
            mr(s, 0).start()
            for d in hops:
                mr(s, 1, d).start()
        area_sum.finish("x")
        area_sum.start("y")

        def table(index, base, rows):
            def down(at):
                hit = lax.broadcasted_iota(jnp.int32, (128, E), 0) + at == index
                v.oht[pl.ds(pl.multiple_of(base + at, 128), 128), :] = hit.astype(f32).astype(bf16)

            by_rows(rows, 128, down)
            column = jnp.transpose(jnp.broadcast_to(index, (128, E)))
            for at in range(0, rows, 128):
                hit = lax.broadcasted_iota(jnp.int32, (E, 128), 1) + at == column
                v.oh[:, base + at : base + at + 128] = hit.astype(f32).astype(bf16)

        table(snd[...], 0, R)
        table(rcv[...], R, Q)

        w_forward(4)
        w_get(4)

        def skip(at):
            v.tp[pl.ds(at, 512), :] = mm(v.gl[pl.ds(at, 512), :], W(5))

        by_rows(S * C, 512, skip)
        area_sum.finish("y")
        area_sum.start("z")
        w_forward(5)

        def pk(t, s, xx):
            rows = v.part.at[s, ds((2 * xx + 1 - p.k) * N, N), :]
            return remote(rows, v.pcr.at[s, xx], v.pk_ss.at[t, s, xx], v.pk_rs.at[t, s, xx], p.peer("k", 1))

        def px(t, s, d):
            return remote(v.pxs.at[s, d - 1], v.pxr.at[s, d - 1], v.px_ss.at[t, s, d - 1], v.px_rs.at[t, s, d - 1], p.peer("x", d))

        def col_second(t, s):
            for xx in range(X):
                pk(t, s, xx).wait_recv()
            for d in hops:
                px_to = p.to("x", d)
                mine = v.part[s, ds((2 * px_to + p.k) * N, N), :]
                v.pxs[s, d - 1] = (mine + v.pcr[s, px_to]).astype(bf16)
                px(t, s, d).start()

        def col_last(t, s):
            total = v.part[s, ds(p.col * N, N), :] + v.pcr[s, p.x]
            for d in hops:
                px(t, s, d).wait_recv()
                total = total + v.pxr[s, d - 1].astype(f32)
            return total

        def arrive(s):
            for d in range(1, Z):
                mz(s, d).wait_recv()
                for b in range(1, Y):
                    my(s, b, d).start()
            for d in hops:
                mr(s, 1, d).wait_recv()
                mr(s, 2, d).start()

        def edges(s):
            for b in range(1, Y):
                for e in range(Z):
                    my(s, b, e).wait_recv()
            mr(s, 0).wait_recv()
            for d in hops:
                mr(s, 2, d).wait_recv()

            def pick(at):
                pre = mm(v.oh[pl.ds(at, 512), :], v.sr[s])
                v.ep[s, pl.ds(at, 512), :] = pre
                v.ac[pl.ds(at, 512), :] = silu(pre).astype(bf16)

            by_rows(E, 512, pick)
            v.part[s] = mm(v.oht[R:, :], v.ac[...])
            for xx in range(X):
                pk(0, s, xx).start()

        def forward(i, carry):
            @pl.when(i < S)
            def _():
                arrive(i)

            @pl.when((i >= 1) & (i <= S))
            def _():
                edges(i - 1)

            @pl.when(i >= 2)
            def _():
                col_second(0, i - 2)

            return carry

        lax.fori_loop(0, S + 2, forward, 0)
        area_sum.finish("z")
        w_get(5)
        for i in (6, 7):
            w_forward(i)
        for s in range(S):
            v.agb[s * N : (s + 1) * N, :] = (col_last(0, s) * (1.0 / DEG)).astype(bf16)

        v.mnb[...] = (v.ml[...] + mm(v.agb[...], W(3))).astype(bf16)
        w_get(6)
        w_get(7)
        v.dp[...] = jnp.zeros((S * C, N_OUT), bf16)
        v.loss[...] = jnp.zeros((8, 128), f32)
        scale = 1.0 / (C_OUT * S * area_sum.value[0:1, 0:1])

        def decode(s, carry):
            at, here = ds(s * C, C), ds(s * N, N)
            rows = mm(v.cm[...], v.mnb[here, :]).astype(bf16)
            pre = mm(rows, W(4)) + v.tp[at, :]
            v.tp[at, :] = pre
            v.go[at, :] = silu(pre).astype(bf16)
            error = mm(v.go[at, :], v.wob[...])[:, :C_OUT] - tgt[s].astype(f32)
            weighted = v.cw[:, :C_OUT] * error
            v.loss[0:1, 0:C_OUT] = v.loss[0:1, 0:C_OUT] + jnp.sum(weighted * error, axis=0, keepdims=True)
            v.dp[at, 0:C_OUT] = (2.0 * weighted * scale).astype(bf16)
            v.dt[at, :] = (silu_slope(v.tp[at, :]) * mm_nt(v.dp[at, :], v.wob[...])).astype(bf16)
            v.sg[here, :] = mm(v.nm[...], v.dt[at, :])
            return carry

        lax.fori_loop(0, S, decode, 0)
        high, low = high_low(v.sg[...])
        v.dmn[...] = mm_nt(high, W(4)) + mm_nt(low, W(4))
        v.dbb[...] = v.dmn[...].astype(bf16)
        v.tmp[0 : S * N, :] = mm_nt(v.dbb[...], W(3))
        for s in range(S):
            v.da[s, ds(p.col * N, N), :] = v.tmp[s * N : (s + 1) * N, :].astype(bf16)

        def ac(s, j, d=0):
            col = 2 * p.to("x", -d) + p.k if j == 2 else p.col
            rows = v.da.at[s, ds(col * N, N), :]
            at = (0, d, X - 1 + d)[j]
            return remote(rows, rows, v.a_ss.at[s, at], v.a_rs.at[s, at], p.peer("x", d) if j == 1 else p.peer("k", 1))

        for s in range(S):
            ac(s, 0).start()
            for d in hops:
                ac(s, 1, d).start()
        loss_sum.value[...] = jnp.broadcast_to(jnp.sum(v.loss[...]), (8, 128))
        loss_sum.start("k")

        first, second, third, fourth, fifth = self.chunks
        first.full[:, 0:D] = mm_tn(v.gl[...], v.dt[...])
        first.full[:, D : D + N_OUT] = mm_tn(v.go[...], v.dp[...])
        first.stage(0)
        high, low = high_low(v.sg[...])
        second.full[:, 0:D] = mm_tn(v.mnb[...], high) + mm_tn(v.mnb[...], low)
        second.full[:, D : 2 * D] = mm_tn(v.agb[...], v.dbb[...])
        second.stage(0)

        def skip_back(at):
            v.tp[pl.ds(at, 512), :] = mm_nt(v.dt[pl.ds(at, 512), :], W(5))

        by_rows(S * C, 512, skip_back)
        loss_sum.finish("k")
        loss_sum.start("x")
        first.stage(1)
        second.stage(1)

        def dy(s, d):
            return remote(v.dys.at[s, d - 1], v.dyr.at[s, d - 1], v.dy_ss.at[s, d - 1], v.dy_rs.at[s, d - 1], p.peer("y", d))

        def dz(s, d):
            return remote(v.dzs.at[s, d - 1], v.dzr.at[s, d - 1], v.dz_ss.at[s, d - 1], v.dz_rs.at[s, d - 1], p.peer("z", d))

        def pass_on(s):
            for d in hops:
                ac(s, 1, d).wait_recv()
                ac(s, 2, d).start()

        def edges_back(s):
            ac(s, 0).wait_recv()
            for d in hops:
                ac(s, 2, d).wait_recv()

            def pick(at):
                grad = mm(v.oh[pl.ds(at, 512), R:], v.da[s])
                v.ac[pl.ds(at, 512), :] = (silu_slope(v.ep[s, pl.ds(at, 512), :]) * grad * (1.0 / DEG)).astype(bf16)

            by_rows(E, 512, pick)
            v.tmp[...] = mm(v.oht[...], v.ac[...])
            for d in range(1, Y):
                for e in range(Z):
                    v.dys[s, d - 1, e] = v.tmp[ds((e * Y + p.to("y", d)) * N, N), :].astype(bf16)
                dy(s, d).start()
            for e in range(Z):
                v.down[s, e] = v.tmp[ds((e * Y + p.y) * N, N), :]
            v.part[s] = v.tmp[R:, :]
            for xx in range(X):
                pk(1, s, xx).start()

        def row_second(s):
            for d in range(1, Y):
                dy(s, d).wait_recv()

            def summed(e):
                total = v.down[s, e]
                for d in range(1, Y):
                    total = total + v.dyr[s, d - 1, e].astype(f32)
                return total

            for d in range(1, Z):
                v.dzs[s, d - 1] = summed(p.to("z", d)).astype(bf16)
                dz(s, d).start()
            v.down[s, p.z] = summed(p.z)

        for s in range(S):
            for xx in range(X):
                pk(0, s, xx).wait_send()
            for d in hops:
                px(0, s, d).wait_send()

        def backward(i, carry):
            @pl.when(i < S)
            def _():
                pass_on(i)
                edges_back(i)

            @pl.when(i >= 1)
            def _():
                col_second(1, i - 1)
                row_second(i - 1)

            return carry

        lax.fori_loop(0, S + 1, backward, 0)
        first.stage(2)
        second.stage(2)
        for s in range(S):
            v.drb[s * N : (s + 1) * N, :] = col_last(1, s).astype(bf16)
        for s in range(S):
            total = v.down[s, p.z]
            for d in range(1, Z):
                dz(s, d).wait_recv()
                total = total + v.dzr[s, d - 1].astype(f32)
            v.dsb[s * N : (s + 1) * N, :] = total.astype(bf16)

        third.full[:, 0:D] = mm_tn(v.mlb[...], v.dsb[...])
        third.full[:, D : 2 * D] = mm_tn(v.mlb[...], v.drb[...])
        third.stage(0)
        whole = v.dmn[...] + mm_nt(v.dsb[...], W(1)) + mm_nt(v.drb[...], W(2))
        v.d2b[...] = (silu_slope(v.sp[...]) * whole).astype(bf16)
        third.stage(1)
        fourth.full[...] = mm_tn(v.av[...], v.d2b[...])
        fourth.stage(0)
        v.dmn[...] = mm_nt(v.d2b[...], W(0))
        first.stage(3)
        second.stage(3)

        def encode_back(s, carry):
            at, here = ds(s * C, C), ds(s * N, N)
            high, low = high_low(v.dmn[here, :] / v.cnt[:, 0:1])
            grad = v.tp[at, :] + mm(v.cmv[...], high) + mm(v.cmv[...], low)
            v.dt[at, :] = (silu_slope(v.fp[at, :]) * grad).astype(bf16)
            return carry

        lax.fori_loop(0, S, encode_back, 0)
        third.stage(2)
        fourth.stage(1)
        fifth.full[:, self.c_in :] = jnp.zeros((D, N_IN - self.c_in), f32)
        for s in range(S):
            grad = mm_tn(v.dt[s * C : (s + 1) * C, :], x[s])
            if s:
                grad = grad + fifth.full[:, : self.c_in]
            fifth.full[:, : self.c_in] = grad
        fifth.stage(0)
        first.stage(4)
        second.stage(4)
        loss_sum.finish("x")
        loss_sum.start("y")
        third.stage(3)
        fourth.stage(2)
        fifth.stage(1)
        first.stage(5)
        second.stage(5)
        third.stage(4)
        fourth.stage(3)
        fifth.stage(2)
        loss_sum.finish("y")
        loss_sum.start("z")
        first.stage(6)
        outs[0][...] = first.out[...]
        second.stage(6)
        outs[1][...] = second.out[...]
        third.stage(5)
        fourth.stage(4)
        fifth.stage(3)
        third.stage(6)
        outs[2][...] = third.out[...]
        fourth.stage(5)
        fifth.stage(4)
        fourth.stage(6)
        outs[3][...] = fourth.out[...]
        fifth.stage(5)
        loss_sum.finish("z")
        stats[...] = loss_sum.value[...] / (C_OUT * S * area_sum.value[...])
        fifth.stage(6)
        outs[4][...] = fifth.out[...]

        for i in range(8):
            w_copy(i, 0).wait_send()
            for d in hops:
                w_copy(i, 1, d).wait_send()
                w_copy(i, 2, d).wait_send()
        for s in range(S):
            for d in range(1, Z):
                mz(s, d).wait_send()
                dz(s, d).wait_send()
            for d in range(1, Y):
                for e in range(Z):
                    my(s, d, e).wait_send()
                dy(s, d).wait_send()
            for copy in (mr, ac):
                copy(s, 0).wait_send()
                for d in hops:
                    copy(s, 1, d).wait_send()
                    copy(s, 2, d).wait_send()
            for xx in range(X):
                pk(1, s, xx).wait_send()
            for d in hops:
                px(1, s, d).wait_send()
        area_sum.drain()
        loss_sum.drain()
        for chunk in self.chunks:
            chunk.drain()

    def __call__(self, count, x, tgt, area, node, snd, rcv, wit, wl, wo):
        vm = pl.BlockSpec(memory_space=pltpu.VMEM)
        return pl.pallas_call(
            self.kernel,
            out_shape=[jax.ShapeDtypeStruct((self.SH, c.w), c.late) for c in self.chunks] + [jax.ShapeDtypeStruct((8, 128), f32)],
            in_specs=[pl.BlockSpec(memory_space=pltpu.SMEM)] + [vm] * 7 + [pl.BlockSpec(memory_space=pl.ANY), vm],
            out_specs=[vm] * 6,
            scratch_shapes=self.scratch(),
            name="train_step",
            compiler_params=pltpu.CompilerParams(collective_id=0, has_side_effects=True, vmem_limit_bytes=67043328),
        )(count, x, tgt, area, node, snd, rcv, wit, wl, wo)


def kernel_body(
    mesh,
    inputs,
    targets,
    cell_area,
    cell_count,
    cell_node,
    edge_senders,
    edge_receivers,
    weight_input,
    weight_latent,
    weight_output,
):
    samples, slots, c_in = inputs.shape
    dim = weight_latent.shape[2]
    step = Step(mesh, samples, slots, dim, edge_senders.shape[0], c_in)
    wit = jnp.pad(weight_input.T.astype(bf16), ((0, 0), (0, N_IN - c_in)))
    one, two, three, four, five, stats = step(
        cell_count,
        inputs,
        targets,
        cell_area[None, :],
        cell_node[None, :],
        edge_senders[None, :],
        edge_receivers[None, :],
        wit,
        weight_latent,
        weight_output,
    )
    two, three, four = (g.astype(f32) for g in (two, three, four))
    gradient_latent = jnp.stack(
        [four[:, :dim], three[:, :dim], three[:, dim : 2 * dim], two[:, dim : 2 * dim], two[:, :dim], one[:, :dim]]
    )
    return stats[0, 0], five[:, :c_in].T, gradient_latent, one[:, dim : dim + C_OUT]


def native_gradients(
    inputs,
    targets,
    cell_area,
    cell_count,
    cell_node,
    edge_senders,
    edge_receivers,
    weight_input,
    weight_latent,
    weight_output,
):
    full_input, complete_latent, full_output = (
        lax.all_gather(weight_input.astype(jnp.bfloat16), "col", axis=1, tiled=True),
        lax.all_gather(weight_latent.astype(jnp.bfloat16), "col", axis=1, tiled=True),
        lax.all_gather(weight_output.astype(jnp.bfloat16), "col", axis=0, tiled=True),
    )
    samples = inputs.shape[0]
    slots = inputs.shape[1]
    valid = (jnp.arange(slots, dtype=jnp.int32) < cell_count[0]).astype(jnp.float32)
    cell_weight = cell_area * valid
    area_total = lax.psum(jnp.sum(cell_weight), ("row", "col"))
    first_pre = reduced_matmul("sci,id->scd", inputs, full_input)
    grid_latent = jax.nn.silu(first_pre).astype(jnp.bfloat16)
    node_match = (cell_node[None, :] == jnp.arange(MESH_DEV, dtype=jnp.int32)[:, None]).astype(
        jnp.float32
    )
    node_match_low = node_match.astype(jnp.bfloat16)
    cell_match = node_match_low.T
    node_valid = node_match * valid[None, :]
    node_sum = reduced_matmul("nc,scd->snd", node_valid.astype(jnp.bfloat16), grid_latent)
    node_lower_limit = jnp.maximum(jnp.sum(node_valid, axis=1), 1.0)
    node_average = node_sum / node_lower_limit[None, :, None]
    average_reduced = node_average.astype(jnp.bfloat16)
    second_activation_input = reduced_matmul("kaj,jz->kaz", average_reduced, complete_latent[0])
    mesh_latent = jax.nn.silu(second_activation_input)
    mesh_state_reduced = mesh_latent.astype(jnp.bfloat16)
    receiver_local_part = reduced_matmul("kaj,jz->kaz", mesh_state_reduced, complete_latent[2])
    receiver_block = lax.all_gather(receiver_local_part, "col", axis=1, tiled=True)
    sender_block = reduced_matmul(
        "kaj,jz->kaz",
        lax.all_gather(mesh_state_reduced, "row", axis=1, tiled=True),
        complete_latent[1],
    )
    receiver_rows = receiver_block.shape[1]
    sender_rows = sender_block.shape[1]
    sender_match = one_hot_table(edge_senders, sender_rows)
    receiver_match = one_hot_table(edge_receivers, receiver_rows)
    edge_pre = pick_rows(sender_match, sender_block) + pick_rows(receiver_match, receiver_block)
    partial_sums = add_into_rows(receiver_match, jax.nn.silu(edge_pre))
    message_total = lax.psum_scatter(partial_sums, "col", scatter_dimension=1, tiled=True) / DEG
    message_total_reduced = message_total.astype(jnp.bfloat16)
    residual_branch = reduced_matmul("kaj,jz->kaz", message_total_reduced, complete_latent[3])
    mesh_next = mesh_latent + residual_branch
    decode_rows = reduced_matmul("cn,snd->scd", cell_match, mesh_next.astype(jnp.bfloat16)).astype(
        jnp.bfloat16
    )
    third_pre = reduced_matmul("scd,de->sce", decode_rows, complete_latent[4]) + reduced_matmul(
        "scd,de->sce", grid_latent, complete_latent[5]
    )
    grid_out = jax.nn.silu(third_pre).astype(jnp.bfloat16)
    predict = reduced_matmul("scd,do->sco", grid_out, full_output)
    error = predict - targets.astype(jnp.float32)
    denominator = C_OUT * samples * area_total
    weighted = cell_weight[None, :, None] * error
    loss_value = lax.psum(jnp.sum(weighted * error), ("row", "col")) / denominator
    d_predict = (2.0 * weighted / denominator).astype(jnp.bfloat16)
    grad_output_local = reduced_matmul("scd,sco->do", grid_out, d_predict)
    d_grid_out = reduced_matmul("sco,do->scd", d_predict, full_output)
    d_third = silu_grad(third_pre, d_grid_out).astype(jnp.bfloat16)
    grad_decode = reduced_matmul("scd,sce->de", decode_rows, d_third)
    grad_skip = reduced_matmul("scd,sce->de", grid_latent, d_third)
    d_decode = reduced_matmul("sce,de->scd", d_third, complete_latent[4])
    d_skip = reduced_matmul("sce,de->scd", d_third, complete_latent[5])
    d_mesh_next = jnp.einsum("nc,scd->snd", node_match, d_decode, precision=highest)
    residual_branch_gradient = d_mesh_next.astype(jnp.bfloat16)
    branch_gradient_sum = reduced_matmul(
        "lhg,lhj->gj", message_total_reduced, residual_branch_gradient
    )
    message_total_gradient = reduced_matmul(
        "pyk,ck->pyc", residual_branch_gradient, complete_latent[3]
    ).astype(jnp.bfloat16)
    d_block = lax.all_gather(message_total_gradient, "col", axis=1, tiled=True)
    d_edge_message = reduced_matmul("es,ksd->ked", receiver_match, d_block)
    d_edge_pre = silu_grad(edge_pre, d_edge_message / DEG)
    d_sender_part = add_into_rows(sender_match, d_edge_pre)
    d_receiver_part = add_into_rows(receiver_match, d_edge_pre)
    sender_gradient = lax.psum_scatter(
        d_sender_part.astype(jnp.bfloat16), "row", scatter_dimension=1, tiled=True
    )
    receiver_gradient = lax.psum_scatter(
        d_receiver_part.astype(jnp.bfloat16), "col", scatter_dimension=1, tiled=True
    )
    sender_weight_gradient = reduced_matmul("lhg,lhj->gj", mesh_state_reduced, sender_gradient)
    receiver_weight_gradient = reduced_matmul("lhg,lhj->gj", mesh_state_reduced, receiver_gradient)
    d_mesh = (
        d_mesh_next
        + reduced_matmul("pyk,ck->pyc", sender_gradient, complete_latent[1])
        + reduced_matmul("pyk,ck->pyc", receiver_gradient, complete_latent[2])
    )
    hidden_second_gradient = silu_grad(second_activation_input, d_mesh).astype(jnp.bfloat16)
    encoder_gradient = reduced_matmul("lhg,lhj->gj", average_reduced, hidden_second_gradient)
    node_average_gradient = (
        reduced_matmul("pyk,ck->pyc", hidden_second_gradient, complete_latent[0])
        / node_lower_limit[None, :, None]
    )
    d_grid = d_skip + valid[None, :, None] * pick_rows(cell_match, node_average_gradient)
    d_first = silu_grad(first_pre, d_grid).astype(jnp.bfloat16)
    grad_input_local = reduced_matmul("sci,scd->id", inputs, d_first)
    grad_latent_local = jnp.stack(
        [
            encoder_gradient,
            sender_weight_gradient,
            receiver_weight_gradient,
            branch_gradient_sum,
            grad_decode,
            grad_skip,
        ]
    )
    local_terms = (grad_input_local, grad_latent_local, grad_output_local)
    whole_input, whole_latent, whole_output = lax.psum(
        (local_terms[0], local_terms[1], local_terms[2]), ("row", "col")
    )
    column = lax.axis_index("col")
    width_input = weight_input.shape[1]
    width_latent = weight_latent.shape[1]
    width_output = weight_output.shape[0]
    gradient_input = lax.dynamic_slice_in_dim(whole_input, column * width_input, width_input, 1)
    gradient_latent = lax.dynamic_slice_in_dim(whole_latent, column * width_latent, width_latent, 1)
    gradient_output = lax.dynamic_slice_in_dim(whole_output, column * width_output, width_output, 0)
    return loss_value, gradient_input, gradient_latent, gradient_output


def body(
    mesh,
    inputs,
    targets,
    cell_area,
    cell_count,
    cell_node,
    edge_senders,
    edge_receivers,
    weight_input,
    weight_latent,
    weight_output,
    mean_input,
    mean_latent,
    mean_output,
    square_input,
    square_latent,
    square_output,
):
    given = (inputs, targets, cell_area, cell_count, cell_node, edge_senders, edge_receivers, weight_input, weight_latent, weight_output)
    step = Step(mesh, inputs.shape[0], inputs.shape[1], weight_latent.shape[2], edge_senders.shape[0], inputs.shape[2])
    if step.vmem_bytes() < VMEM_ROOM:
        loss_value, gradient_input, gradient_latent, gradient_output = kernel_body(mesh, *given)
    else:
        loss_value, gradient_input, gradient_latent, gradient_output = native_gradients(*given)
    first_input, second_input, update_input = adam_parts(
        weight_input, gradient_input, mean_input, square_input
    )
    first_latent, second_latent, update_latent = adam_parts(
        weight_latent, gradient_latent, mean_latent, square_latent
    )
    first_output, second_output, update_output = adam_parts(
        weight_output, gradient_output, mean_output, square_output
    )
    weight_sums = jnp.concatenate(
        [
            jnp.sum(weight_input * weight_input)[None],
            jnp.sum(weight_latent * weight_latent, axis=(1, 2)),
            jnp.sum(weight_output * weight_output)[None],
        ]
    )
    update_sums = jnp.concatenate(
        [
            jnp.sum(update_input * update_input)[None],
            jnp.sum(update_latent * update_latent, axis=(1, 2)),
            jnp.sum(update_output * update_output)[None],
        ]
    )
    norm_sums = lax.psum(jnp.stack([weight_sums, update_sums]), "col")
    trust_norms = jnp.sqrt(norm_sums)
    ratio = trust_norms[0] / (trust_norms[1] + trust_epsilon)
    master_input = weight_input - learn_rate * ratio[0] * update_input
    master_latent = weight_latent - learn_rate * ratio[1:7][:, None, None] * update_latent
    master_output = weight_output - learn_rate * ratio[7] * update_output
    return (
        loss_value,
        gradient_input,
        gradient_latent,
        gradient_output,
        first_input,
        first_latent,
        first_output,
        second_input,
        second_latent,
        second_output,
        master_input,
        master_latent,
        master_output,
        master_input.astype(jnp.bfloat16),
        master_latent.astype(jnp.bfloat16),
        master_output.astype(jnp.bfloat16),
        trust_norms,
    )


def solution(mesh):
    placed = (
        P(None, ("row", "col"), None),
        P(None, ("row", "col"), None),
        P(("row", "col")),
        P(("row", "col")),
        P(("row", "col")),
        P(("row", "col")),
        P(("row", "col")),
        P(None, "col"),
        P(None, "col", None),
        P("col", None),
        P(None, "col"),
        P(None, "col", None),
        P("col", None),
        P(None, "col"),
        P(None, "col", None),
        P("col", None),
    )
    return jax.shard_map(
        functools.partial(body, mesh),
        mesh=mesh,
        in_specs=placed,
        out_specs=(
            P(),
            P(None, "col"),
            P(None, "col", None),
            P("col", None),
            P(None, "col"),
            P(None, "col", None),
            P("col", None),
            P(None, "col"),
            P(None, "col", None),
            P("col", None),
            P(None, "col"),
            P(None, "col", None),
            P("col", None),
            P(None, "col"),
            P(None, "col", None),
            P("col", None),
            P(),
        ),
        check_vma=False,
    )
```

```python
import functools
import types

import jax
import jax.numpy as jnp
from jax import lax
from jax.experimental import pallas as pl
from jax.experimental.pallas import tpu as pltpu
from jax.sharding import PartitionSpec as P

C_OUT = 83
DEG = 16
MESH_DEV = 64


highest = lax.Precision.HIGHEST
beta_first = 0.5
beta_second = 0.5
adam_epsilon = 1e-08
trust_epsilon = 1e-06
weight_decay = 0.01
learn_rate = 0.1


def silu_grad(pre_act, grad_out):
    sigma = jax.nn.sigmoid(pre_act)
    return grad_out * sigma * (1.0 + pre_act * (1.0 - sigma))


def reduced_matmul(form, left, right):
    return jnp.einsum(form, left, right, preferred_element_type=jnp.float32)


def split_parts(values):
    upper = values.astype(jnp.bfloat16)
    rest = values - upper.astype(jnp.float32)
    middle = rest.astype(jnp.bfloat16)
    lower = (rest - middle.astype(jnp.float32)).astype(jnp.bfloat16)
    return (upper, middle, lower)


def pick_rows(match, values):
    upper, middle, lower = split_parts(values)
    total = reduced_matmul("es,ksd->ked", match, upper)
    total = total + reduced_matmul("es,ksd->ked", match, middle)
    return total + reduced_matmul("es,ksd->ked", match, lower)


def add_into_rows(match, values):
    upper, middle, lower = split_parts(values)
    total = reduced_matmul("es,ked->ksd", match, upper)
    total = total + reduced_matmul("es,ked->ksd", match, middle)
    return total + reduced_matmul("es,ked->ksd", match, lower)


def one_hot_table(indices, count):
    return (indices[:, None] == jnp.arange(count, dtype=jnp.int32)[None, :]).astype(jnp.bfloat16)


def adam_parts(weight, gradient, first, second):
    new_first = beta_first * first + (1.0 - beta_first) * gradient
    new_second = beta_second * second + (1.0 - beta_second) * gradient * gradient
    update = new_first / (jnp.sqrt(new_second) + adam_epsilon) + weight_decay * weight
    return (new_first, new_second, update)


MESH = pl.DeviceIdType.MESH
bf16 = jnp.bfloat16
f32 = jnp.float32
VMEM_ROOM = 63 * 2**20
N_IN = 256
N_OUT = 128
WIRE = ("in", 0, 1, 2, 5, 3, 4, "out")


def sizes_of(n_row, n_col):
    X = n_col // 2
    Y = X if n_row % X == 0 else 1
    return X, Y, n_row // Y


class Place:
    def __init__(self, n_row, n_col):
        self.K = 2
        self.X, self.Y, self.Z = sizes_of(n_row, n_col)
        self.row, self.col = lax.axis_index("row"), lax.axis_index("col")
        self.z, self.y = self.row // self.Y, self.row % self.Y
        self.x, self.k = self.col // 2, self.col % 2

    def to(self, axis, d):
        n = getattr(self, axis.upper())
        return (getattr(self, axis) + d) % n

    def peer(self, axis, d):
        at = {a: getattr(self, a) for a in "zyxk"}
        at[axis] = self.to(axis, d)
        return (at["z"] * self.Y + at["y"], at["x"] * 2 + at["k"])

    def barrier(self):
        sem = pltpu.get_barrier_semaphore()
        peers = [self.peer(a, d) for a in "kxyz" for d in range(1, getattr(self, a.upper()))]
        for peer in peers:
            pl.semaphore_signal(sem, inc=1, device_id=peer, device_id_type=MESH)
        pl.semaphore_wait(sem, len(peers))


def remote(src, dst, send_sem, recv_sem, device):
    return pltpu.make_async_remote_copy(
        src_ref=src,
        dst_ref=dst,
        send_sem=send_sem,
        recv_sem=recv_sem,
        device_id=device,
        device_id_type=MESH,
    )


def ds(start, size):
    if isinstance(start, int):
        return pl.ds(start, size)
    return pl.ds(pl.multiple_of(start, size if size % 128 else 128), size)


def by_rows(count, step, todo):
    def one(i, carry):
        todo(pl.multiple_of(i * step, step))
        return carry

    lax.fori_loop(0, count // step, one, 0)


def mm(a, b):
    return jnp.dot(a, b, preferred_element_type=f32)


def mm_nt(a, b):
    return lax.dot_general(a, b, (((1,), (1,)), ((), ())), preferred_element_type=f32)


def mm_tn(a, b):
    return lax.dot_general(a, b, (((0,), (0,)), ((), ())), preferred_element_type=f32)


def sigmoid(v):
    return 0.5 * jnp.tanh(0.5 * v) + 0.5


def silu(v):
    return v * sigmoid(v)


def silu_slope(v):
    s = sigmoid(v)
    return s * (1.0 + v * (1.0 - s))


def high_low(v):
    high = v.astype(bf16)
    return high, (v - high.astype(f32)).astype(bf16)


class Total:
    AXES = "kxyz"

    @staticmethod
    def scratch(X, Y, Z):
        many = 1 + X - 1 + Y - 1 + Z - 1
        return [pltpu.VMEM((n, 8, 128), f32) for n in (2, X, Y, Z)] + [
            pltpu.VMEM((8, 128), f32),
            pltpu.SemaphoreType.DMA((many,)),
            pltpu.SemaphoreType.DMA((many,)),
        ]

    def __init__(self, place, refs):
        self.p, self.bufs, (self.value, self.ss, self.rs) = place, dict(zip("kxyz", refs[:4])), refs[4:]

    def _copies(self, axis):
        p, buf = self.p, self.bufs[axis]
        base = sum(getattr(p, a.upper()) - 1 for a in self.AXES[: self.AXES.index(axis)])
        here = buf.at[getattr(p, axis)]
        for d in range(1, getattr(p, axis.upper())):
            i = base + d - 1
            yield remote(here, here, self.ss.at[i], self.rs.at[i], p.peer(axis, d))

    def start(self, axis):
        self.bufs[axis][getattr(self.p, axis)] = self.value[...]
        for copy in self._copies(axis):
            copy.start()

    def finish(self, axis):
        for copy in self._copies(axis):
            copy.wait_recv()
        buf = self.bufs[axis]
        value = buf[0]
        for i in range(1, getattr(self.p, axis.upper())):
            value = value + buf[i]
        self.value[...] = value

    def drain(self, axes):
        for axis in axes:
            for copy in self._copies(axis):
                copy.wait_send()


class Reduce:
    def __init__(self, grid, dim, n_col, width, late):
        self.X, self.Y, self.Z = grid
        self.dim, self.shard, self.late = dim, dim // n_col, late
        self.ry = self.shard // self.Y
        self.zr = min(self.ry // 16, self.Z)
        self.zl = self.Z // self.zr
        self.rz = self.ry // self.zr
        self.w = -(-width // (128 * self.zl)) * 128 * self.zl
        self.wz = self.w // self.zl

    def scratch(self):
        X, Y, Z, w = self.X, self.Y, self.Z, self.w
        many = X + (X - 1) + 2 * (Y - 1) + 2 * (Z - 1)
        return [
            pltpu.VMEM((self.dim, w), f32),
            pltpu.VMEM((X, self.shard, w), f32),
            pltpu.VMEM((X - 1, self.shard, w), bf16),
            pltpu.VMEM((X - 1, self.shard, w), bf16),
            pltpu.VMEM((Y - 1, self.ry, w), bf16),
            pltpu.VMEM((Y - 1, self.ry, w), bf16),
            pltpu.VMEM((Z - 1, self.rz, self.wz), self.late),
            pltpu.VMEM((Z - 1, self.rz, self.wz), self.late),
            pltpu.VMEM((self.rz, self.wz), f32),
            pltpu.VMEM((self.shard, w), self.late),
            pltpu.SemaphoreType.DMA((many,)),
            pltpu.SemaphoreType.DMA((many,)),
        ]

    def bind(self, place, refs):
        (self.full, self.cr, self.xs, self.xr, self.ys, self.yr, self.zs, self.zin, self.piece, self.out, self.ss, self.rs) = refs
        self.p = place
        self.copies = []

    def rows_of(self, x, k):
        return (2 * x + k) * self.shard

    def piece_at(self, z):
        rows = pl.multiple_of((z // self.zl) * self.rz, 16)
        if self.zl == 1:
            return rows, pl.ds(0, self.wz)
        return rows, pl.ds(pl.multiple_of((z % self.zl) * self.wz, 128), self.wz)

    def _send(self, i, src, dst, device):
        copy = remote(src, dst, self.ss.at[i], self.rs.at[i], device)
        copy.start()
        self.copies.append(copy)
        return copy

    def stage(self, s):
        p, X, Y, Z = self.p, self.X, self.Y, self.Z
        if s == 0:
            self.core = [
                self._send(x, self.full.at[ds(self.rows_of(x, 1 - p.k), self.shard), :], self.cr.at[x], p.peer("k", 1))
                for x in range(X)
            ]
        elif s == 1:
            for copy in self.core:
                copy.wait_recv()
            self.xc = []
            for d in range(1, X):
                to = p.to("x", d)

                def one(at, to=to, d=d):
                    mine = self.full[pl.ds(pl.multiple_of(self.rows_of(to, p.k) + at, 16), 16), :]
                    self.xs[d - 1, pl.ds(at, 16), :] = (mine + self.cr[to, pl.ds(at, 16), :]).astype(bf16)

                by_rows(self.shard, 16, one)
                self.xc.append(self._send(X + d - 1, self.xs.at[d - 1], self.xr.at[d - 1], p.peer("x", d)))
        elif s == 2:
            for copy in self.xc:
                copy.wait_recv()

            def total(at, n=16):
                value = self.full[pl.ds(pl.multiple_of(self.rows_of(p.x, p.k) + at, 16), n), :]
                value = value + self.cr[p.x, pl.ds(at, n), :]
                for d in range(1, X):
                    value = value + self.xr[d - 1, pl.ds(at, n), :].astype(f32)
                return value

            self.yc = []
            for d in range(1, Y):
                base = p.to("y", d) * self.ry

                def one(at, base=base, d=d):
                    self.ys[d - 1, pl.ds(at, 16), :] = total(pl.multiple_of(base + at, 16)).astype(bf16)

                by_rows(self.ry, 16, one)
                self.yc.append(self._send(2 * X - 2 + d, self.ys.at[d - 1], self.yr.at[d - 1], p.peer("y", d)))

            def mine(at):
                at = pl.multiple_of(p.y * self.ry + at, 16)
                self.cr[p.x, pl.ds(at, 16), :] = total(at)

            by_rows(self.ry, 16, mine)
        elif s == 3:
            for copy in self.yc:
                copy.wait_recv()

            def total(z):
                rows, lanes = self.piece_at(z)
                value = self.cr[p.x, pl.ds(pl.multiple_of(p.y * self.ry + rows, 16), self.rz), lanes]
                for d in range(1, Y):
                    value = value + self.yr[d - 1, pl.ds(rows, self.rz), lanes].astype(f32)
                return value

            self.zc = []
            base = 2 * X - 1 + Y - 1
            for d in range(1, Z):
                self.zs[d - 1] = total(p.to("z", d)).astype(self.late)
                self.zc.append(self._send(base + d - 1, self.zs.at[d - 1], self.zin.at[d - 1], p.peer("z", d)))
            self.piece[...] = total(p.z)
        elif s == 4:
            for copy in self.zc:
                copy.wait_recv()
            value = self.piece[...]
            for d in range(1, Z):
                value = value + self.zin[d - 1].astype(f32)
            self.piece[...] = value
            rows, lanes = self.piece_at(p.z)
            here = self.out.at[pl.ds(pl.multiple_of(p.y * self.ry + rows, 16), self.rz), lanes]
            here[...] = value.astype(self.late)
            base = 2 * X - 1 + Y - 1 + Z - 1
            self.gz = [self._send(base + d - 1, here, here, p.peer("z", d)) for d in range(1, Z)]
        elif s == 5:
            for copy in self.gz:
                copy.wait_recv()
            here = self.out.at[pl.ds(pl.multiple_of(p.y * self.ry, 16), self.ry), :]
            base = 2 * X - 1 + Y - 1 + 2 * (Z - 1)
            self.gy = [self._send(base + d - 1, here, here, p.peer("y", d)) for d in range(1, Y)]
        elif s == 6:
            for copy in self.gy:
                copy.wait_recv()

    def drain(self):
        for copy in self.copies:
            copy.wait_send()


STAGES = 7


class Step:
    def __init__(self, mesh, samples, slots, dim, edges, c_in):
        self.n_row, self.n_col = mesh.shape["row"], mesh.shape["col"]
        self.grid = sizes_of(self.n_row, self.n_col)
        self.S, self.C, self.D, self.E, self.c_in = samples, slots, dim, edges, c_in
        self.N = MESH_DEV
        self.SH = dim // self.n_col
        self.R, self.Q = self.n_row * self.N, self.n_col * self.N
        chunk = lambda width, late: Reduce(self.grid, dim, self.n_col, width, late)
        self.chunks = [
            chunk(dim + N_OUT, f32),
            chunk(2 * dim, bf16),
            chunk(2 * dim, bf16),
            chunk(dim, bf16),
            chunk(N_IN, f32),
        ]
        X, Y, Z = self.grid
        S, C, D, E, N, R, Q = self.S, self.C, self.D, self.E, self.N, self.R, self.Q
        vm = pltpu.VMEM
        dma = lambda *shape: pltpu.SemaphoreType.DMA(shape)
        self.shapes = dict(
            wib=vm((D, N_IN), bf16),
            wlb=vm((6, D, D), bf16),
            wob=vm((D, N_OUT), bf16),
            nm=vm((N, C), bf16),
            nv=vm((N, C), bf16),
            cm=vm((C, N), bf16),
            cmv=vm((C, N), bf16),
            cw=vm((C, 128), f32),
            cnt=vm((N, 128), f32),
            fp=vm((S * C, D), f32),
            gl=vm((S * C, D), bf16),
            tp=vm((S * C, D), f32),
            go=vm((S * C, D), bf16),
            dp=vm((S * C, N_OUT), bf16),
            dt=vm((S * C, D), bf16),
            av=vm((S * N, D), bf16),
            sp=vm((S * N, D), f32),
            mlb=vm((S * N, D), bf16),
            agb=vm((S * N, D), bf16),
            mnb=vm((S * N, D), bf16),
            sg=vm((S * N, D), f32),
            dmn=vm((S * N, D), f32),
            dsb=vm((S * N, D), bf16),
            drb=vm((S * N, D), bf16),
            d2b=vm((S * N, D), bf16),
            sr=vm((S, R + Q, D), bf16),
            oh=vm((E, R + Q), bf16),
            oht=vm((R + Q, E), bf16),
            ep=vm((S, E, D), f32),
            ac=vm((E, D), bf16),
            tmp=vm((R + Q, D), f32),
            part=vm((S, Q, D), f32),
            pcr=vm((S, X, N, D), f32),
            pxs=vm((S, X - 1, N, D), bf16),
            pxr=vm((S, X - 1, N, D), bf16),
            da=vm((S, Q, D), bf16),
            down=vm((S, Z, N, D), f32),
            dys=vm((S, Y - 1, Z, N, D), bf16),
            dyr=vm((S, Y - 1, Z, N, D), bf16),
            dzs=vm((S, Z - 1, N, D), bf16),
            dzr=vm((S, Z - 1, N, D), bf16),
            loss=vm((8, 128), f32),
            l_sem=dma(24),
            w_ss=dma(8, 1 + 2 * (X - 1)),
            w_rs=dma(8, 1 + 2 * (X - 1)),
            mz_ss=dma(S, Z - 1),
            mz_rs=dma(S, Z - 1),
            my_ss=dma(S, Y - 1, Z),
            my_rs=dma(S, Y - 1, Z),
            mr_ss=dma(S, 1 + 2 * (X - 1)),
            mr_rs=dma(S, 1 + 2 * (X - 1)),
            pk_ss=dma(2, S, X),
            pk_rs=dma(2, S, X),
            px_ss=dma(2, S, X - 1),
            px_rs=dma(2, S, X - 1),
            a_ss=dma(S, 1 + 2 * (X - 1)),
            a_rs=dma(S, 1 + 2 * (X - 1)),
            dy_ss=dma(S, Y - 1),
            dy_rs=dma(S, Y - 1),
            dz_ss=dma(S, Z - 1),
            dz_rs=dma(S, Z - 1),
        )

    def vmem_bytes(self):
        total = 0
        for s in [*self.shapes.values(), *[s for c in self.chunks for s in c.scratch()]]:
            dtype = getattr(s, "dtype", None)
            if dtype in (jnp.dtype(f32), jnp.dtype(bf16)):
                size = jnp.dtype(dtype).itemsize
                for n in s.shape[:-1]:
                    size *= n
                total += size * -(-s.shape[-1] // 128) * 128
        return total

    def scratch(self):
        total = Total.scratch(*self.grid)
        return [*self.shapes.values(), *total * 3, *[s for c in self.chunks for s in c.scratch()]]

    def kernel(self, count, x, tgt, area, node, snd, rcv, wi, wl, wo, mi, mal, mo, si, sal, so, *refs):
        S, C, D, E, N, R, Q, SH = self.S, self.C, self.D, self.E, self.N, self.R, self.Q, self.SH
        X, Y, Z = self.grid
        (g_in, g_out, g_skip, g_two, g_three, g_four, stats), refs = refs[:7], refs[7:]
        v = types.SimpleNamespace(**dict(zip(self.shapes, refs)))
        refs = refs[len(self.shapes) :]
        p = Place(self.n_row, self.n_col)
        area_sum, loss_sum, norm_sum = (Total(p, refs[i : i + 7]) for i in (0, 7, 14))
        refs = refs[21:]
        for chunk in self.chunks:
            many = len(chunk.scratch())
            chunk.bind(p, refs[:many])
            refs = refs[many:]

        def weight_rows(i, col):
            which = WIRE[i]
            whole = v.wib if which == "in" else v.wob if which == "out" else v.wlb.at[which]
            return whole.at[ds(col * SH, SH), :]

        def w_copy(i, j, d=0):
            rows = weight_rows(i, 2 * p.to("x", -d) + p.k if j == 2 else p.col)
            at = (0, d, X - 1 + d)[j]
            device = p.peer("x", d) if j == 1 else p.peer("k", 1)
            return remote(rows, rows, v.w_ss.at[i, at], v.w_rs.at[i, at], device)

        hops = range(1, X)

        def w_forward(i):
            for d in hops:
                w_copy(i, 1, d).wait_recv()
                w_copy(i, 2, d).start()

        def w_get(i):
            w_copy(i, 0).wait_recv()
            for d in hops:
                w_copy(i, 2, d).wait_recv()

        W = lambda which: v.wlb[which]
        own = ds(p.col * SH, SH)

        def turned(ref, n):
            v.tmp[0:n, 0:SH] = jnp.zeros((n, SH), f32)
            v.tmp[0 : ref.shape[0], 0:SH] = ref[...]
            return jnp.transpose(v.tmp[0:n, 0:SH])

        v.wib[own, :] = turned(wi, N_IN).astype(bf16)
        loads = [pltpu.make_async_copy(wl.at[m], v.fp.at[m * SH : (m + 1) * SH, :], v.l_sem.at[m]) for m in range(6)]
        for load in loads:
            load.start()
        for m, load in enumerate(loads):
            load.wait()
            v.wlb[m, own, :] = v.fp[m * SH : (m + 1) * SH, :].astype(bf16)
        v.wob[own, :] = turned(wo, N_OUT).astype(bf16)
        p.barrier()
        for i in range(8):
            w_copy(i, 0).start()
            for d in hops:
                w_copy(i, 1, d).start()

        used = count[0]
        node_row = node[...].reshape(1, C)
        match = (lax.broadcasted_iota(jnp.int32, (N, C), 0) == node_row).astype(f32)
        v.nm[...] = match.astype(bf16)
        match = match * (lax.broadcasted_iota(jnp.int32, (N, C), 1) < used).astype(f32)
        v.nv[...] = match.astype(bf16)
        v.cnt[...] = jnp.broadcast_to(jnp.maximum(jnp.sum(match, axis=1, keepdims=True), 1.0), (N, 128))
        node_col = jnp.transpose(jnp.broadcast_to(node_row, (128, C)))
        area_row = area[...].reshape(1, C) * (lax.broadcasted_iota(jnp.int32, (1, C), 1) < used).astype(f32)
        v.cw[...] = jnp.transpose(jnp.broadcast_to(area_row, (128, C)))
        match = (lax.broadcasted_iota(jnp.int32, (C, 128), 1) == node_col).astype(f32)
        v.cm[...] = match[:, :N].astype(bf16)
        match = match * (lax.broadcasted_iota(jnp.int32, (C, 128), 0) < used).astype(f32)
        v.cmv[...] = match[:, :N].astype(bf16)
        area_sum.value[...] = jnp.broadcast_to(jnp.sum(area_row), (8, 128))
        area_sum.start("k")

        w_forward(0)
        w_get(0)

        def encode(s, carry):
            at = ds(s * C, C)
            pre = mm_nt(x[s], v.wib[:, : self.c_in])
            v.fp[at, :] = pre
            v.gl[at, :] = silu(pre).astype(bf16)
            here = ds(s * N, N)
            v.av[here, :] = (mm(v.nv[...], v.gl[at, :]) / v.cnt[:, 0:1]).astype(bf16)
            return carry

        lax.fori_loop(0, S, encode, 0)
        area_sum.finish("k")
        area_sum.start("x")
        w_forward(1)
        w_get(1)
        pre = mm(v.av[...], W(0))
        v.sp[...] = pre
        v.mlb[...] = silu(pre).astype(bf16)
        w_forward(2)
        w_get(2)
        v.tmp[0 : S * N, :] = mm(v.mlb[...], W(1))
        for s in range(S):
            v.sr[s, ds(p.row * N, N), :] = v.tmp[s * N : (s + 1) * N, :].astype(bf16)
        w_forward(3)
        w_get(3)

        def mz(s, d):
            rows = v.sr.at[s, ds(p.row * N, N), :]
            return remote(rows, rows, v.mz_ss.at[s, d - 1], v.mz_rs.at[s, d - 1], p.peer("z", d))

        def my(s, d, e):
            rows = v.sr.at[s, ds((p.to("z", -e) * Y + p.y) * N, N), :]
            return remote(rows, rows, v.my_ss.at[s, d - 1, e], v.my_rs.at[s, d - 1, e], p.peer("y", d))

        def mr(s, j, d=0):
            col = 2 * p.to("x", -d) + p.k if j == 2 else p.col
            rows = v.sr.at[s, ds(R + col * N, N), :]
            at = (0, d, X - 1 + d)[j]
            return remote(rows, rows, v.mr_ss.at[s, at], v.mr_rs.at[s, at], p.peer("x", d) if j == 1 else p.peer("k", 1))

        for s in range(S):
            for d in range(1, Z):
                mz(s, d).start()
            for d in range(1, Y):
                my(s, d, 0).start()
        v.tmp[0 : S * N, :] = mm(v.mlb[...], W(2))
        for s in range(S):
            v.sr[s, ds(R + p.col * N, N), :] = v.tmp[s * N : (s + 1) * N, :].astype(bf16)
        for s in range(S):
            mr(s, 0).start()
            for d in hops:
                mr(s, 1, d).start()
        area_sum.finish("x")
        area_sum.start("y")

        def table(index, base, rows):
            def down(at):
                hit = lax.broadcasted_iota(jnp.int32, (128, E), 0) + at == index
                v.oht[pl.ds(pl.multiple_of(base + at, 128), 128), :] = hit.astype(f32).astype(bf16)

            by_rows(rows, 128, down)
            column = jnp.transpose(jnp.broadcast_to(index, (128, E)))
            for at in range(0, rows, 128):
                hit = lax.broadcasted_iota(jnp.int32, (E, 128), 1) + at == column
                v.oh[:, base + at : base + at + 128] = hit.astype(f32).astype(bf16)

        table(snd[...], 0, R)
        table(rcv[...], R, Q)

        w_forward(4)
        w_get(4)

        def skip(at):
            v.tp[pl.ds(at, 512), :] = mm(v.gl[pl.ds(at, 512), :], W(5))

        by_rows(S * C, 512, skip)
        area_sum.finish("y")
        area_sum.start("z")
        w_forward(5)

        def pk(t, s, xx):
            rows = v.part.at[s, ds((2 * xx + 1 - p.k) * N, N), :]
            return remote(rows, v.pcr.at[s, xx], v.pk_ss.at[t, s, xx], v.pk_rs.at[t, s, xx], p.peer("k", 1))

        def px(t, s, d):
            return remote(v.pxs.at[s, d - 1], v.pxr.at[s, d - 1], v.px_ss.at[t, s, d - 1], v.px_rs.at[t, s, d - 1], p.peer("x", d))

        def col_second(t, s):
            for xx in range(X):
                pk(t, s, xx).wait_recv()
            for d in hops:
                px_to = p.to("x", d)
                mine = v.part[s, ds((2 * px_to + p.k) * N, N), :]
                v.pxs[s, d - 1] = (mine + v.pcr[s, px_to]).astype(bf16)
                px(t, s, d).start()

        def col_last(t, s):
            total = v.part[s, ds(p.col * N, N), :] + v.pcr[s, p.x]
            for d in hops:
                px(t, s, d).wait_recv()
                total = total + v.pxr[s, d - 1].astype(f32)
            return total

        def arrive(s):
            for d in range(1, Z):
                mz(s, d).wait_recv()
                for b in range(1, Y):
                    my(s, b, d).start()
            for d in hops:
                mr(s, 1, d).wait_recv()
                mr(s, 2, d).start()

        def edges(s):
            for b in range(1, Y):
                for e in range(Z):
                    my(s, b, e).wait_recv()
            mr(s, 0).wait_recv()
            for d in hops:
                mr(s, 2, d).wait_recv()

            def pick(at):
                pre = mm(v.oh[pl.ds(at, 512), :], v.sr[s])
                v.ep[s, pl.ds(at, 512), :] = pre
                v.ac[pl.ds(at, 512), :] = silu(pre).astype(bf16)

            by_rows(E, 512, pick)
            v.part[s] = mm(v.oht[R:, :], v.ac[...])
            for xx in range(X):
                pk(0, s, xx).start()

        def forward(i, carry):
            @pl.when(i < S)
            def _():
                arrive(i)

            @pl.when((i >= 1) & (i <= S))
            def _():
                edges(i - 1)

            @pl.when(i >= 2)
            def _():
                col_second(0, i - 2)

            return carry

        lax.fori_loop(0, S + 2, forward, 0)
        area_sum.finish("z")
        w_get(5)
        for i in (6, 7):
            w_forward(i)
        for s in range(S):
            v.agb[s * N : (s + 1) * N, :] = (col_last(0, s) * (1.0 / DEG)).astype(bf16)

        v.mnb[...] = (silu(v.sp[...]) + mm(v.agb[...], W(3))).astype(bf16)
        w_get(6)
        w_get(7)
        v.dp[...] = jnp.zeros((S * C, N_OUT), bf16)
        v.loss[...] = jnp.zeros((8, 128), f32)
        scale = 1.0 / (C_OUT * S * area_sum.value[0:1, 0:1])

        def decode(s, carry):
            at, here = ds(s * C, C), ds(s * N, N)
            rows = mm(v.cm[...], v.mnb[here, :]).astype(bf16)
            pre = mm(rows, W(4)) + v.tp[at, :]
            v.tp[at, :] = pre
            v.go[at, :] = silu(pre).astype(bf16)
            error = mm(v.go[at, :], v.wob[...])[:, :C_OUT] - tgt[s].astype(f32)
            weighted = v.cw[:, :C_OUT] * error
            v.loss[0:1, 0:C_OUT] = v.loss[0:1, 0:C_OUT] + jnp.sum(weighted * error, axis=0, keepdims=True)
            v.dp[at, 0:C_OUT] = (2.0 * weighted * scale).astype(bf16)
            v.dt[at, :] = (silu_slope(v.tp[at, :]) * mm_nt(v.dp[at, :], v.wob[...])).astype(bf16)
            v.sg[here, :] = mm(v.nm[...], v.dt[at, :])
            return carry

        lax.fori_loop(0, S, decode, 0)
        high, low = high_low(v.sg[...])
        v.dmn[...] = mm_nt(high, W(4)) + mm_nt(low, W(4))
        v.tmp[0 : S * N, :] = mm_nt(v.dmn[...].astype(bf16), W(3))
        for s in range(S):
            v.da[s, ds(p.col * N, N), :] = v.tmp[s * N : (s + 1) * N, :].astype(bf16)

        def ac(s, j, d=0):
            col = 2 * p.to("x", -d) + p.k if j == 2 else p.col
            rows = v.da.at[s, ds(col * N, N), :]
            at = (0, d, X - 1 + d)[j]
            return remote(rows, rows, v.a_ss.at[s, at], v.a_rs.at[s, at], p.peer("x", d) if j == 1 else p.peer("k", 1))

        for s in range(S):
            ac(s, 0).start()
            for d in hops:
                ac(s, 1, d).start()
        loss_sum.value[...] = jnp.broadcast_to(jnp.sum(v.loss[...]), (8, 128))
        loss_sum.start("k")

        first, second, third, fourth, fifth = self.chunks
        first.full[:, 0:D] = mm_tn(v.gl[...], v.dt[...])
        first.full[:, D : D + N_OUT] = mm_tn(v.go[...], v.dp[...])
        first.stage(0)
        high, low = high_low(v.sg[...])
        second.full[:, 0:D] = mm_tn(v.mnb[...], high) + mm_tn(v.mnb[...], low)
        second.full[:, D : 2 * D] = mm_tn(v.agb[...], v.dmn[...].astype(bf16))
        second.stage(0)

        def skip_back(at):
            v.tp[pl.ds(at, 512), :] = mm_nt(v.dt[pl.ds(at, 512), :], W(5))

        by_rows(S * C, 512, skip_back)
        loss_sum.finish("k")
        loss_sum.start("x")
        first.stage(1)
        second.stage(1)

        def dy(s, d):
            return remote(v.dys.at[s, d - 1], v.dyr.at[s, d - 1], v.dy_ss.at[s, d - 1], v.dy_rs.at[s, d - 1], p.peer("y", d))

        def dz(s, d):
            return remote(v.dzs.at[s, d - 1], v.dzr.at[s, d - 1], v.dz_ss.at[s, d - 1], v.dz_rs.at[s, d - 1], p.peer("z", d))

        def pass_on(s):
            for d in hops:
                ac(s, 1, d).wait_recv()
                ac(s, 2, d).start()

        def edges_back(s):
            ac(s, 0).wait_recv()
            for d in hops:
                ac(s, 2, d).wait_recv()

            def pick(at):
                grad = mm(v.oh[pl.ds(at, 512), R:], v.da[s])
                v.ac[pl.ds(at, 512), :] = (silu_slope(v.ep[s, pl.ds(at, 512), :]) * grad * (1.0 / DEG)).astype(bf16)

            by_rows(E, 512, pick)
            v.tmp[...] = mm(v.oht[...], v.ac[...])
            for d in range(1, Y):
                for e in range(Z):
                    v.dys[s, d - 1, e] = v.tmp[ds((e * Y + p.to("y", d)) * N, N), :].astype(bf16)
                dy(s, d).start()
            for e in range(Z):
                v.down[s, e] = v.tmp[ds((e * Y + p.y) * N, N), :]
            v.part[s] = v.tmp[R:, :]
            for xx in range(X):
                pk(1, s, xx).start()

        def row_second(s):
            for d in range(1, Y):
                dy(s, d).wait_recv()

            def summed(e):
                total = v.down[s, e]
                for d in range(1, Y):
                    total = total + v.dyr[s, d - 1, e].astype(f32)
                return total

            for d in range(1, Z):
                v.dzs[s, d - 1] = summed(p.to("z", d)).astype(bf16)
                dz(s, d).start()
            v.down[s, p.z] = summed(p.z)

        for s in range(S):
            for xx in range(X):
                pk(0, s, xx).wait_send()
            for d in hops:
                px(0, s, d).wait_send()

        def backward(i, carry):
            @pl.when(i < S)
            def _():
                pass_on(i)
                edges_back(i)

            @pl.when(i >= 1)
            def _():
                col_second(1, i - 1)
                row_second(i - 1)

            return carry

        lax.fori_loop(0, S + 1, backward, 0)
        states = [
            pltpu.make_async_copy(a.at[m], v.ep.at[j, m * SH : (m + 1) * SH, :], v.l_sem.at[6 + 6 * j + m])
            for j, a in enumerate((wl, mal, sal))
            for m in range(6)
        ]
        for load in states:
            load.start()
        first.stage(2)
        second.stage(2)
        for s in range(S):
            v.drb[s * N : (s + 1) * N, :] = col_last(1, s).astype(bf16)
        for s in range(S):
            total = v.down[s, p.z]
            for d in range(1, Z):
                dz(s, d).wait_recv()
                total = total + v.dzr[s, d - 1].astype(f32)
            v.dsb[s * N : (s + 1) * N, :] = total.astype(bf16)

        third.full[:, 0:D] = mm_tn(v.mlb[...], v.dsb[...])
        third.full[:, D : 2 * D] = mm_tn(v.mlb[...], v.drb[...])
        third.stage(0)
        whole = v.dmn[...] + mm_nt(v.dsb[...], W(1)) + mm_nt(v.drb[...], W(2))
        v.d2b[...] = (silu_slope(v.sp[...]) * whole).astype(bf16)
        third.stage(1)
        fourth.full[...] = mm_tn(v.av[...], v.d2b[...])
        fourth.stage(0)
        v.dmn[...] = mm_nt(v.d2b[...], W(0))
        first.stage(3)
        second.stage(3)

        def encode_back(s, carry):
            at, here = ds(s * C, C), ds(s * N, N)
            high, low = high_low(v.dmn[here, :] / v.cnt[:, 0:1])
            grad = v.tp[at, :] + mm(v.cmv[...], high) + mm(v.cmv[...], low)
            v.dt[at, :] = (silu_slope(v.fp[at, :]) * grad).astype(bf16)
            return carry

        lax.fori_loop(0, S, encode_back, 0)
        third.stage(2)
        fourth.stage(1)
        fifth.full[:, self.c_in :] = jnp.zeros((D, N_IN - self.c_in), f32)
        for s in range(S):
            grad = mm_tn(v.dt[s * C : (s + 1) * C, :], x[s])
            if s:
                grad = grad + fifth.full[:, : self.c_in]
            fifth.full[:, : self.c_in] = grad
        fifth.stage(0)
        first.stage(4)
        second.stage(4)
        loss_sum.finish("x")
        loss_sum.start("y")
        third.stage(3)
        fourth.stage(2)
        fifth.stage(1)
        first.stage(5)
        second.stage(5)
        third.stage(4)
        fourth.stage(3)
        fifth.stage(2)
        loss_sum.finish("y")
        loss_sum.start("z")
        for load in states:
            load.wait()
        lane = lax.broadcasted_iota(jnp.int32, (8, 128), 1)
        row = lax.broadcasted_iota(jnp.int32, (8, 128), 0)
        norm_sum.value[...] = jnp.zeros((8, 128), f32)

        def note(j, weight, gradient, mean, square):
            _, _, update = adam_parts(weight, gradient, mean, square)
            for i, what in enumerate((weight, update)):
                norm_sum.value[...] += jnp.where((row == i) & (lane == j), jnp.sum(what * what), 0.0)

        def note_latent(m, gradient):
            weight, mean, square = (v.ep[j, m * SH : (m + 1) * SH, :] for j in range(3))
            note(1 + m, weight, gradient.astype(f32), mean, square)

        first.stage(6)
        g_skip[...] = first.out[:, :D]
        g_out[...] = jnp.transpose(first.out[:, D : D + N_OUT])[: g_out.shape[0], :]
        second.stage(6)
        g_two[...] = second.out[:, : 2 * D]
        third.stage(5)
        fourth.stage(4)
        fifth.stage(3)
        note_latent(5, first.out[:, :D])
        note(7, wo[...], g_out[...], mo[...], so[...])
        note_latent(4, second.out[:, 0:D])
        note_latent(3, second.out[:, D : 2 * D])
        third.stage(6)
        g_three[...] = third.out[:, : 2 * D]
        fourth.stage(5)
        fifth.stage(4)
        note_latent(1, third.out[:, 0:D])
        note_latent(2, third.out[:, D : 2 * D])
        fourth.stage(6)
        g_four[...] = fourth.out[:, :D]
        fifth.stage(5)
        note_latent(0, fourth.out[:, :D])
        loss_sum.finish("z")
        fifth.stage(6)
        g_in[...] = jnp.transpose(fifth.out[:, :N_IN])[: g_in.shape[0], :]
        note(0, wi[...], g_in[...], mi[...], si[...])
        norm_sum.start("k")
        norm_sum.finish("k")
        norm_sum.start("x")
        norm_sum.finish("x")
        stats[...] = jnp.where(row < 2, norm_sum.value[...], loss_sum.value[...] / (C_OUT * S * area_sum.value[...]))

        for i in range(8):
            w_copy(i, 0).wait_send()
            for d in hops:
                w_copy(i, 1, d).wait_send()
                w_copy(i, 2, d).wait_send()
        for s in range(S):
            for d in range(1, Z):
                mz(s, d).wait_send()
                dz(s, d).wait_send()
            for d in range(1, Y):
                for e in range(Z):
                    my(s, d, e).wait_send()
                dy(s, d).wait_send()
            for copy in (mr, ac):
                copy(s, 0).wait_send()
                for d in hops:
                    copy(s, 1, d).wait_send()
                    copy(s, 2, d).wait_send()
            for xx in range(X):
                pk(1, s, xx).wait_send()
            for d in hops:
                px(1, s, d).wait_send()
        area_sum.drain("kxyz")
        loss_sum.drain("kxyz")
        norm_sum.drain("kx")
        for chunk in self.chunks:
            chunk.drain()

    def __call__(self, count, x, tgt, area, node, snd, rcv, *states):
        vm, hbm = pl.BlockSpec(memory_space=pltpu.VMEM), pl.BlockSpec(memory_space=pl.ANY)
        D, SH = self.D, self.SH
        outs = [(states[0].shape, f32), (states[2].shape, f32), ((SH, D), f32), ((SH, 2 * D), bf16), ((SH, 2 * D), bf16), ((SH, D), bf16), ((8, 128), f32)]
        return pl.pallas_call(
            self.kernel,
            out_shape=[jax.ShapeDtypeStruct(*o) for o in outs],
            in_specs=[pl.BlockSpec(memory_space=pltpu.SMEM)] + [vm] * 6 + [vm, hbm, vm] * 3,
            out_specs=[vm] * 7,
            scratch_shapes=self.scratch(),
            name="train_step",
            compiler_params=pltpu.CompilerParams(collective_id=0, has_side_effects=True, vmem_limit_bytes=67043328),
        )(count, x, tgt, area, node, snd, rcv, *states)


def update_kernel(g_in, g_out, g_skip, g_two, g_three, g_four, stats, wi, wl, wo, mi, mal, mo, si, sal, so, *refs):
    loss, *outs, norms = refs[:17]
    in_buf, out_buf, low_buf, in_sem, out_sem = refs[17:]
    SH, D = g_skip.shape
    loads = [[pltpu.make_async_copy(a.at[m], in_buf.at[j, m], in_sem.at[j, m]) for j, a in enumerate((wl, mal, sal))] for m in range(6)]
    order = (5, 4, 3, 2, 1, 0)
    for m in order:
        for load in loads[m]:
            load.start()
    root = jnp.sqrt(stats[...])
    norms[...] = root[0:2, 0:8]
    loss[...] = stats[2:3, 0:1]

    def step(j, weight, gradient, mean, square):
        first, second, update = adam_parts(weight, gradient, mean, square)
        ratio = root[0:1, j : j + 1] / (root[1:2, j : j + 1] + trust_epsilon)
        master = weight - learn_rate * ratio * update
        return gradient, first, second, master, master.astype(bf16)

    grads = {5: (g_skip, 0), 4: (g_two, 0), 3: (g_two, D), 2: (g_three, D), 1: (g_three, 0), 0: (g_four, 0)}
    stores = []
    for m in order:
        for load in loads[m]:
            load.wait()
        ref, at = grads[m]
        results = step(1 + m, in_buf[0, m], ref[:, at : at + D].astype(f32), in_buf[1, m], in_buf[2, m])
        for j, result in enumerate(results):
            buf = low_buf.at[m] if j == 4 else out_buf.at[j, m]
            buf[...] = result
            stores.append(pltpu.make_async_copy(buf, outs[3 * j + 1].at[m], out_sem.at[j, m]))
            stores[-1].start()
    for j, result in enumerate(step(0, wi[...], g_in[...], mi[...], si[...])):
        outs[3 * j][...] = result
    for j, result in enumerate(step(7, wo[...], g_out[...], mo[...], so[...])):
        outs[3 * j + 2][...] = result
    for store in stores:
        store.wait()


def update_all(grads, states):
    vm, hbm = pl.BlockSpec(memory_space=pltpu.VMEM), pl.BlockSpec(memory_space=pl.ANY)
    kinds = [f32] * 4 + [bf16]
    shapes = [states[0].shape, states[1].shape, states[2].shape]
    n, SH, D = states[1].shape
    return pl.pallas_call(
        update_kernel,
        out_shape=[jax.ShapeDtypeStruct((1, 1), f32)]
        + [jax.ShapeDtypeStruct(s, k) for k in kinds for s in shapes]
        + [jax.ShapeDtypeStruct((2, 8), f32)],
        in_specs=[vm] * 7 + [vm, hbm, vm] * 3,
        out_specs=[vm] + [vm, hbm, vm] * 5 + [vm],
        scratch_shapes=[
            pltpu.VMEM((3, n, SH, D), f32),
            pltpu.VMEM((4, n, SH, D), f32),
            pltpu.VMEM((n, SH, D), bf16),
            pltpu.SemaphoreType.DMA((3, n)),
            pltpu.SemaphoreType.DMA((5, n)),
        ],
        name="lamb",
        compiler_params=pltpu.CompilerParams(vmem_limit_bytes=67043328),
    )(*grads, *states)


def kernel_body(mesh, step, inputs, targets, cell_area, cell_count, cell_node, edge_senders, edge_receivers, *states):
    states = [a.T if i % 3 == 2 else a for i, a in enumerate(states)]
    grads = step(cell_count, inputs, targets, cell_area, cell_node, edge_senders[None, :], edge_receivers[None, :], *states)
    loss, *outs, norms = update_all(grads, states)
    outs = [a.T if i % 3 == 2 else a for i, a in enumerate(outs)]
    return (loss[0, 0], *outs, norms)


def native_gradients(
    inputs,
    targets,
    cell_area,
    cell_count,
    cell_node,
    edge_senders,
    edge_receivers,
    weight_input,
    weight_latent,
    weight_output,
):
    full_input, complete_latent, full_output = (
        lax.all_gather(weight_input.astype(jnp.bfloat16), "col", axis=1, tiled=True),
        lax.all_gather(weight_latent.astype(jnp.bfloat16), "col", axis=1, tiled=True),
        lax.all_gather(weight_output.astype(jnp.bfloat16), "col", axis=0, tiled=True),
    )
    samples = inputs.shape[0]
    slots = inputs.shape[1]
    valid = (jnp.arange(slots, dtype=jnp.int32) < cell_count[0]).astype(jnp.float32)
    cell_weight = cell_area * valid
    area_total = lax.psum(jnp.sum(cell_weight), ("row", "col"))
    first_pre = reduced_matmul("sci,id->scd", inputs, full_input)
    grid_latent = jax.nn.silu(first_pre).astype(jnp.bfloat16)
    node_match = (cell_node[None, :] == jnp.arange(MESH_DEV, dtype=jnp.int32)[:, None]).astype(
        jnp.float32
    )
    node_match_low = node_match.astype(jnp.bfloat16)
    cell_match = node_match_low.T
    node_valid = node_match * valid[None, :]
    node_sum = reduced_matmul("nc,scd->snd", node_valid.astype(jnp.bfloat16), grid_latent)
    node_lower_limit = jnp.maximum(jnp.sum(node_valid, axis=1), 1.0)
    node_average = node_sum / node_lower_limit[None, :, None]
    average_reduced = node_average.astype(jnp.bfloat16)
    second_activation_input = reduced_matmul("kaj,jz->kaz", average_reduced, complete_latent[0])
    mesh_latent = jax.nn.silu(second_activation_input)
    mesh_state_reduced = mesh_latent.astype(jnp.bfloat16)
    receiver_local_part = reduced_matmul("kaj,jz->kaz", mesh_state_reduced, complete_latent[2])
    receiver_block = lax.all_gather(receiver_local_part, "col", axis=1, tiled=True)
    sender_block = reduced_matmul(
        "kaj,jz->kaz",
        lax.all_gather(mesh_state_reduced, "row", axis=1, tiled=True),
        complete_latent[1],
    )
    receiver_rows = receiver_block.shape[1]
    sender_rows = sender_block.shape[1]
    sender_match = one_hot_table(edge_senders, sender_rows)
    receiver_match = one_hot_table(edge_receivers, receiver_rows)
    edge_pre = pick_rows(sender_match, sender_block) + pick_rows(receiver_match, receiver_block)
    partial_sums = add_into_rows(receiver_match, jax.nn.silu(edge_pre))
    message_total = lax.psum_scatter(partial_sums, "col", scatter_dimension=1, tiled=True) / DEG
    message_total_reduced = message_total.astype(jnp.bfloat16)
    residual_branch = reduced_matmul("kaj,jz->kaz", message_total_reduced, complete_latent[3])
    mesh_next = mesh_latent + residual_branch
    decode_rows = reduced_matmul("cn,snd->scd", cell_match, mesh_next.astype(jnp.bfloat16)).astype(
        jnp.bfloat16
    )
    third_pre = reduced_matmul("scd,de->sce", decode_rows, complete_latent[4]) + reduced_matmul(
        "scd,de->sce", grid_latent, complete_latent[5]
    )
    grid_out = jax.nn.silu(third_pre).astype(jnp.bfloat16)
    predict = reduced_matmul("scd,do->sco", grid_out, full_output)
    error = predict - targets.astype(jnp.float32)
    denominator = C_OUT * samples * area_total
    weighted = cell_weight[None, :, None] * error
    loss_value = lax.psum(jnp.sum(weighted * error), ("row", "col")) / denominator
    d_predict = (2.0 * weighted / denominator).astype(jnp.bfloat16)
    grad_output_local = reduced_matmul("scd,sco->do", grid_out, d_predict)
    d_grid_out = reduced_matmul("sco,do->scd", d_predict, full_output)
    d_third = silu_grad(third_pre, d_grid_out).astype(jnp.bfloat16)
    grad_decode = reduced_matmul("scd,sce->de", decode_rows, d_third)
    grad_skip = reduced_matmul("scd,sce->de", grid_latent, d_third)
    d_decode = reduced_matmul("sce,de->scd", d_third, complete_latent[4])
    d_skip = reduced_matmul("sce,de->scd", d_third, complete_latent[5])
    d_mesh_next = jnp.einsum("nc,scd->snd", node_match, d_decode, precision=highest)
    residual_branch_gradient = d_mesh_next.astype(jnp.bfloat16)
    branch_gradient_sum = reduced_matmul(
        "lhg,lhj->gj", message_total_reduced, residual_branch_gradient
    )
    message_total_gradient = reduced_matmul(
        "pyk,ck->pyc", residual_branch_gradient, complete_latent[3]
    ).astype(jnp.bfloat16)
    d_block = lax.all_gather(message_total_gradient, "col", axis=1, tiled=True)
    d_edge_message = reduced_matmul("es,ksd->ked", receiver_match, d_block)
    d_edge_pre = silu_grad(edge_pre, d_edge_message / DEG)
    d_sender_part = add_into_rows(sender_match, d_edge_pre)
    d_receiver_part = add_into_rows(receiver_match, d_edge_pre)
    sender_gradient = lax.psum_scatter(
        d_sender_part.astype(jnp.bfloat16), "row", scatter_dimension=1, tiled=True
    )
    receiver_gradient = lax.psum_scatter(
        d_receiver_part.astype(jnp.bfloat16), "col", scatter_dimension=1, tiled=True
    )
    sender_weight_gradient = reduced_matmul("lhg,lhj->gj", mesh_state_reduced, sender_gradient)
    receiver_weight_gradient = reduced_matmul("lhg,lhj->gj", mesh_state_reduced, receiver_gradient)
    d_mesh = (
        d_mesh_next
        + reduced_matmul("pyk,ck->pyc", sender_gradient, complete_latent[1])
        + reduced_matmul("pyk,ck->pyc", receiver_gradient, complete_latent[2])
    )
    hidden_second_gradient = silu_grad(second_activation_input, d_mesh).astype(jnp.bfloat16)
    encoder_gradient = reduced_matmul("lhg,lhj->gj", average_reduced, hidden_second_gradient)
    node_average_gradient = (
        reduced_matmul("pyk,ck->pyc", hidden_second_gradient, complete_latent[0])
        / node_lower_limit[None, :, None]
    )
    d_grid = d_skip + valid[None, :, None] * pick_rows(cell_match, node_average_gradient)
    d_first = silu_grad(first_pre, d_grid).astype(jnp.bfloat16)
    grad_input_local = reduced_matmul("sci,scd->id", inputs, d_first)
    grad_latent_local = jnp.stack(
        [
            encoder_gradient,
            sender_weight_gradient,
            receiver_weight_gradient,
            branch_gradient_sum,
            grad_decode,
            grad_skip,
        ]
    )
    local_terms = (grad_input_local, grad_latent_local, grad_output_local)
    whole_input, whole_latent, whole_output = lax.psum(
        (local_terms[0], local_terms[1], local_terms[2]), ("row", "col")
    )
    column = lax.axis_index("col")
    width_input = weight_input.shape[1]
    width_latent = weight_latent.shape[1]
    width_output = weight_output.shape[0]
    gradient_input = lax.dynamic_slice_in_dim(whole_input, column * width_input, width_input, 1)
    gradient_latent = lax.dynamic_slice_in_dim(whole_latent, column * width_latent, width_latent, 1)
    gradient_output = lax.dynamic_slice_in_dim(whole_output, column * width_output, width_output, 0)
    return loss_value, gradient_input, gradient_latent, gradient_output


def body(
    mesh,
    inputs,
    targets,
    cell_area,
    cell_count,
    cell_node,
    edge_senders,
    edge_receivers,
    weight_input,
    weight_latent,
    weight_output,
    mean_input,
    mean_latent,
    mean_output,
    square_input,
    square_latent,
    square_output,
):
    given = (inputs, targets, cell_area, cell_count, cell_node, edge_senders, edge_receivers, weight_input, weight_latent, weight_output)
    states = (mean_input, mean_latent, mean_output, square_input, square_latent, square_output)
    step = Step(mesh, inputs.shape[0], inputs.shape[1], weight_latent.shape[2], edge_senders.shape[0], inputs.shape[2])
    if step.vmem_bytes() < VMEM_ROOM:
        return kernel_body(mesh, step, *given, *states)
    loss_value, gradient_input, gradient_latent, gradient_output = native_gradients(*given)
    first_input, second_input, update_input = adam_parts(
        weight_input, gradient_input, mean_input, square_input
    )
    first_latent, second_latent, update_latent = adam_parts(
        weight_latent, gradient_latent, mean_latent, square_latent
    )
    first_output, second_output, update_output = adam_parts(
        weight_output, gradient_output, mean_output, square_output
    )
    weight_sums = jnp.concatenate(
        [
            jnp.sum(weight_input * weight_input)[None],
            jnp.sum(weight_latent * weight_latent, axis=(1, 2)),
            jnp.sum(weight_output * weight_output)[None],
        ]
    )
    update_sums = jnp.concatenate(
        [
            jnp.sum(update_input * update_input)[None],
            jnp.sum(update_latent * update_latent, axis=(1, 2)),
            jnp.sum(update_output * update_output)[None],
        ]
    )
    norm_sums = lax.psum(jnp.stack([weight_sums, update_sums]), "col")
    trust_norms = jnp.sqrt(norm_sums)
    ratio = trust_norms[0] / (trust_norms[1] + trust_epsilon)
    master_input = weight_input - learn_rate * ratio[0] * update_input
    master_latent = weight_latent - learn_rate * ratio[1:7][:, None, None] * update_latent
    master_output = weight_output - learn_rate * ratio[7] * update_output
    return (
        loss_value,
        gradient_input,
        gradient_latent,
        gradient_output,
        first_input,
        first_latent,
        first_output,
        second_input,
        second_latent,
        second_output,
        master_input,
        master_latent,
        master_output,
        master_input.astype(jnp.bfloat16),
        master_latent.astype(jnp.bfloat16),
        master_output.astype(jnp.bfloat16),
        trust_norms,
    )


def solution(mesh):
    placed = (
        P(None, ("row", "col"), None),
        P(None, ("row", "col"), None),
        P(("row", "col")),
        P(("row", "col")),
        P(("row", "col")),
        P(("row", "col")),
        P(("row", "col")),
        P(None, "col"),
        P(None, "col", None),
        P("col", None),
        P(None, "col"),
        P(None, "col", None),
        P("col", None),
        P(None, "col"),
        P(None, "col", None),
        P("col", None),
    )
    return jax.shard_map(
        functools.partial(body, mesh),
        mesh=mesh,
        in_specs=placed,
        out_specs=(
            P(),
            P(None, "col"),
            P(None, "col", None),
            P("col", None),
            P(None, "col"),
            P(None, "col", None),
            P("col", None),
            P(None, "col"),
            P(None, "col", None),
            P("col", None),
            P(None, "col"),
            P(None, "col", None),
            P("col", None),
            P(None, "col"),
            P(None, "col", None),
            P("col", None),
            P(),
        ),
        check_vma=False,
    )
```

```python
import functools
import types

import jax
import jax.numpy as jnp
from jax import lax
from jax.experimental import pallas as pl
from jax.experimental.pallas import tpu as pltpu
from jax.sharding import PartitionSpec as P

C_OUT = 83
DEG = 16
MESH_DEV = 64


highest = lax.Precision.HIGHEST
beta_first = 0.5
beta_second = 0.5
adam_epsilon = 1e-08
trust_epsilon = 1e-06
weight_decay = 0.01
learn_rate = 0.1


def silu_grad(pre_act, grad_out):
    sigma = jax.nn.sigmoid(pre_act)
    return grad_out * sigma * (1.0 + pre_act * (1.0 - sigma))


def reduced_matmul(form, left, right):
    return jnp.einsum(form, left, right, preferred_element_type=jnp.float32)


def split_parts(values):
    upper = values.astype(jnp.bfloat16)
    rest = values - upper.astype(jnp.float32)
    middle = rest.astype(jnp.bfloat16)
    lower = (rest - middle.astype(jnp.float32)).astype(jnp.bfloat16)
    return (upper, middle, lower)


def pick_rows(match, values):
    upper, middle, lower = split_parts(values)
    total = reduced_matmul("es,ksd->ked", match, upper)
    total = total + reduced_matmul("es,ksd->ked", match, middle)
    return total + reduced_matmul("es,ksd->ked", match, lower)


def add_into_rows(match, values):
    upper, middle, lower = split_parts(values)
    total = reduced_matmul("es,ked->ksd", match, upper)
    total = total + reduced_matmul("es,ked->ksd", match, middle)
    return total + reduced_matmul("es,ked->ksd", match, lower)


def one_hot_table(indices, count):
    return (indices[:, None] == jnp.arange(count, dtype=jnp.int32)[None, :]).astype(jnp.bfloat16)


def adam_parts(weight, gradient, first, second):
    new_first = beta_first * first + (1.0 - beta_first) * gradient
    new_second = beta_second * second + (1.0 - beta_second) * gradient * gradient
    update = new_first / (jnp.sqrt(new_second) + adam_epsilon) + weight_decay * weight
    return (new_first, new_second, update)


MESH = pl.DeviceIdType.MESH
bf16 = jnp.bfloat16
f32 = jnp.float32
VMEM_ROOM = 63 * 2**20
N_IN = 256
N_OUT = 128
WIRE = ("in", 0, 1, 2, 5, 3, 4, "out")


def sizes_of(n_row, n_col):
    X = n_col // 2
    Y = X if n_row % X == 0 else 1
    return X, Y, n_row // Y


class Place:
    def __init__(self, n_row, n_col):
        self.K = 2
        self.X, self.Y, self.Z = sizes_of(n_row, n_col)
        self.row, self.col = lax.axis_index("row"), lax.axis_index("col")
        self.z, self.y = self.row // self.Y, self.row % self.Y
        self.x, self.k = self.col // 2, self.col % 2

    def to(self, axis, d):
        n = getattr(self, axis.upper())
        return (getattr(self, axis) + d) % n

    def peer(self, axis, d):
        at = {a: getattr(self, a) for a in "zyxk"}
        at[axis] = self.to(axis, d)
        return (at["z"] * self.Y + at["y"], at["x"] * 2 + at["k"])

    def greet(self):
        sem = pltpu.get_barrier_semaphore()
        peers = [self.peer(a, d) for a in "kxyz" for d in range(1, getattr(self, a.upper()))]
        for peer in peers:
            pl.semaphore_signal(sem, inc=1, device_id=peer, device_id_type=MESH)
        return sem, len(peers)


def remote(src, dst, send_sem, recv_sem, device):
    return pltpu.make_async_remote_copy(
        src_ref=src,
        dst_ref=dst,
        send_sem=send_sem,
        recv_sem=recv_sem,
        device_id=device,
        device_id_type=MESH,
    )


def ds(start, size):
    if isinstance(start, int):
        return pl.ds(start, size)
    return pl.ds(pl.multiple_of(start, size if size % 128 else 128), size)


def by_rows(count, step, todo):
    def one(i, carry):
        todo(pl.multiple_of(i * step, step))
        return carry

    lax.fori_loop(0, count // step, one, 0)


def mm(a, b):
    return jnp.dot(a, b, preferred_element_type=f32)


def mm_nt(a, b):
    return lax.dot_general(a, b, (((1,), (1,)), ((), ())), preferred_element_type=f32)


def mm_tn(a, b):
    return lax.dot_general(a, b, (((0,), (0,)), ((), ())), preferred_element_type=f32)


def sigmoid(v):
    return 0.5 * jnp.tanh(0.5 * v) + 0.5


def silu(v):
    return v * sigmoid(v)


def silu_slope(v):
    s = sigmoid(v)
    return s * (1.0 + v * (1.0 - s))


def high_low(v):
    high = v.astype(bf16)
    return high, (v - high.astype(f32)).astype(bf16)


class Total:
    AXES = "kxyz"

    @staticmethod
    def scratch(X, Y, Z):
        many = 1 + X - 1 + Y - 1 + Z - 1
        return [pltpu.VMEM((n, 8, 128), f32) for n in (2, X, Y, Z)] + [
            pltpu.VMEM((8, 128), f32),
            pltpu.SemaphoreType.DMA((many,)),
            pltpu.SemaphoreType.DMA((many,)),
        ]

    def __init__(self, place, refs):
        self.p, self.bufs, (self.value, self.ss, self.rs) = place, dict(zip("kxyz", refs[:4])), refs[4:]

    def _copies(self, axis):
        p, buf = self.p, self.bufs[axis]
        base = sum(getattr(p, a.upper()) - 1 for a in self.AXES[: self.AXES.index(axis)])
        here = buf.at[getattr(p, axis)]
        for d in range(1, getattr(p, axis.upper())):
            i = base + d - 1
            yield remote(here, here, self.ss.at[i], self.rs.at[i], p.peer(axis, d))

    def start(self, axis):
        self.bufs[axis][getattr(self.p, axis)] = self.value[...]
        for copy in self._copies(axis):
            copy.start()

    def finish(self, axis):
        for copy in self._copies(axis):
            copy.wait_recv()
        buf = self.bufs[axis]
        value = buf[0]
        for i in range(1, getattr(self.p, axis.upper())):
            value = value + buf[i]
        self.value[...] = value

    def drain(self, axes):
        for axis in axes:
            for copy in self._copies(axis):
                copy.wait_send()


class Reduce:
    def __init__(self, grid, dim, n_col, width, late, order, lender=None, lanes=0):
        self.X, self.Y, self.Z = grid
        self.dim, self.shard, self.late, self.order = dim, dim // n_col, late, order
        self.ry = self.shard // self.Y
        self.rz = self.ry // self.Z
        self.w = width
        self.lender, self.lanes, self.lent = lender, lanes, False

    def scratch(self):
        X, Y, Z, w = self.X, self.Y, self.Z, self.w
        many = X + (X - 1) + 2 * (Y - 1) + 2 * (Z - 1)
        along_x = (X - 1, 1, self.shard, w) if self.order == "xy" else (X - 1, 1, self.ry, w)
        along_y = (Y - 1, 1, self.ry, w) if self.order == "xy" else (Y - 1, X, self.ry, w)
        return [
            *([] if self.lender else [pltpu.VMEM((self.dim, w), f32)]),
            pltpu.VMEM((X, self.shard, w), f32),
            pltpu.VMEM(along_x, bf16),
            pltpu.VMEM(along_x, bf16),
            pltpu.VMEM(along_y, bf16),
            pltpu.VMEM(along_y, bf16),
            pltpu.VMEM((Z - 1, self.rz, w), self.late),
            pltpu.VMEM((Z - 1, self.rz, w), self.late),
            pltpu.VMEM((self.rz, w), f32),
            pltpu.VMEM((self.shard, w), self.late),
            pltpu.SemaphoreType.DMA((many,)),
            pltpu.SemaphoreType.DMA((many,)),
        ]

    def bind(self, place, refs):
        if self.lender:
            refs = (self.lender.full.at[:, self.lanes : self.lanes + self.w], *refs)
        (self.full, self.cr, self.xs, self.xr, self.ys, self.yr, self.zs, self.zin, self.piece, self.out, self.ss, self.rs) = refs
        self.p = place

    def lend(self):
        for copy in self.copies(0):
            copy.wait_send()

    def rows_of(self, x, k):
        return (2 * x + k) * self.shard

    def place_z(self):
        return pl.ds(pl.multiple_of(self.p.y * self.ry + self.p.z * self.rz, 16), self.rz)

    def copies(self, stage):
        p, X, Y, Z = self.p, self.X, self.Y, self.Z
        first_x = self.order == "xy"
        x_base, y_base = (X, 2 * X - 1) if first_x else (X + Y - 1, X)
        base = (0, x_base if first_x else y_base, y_base if first_x else x_base, 2 * X + Y - 2, 2 * X + Y + Z - 3, 2 * X + Y + 2 * Z - 4)[stage]
        if stage == 0:
            many = [(self.full.at[ds(self.rows_of(x, 1 - p.k), self.shard), :], self.cr.at[x], p.peer("k", 1)) for x in range(X)]
        elif stage == (1 if first_x else 2):
            many = [(self.xs.at[d - 1], self.xr.at[d - 1], p.peer("x", d)) for d in range(1, X)]
        elif stage == (2 if first_x else 1):
            many = [(self.ys.at[d - 1], self.yr.at[d - 1], p.peer("y", d)) for d in range(1, Y)]
        elif stage == 3:
            many = [(self.zs.at[d - 1], self.zin.at[d - 1], p.peer("z", d)) for d in range(1, Z)]
        elif stage == 4:
            here = self.out.at[self.place_z(), :]
            many = [(here, here, p.peer("z", d)) for d in range(1, Z)]
        else:
            here = self.out.at[pl.ds(pl.multiple_of(p.y * self.ry, 16), self.ry), :]
            many = [(here, here, p.peer("y", d)) for d in range(1, Y)]
        return [remote(src, dst, self.ss.at[base + i], self.rs.at[base + i], to) for i, (src, dst, to) in enumerate(many)]

    def sum_core(self, x, at, n=16):
        mine = self.full[pl.ds(pl.multiple_of(self.rows_of(x, self.p.k) + at, 16), n), :]
        return mine + self.cr[x, pl.ds(at, n), :]

    def sum_first(self, x, y, at):
        rows = pl.multiple_of(y * self.ry + at, 16)
        value = self.sum_core(x, rows)
        if self.order == "xy":
            for d in range(1, self.X):
                value = value + self.xr[d - 1, 0, pl.ds(rows, 16), :].astype(f32)
        else:
            for d in range(1, self.Y):
                value = value + self.yr[d - 1, x, pl.ds(at, 16), :].astype(f32)
        return value

    def stage(self, s):
        p, X, Y, Z = self.p, self.X, self.Y, self.Z
        if s:
            for copy in self.copies(s - 1):
                copy.wait_recv()
        if s == 1 and self.order == "xy":
            for d in range(1, X):
                to = p.to("x", d)

                def one(at, to=to, d=d):
                    self.xs[d - 1, 0, pl.ds(at, 16), :] = self.sum_core(to, at).astype(bf16)

                by_rows(self.shard, 16, one)
        elif s == 1:
            for d in range(1, Y):
                base = p.to("y", d) * self.ry

                def one(at, base=base, d=d):
                    for x in range(X):
                        self.ys[d - 1, x, pl.ds(at, 16), :] = self.sum_core(x, pl.multiple_of(base + at, 16)).astype(bf16)

                by_rows(self.ry, 16, one)
        elif s == 2:
            if self.order == "xy":
                for d in range(1, Y):

                    def one(at, to=p.to("y", d), d=d):
                        self.ys[d - 1, 0, pl.ds(at, 16), :] = self.sum_first(p.x, to, at).astype(bf16)

                    by_rows(self.ry, 16, one)
            else:
                for d in range(1, X):

                    def one(at, to=p.to("x", d), d=d):
                        self.xs[d - 1, 0, pl.ds(at, 16), :] = self.sum_first(to, p.y, at).astype(bf16)

                    by_rows(self.ry, 16, one)

            def mine(at):
                self.cr[p.x, pl.ds(pl.multiple_of(p.y * self.ry + at, 16), 16), :] = self.sum_first(p.x, p.y, at)

            by_rows(self.ry, 16, mine)
        elif s == 3:

            def total(z):
                rows = pl.multiple_of(z * self.rz, 16)
                value = self.cr[p.x, pl.ds(pl.multiple_of(p.y * self.ry + rows, 16), self.rz), :]
                arrived = self.yr if self.order == "xy" else self.xr
                for d in range(1, Y if self.order == "xy" else X):
                    value = value + arrived[d - 1, 0, pl.ds(rows, self.rz), :].astype(f32)
                return value

            for d in range(1, Z):
                self.zs[d - 1] = total(p.to("z", d)).astype(self.late)
            self.piece[...] = total(p.z)
        elif s == 4:
            value = self.piece[...]
            for d in range(1, Z):
                value = value + self.zin[d - 1].astype(f32)
            self.piece[...] = value
            self.out[self.place_z(), :] = value.astype(self.late)
        if s < STAGES - 1:
            for copy in self.copies(s):
                copy.start()

    def drain(self):
        for s in range(1 if self.lent else 0, STAGES - 1):
            for copy in self.copies(s):
                copy.wait_send()


STAGES = 7


class Step:
    def __init__(self, mesh, samples, slots, dim, edges, c_in):
        self.n_row, self.n_col = mesh.shape["row"], mesh.shape["col"]
        self.grid = sizes_of(self.n_row, self.n_col)
        self.S, self.C, self.D, self.E, self.c_in = samples, slots, dim, edges, c_in
        self.N = MESH_DEV
        self.SH = dim // self.n_col
        self.R, self.Q = self.n_row * self.N, self.n_col * self.N
        chunk = functools.partial(Reduce, self.grid, dim, self.n_col)
        skips, decoders = chunk(dim + N_OUT, f32, "xy"), chunk(2 * dim, bf16, "xy")
        skips.lent = decoders.lent = True
        self.chunks = [
            skips,
            decoders,
            chunk(dim, bf16, "xy", decoders, 0),
            chunk(dim, bf16, "xy", decoders, dim),
            chunk(dim, bf16, "yx", skips, 0),
            chunk(N_IN, f32, "yx"),
        ]
        X, Y, Z = self.grid
        S, C, D, E, N, R, Q = self.S, self.C, self.D, self.E, self.N, self.R, self.Q
        vm = pltpu.VMEM
        dma = lambda *shape: pltpu.SemaphoreType.DMA(shape)
        self.shapes = dict(
            wib=vm((D, N_IN), bf16),
            wlb=vm((6, D, D), bf16),
            wob=vm((D, N_OUT), bf16),
            nm=vm((N, C), bf16),
            nv=vm((N, C), bf16),
            cm=vm((C, N), bf16),
            cmv=vm((C, N), bf16),
            cw=vm((C, 128), f32),
            cnt=vm((N, 128), f32),
            fp=vm((S * C, D), f32),
            gl=vm((S * C, D), bf16),
            tp=vm((S * C, D), f32),
            go=vm((S * C, D), bf16),
            dp=vm((S * C, N_OUT), bf16),
            dt=vm((S * C, D), bf16),
            av=vm((S * N, D), bf16),
            sp=vm((S * N, D), f32),
            mlb=vm((S * N, D), bf16),
            agb=vm((S * N, D), bf16),
            mnb=vm((S * N, D), bf16),
            sg=vm((S * N, D), f32),
            dmn=vm((S * N, D), f32),
            dsb=vm((S * N, D), bf16),
            drb=vm((S * N, D), bf16),
            d2b=vm((S * N, D), bf16),
            sr=vm((S, R + Q, D), bf16),
            oh=vm((E, R + Q), bf16),
            oht=vm((R + Q, E), bf16),
            ep=vm((S, E, D), f32),
            ac=vm((E, D), bf16),
            tmp=vm((R + Q, D), f32),
            part=vm((S, Q, D), f32),
            pcr=vm((S, X, N, D), f32),
            pxs=vm((S, X - 1, N, D), bf16),
            pxr=vm((S, X - 1, N, D), bf16),
            da=vm((S, Q, D), bf16),
            down=vm((S, Z, N, D), f32),
            dys=vm((S, Y - 1, Z, N, D), bf16),
            dyr=vm((S, Y - 1, Z, N, D), bf16),
            dzs=vm((S, Z - 1, N, D), bf16),
            dzr=vm((S, Z - 1, N, D), bf16),
            loss=vm((8, 128), f32),
            l_sem=dma(24),
            w_ss=dma(8, 1 + 2 * (X - 1)),
            w_rs=dma(8, 1 + 2 * (X - 1)),
            mz_ss=dma(S, Z - 1),
            mz_rs=dma(S, Z - 1),
            my_ss=dma(S, Y - 1, Z),
            my_rs=dma(S, Y - 1, Z),
            mr_ss=dma(S, 1 + 2 * (X - 1)),
            mr_rs=dma(S, 1 + 2 * (X - 1)),
            pk_ss=dma(2, S, X),
            pk_rs=dma(2, S, X),
            px_ss=dma(2, S, X - 1),
            px_rs=dma(2, S, X - 1),
            a_ss=dma(S, 1 + 2 * (X - 1)),
            a_rs=dma(S, 1 + 2 * (X - 1)),
            dy_ss=dma(S, Y - 1, Z),
            dy_rs=dma(S, Y - 1, Z),
            dz_ss=dma(S, Z - 1),
            dz_rs=dma(S, Z - 1),
        )

    def fits(self):
        X, Y, Z = self.grid
        return self.SH % (16 * Y * Z) == 0 and self.SH % 128 == 0 and self.vmem_bytes() < VMEM_ROOM

    def vmem_bytes(self):
        total = 0
        for s in [*self.shapes.values(), *[s for c in self.chunks for s in c.scratch()]]:
            dtype = getattr(s, "dtype", None)
            if dtype in (jnp.dtype(f32), jnp.dtype(bf16)):
                size = jnp.dtype(dtype).itemsize
                for n in s.shape[:-1]:
                    size *= n
                total += size * -(-s.shape[-1] // 128) * 128
        return total

    def scratch(self):
        total = Total.scratch(*self.grid)
        return [*self.shapes.values(), *total * 2, *[s for c in self.chunks for s in c.scratch()]]

    def kernel(self, count, x, tgt, area, node, snd, rcv, wi, wl, wo, mi, mal, mo, si, sal, so, *refs):
        S, C, D, E, N, R, Q, SH = self.S, self.C, self.D, self.E, self.N, self.R, self.Q, self.SH
        X, Y, Z = self.grid
        (g_in, g_out, g_skip, g_two, g_three, g_four, stats), refs = refs[:7], refs[7:]
        v = types.SimpleNamespace(**dict(zip(self.shapes, refs)))
        refs = refs[len(self.shapes) :]
        p = Place(self.n_row, self.n_col)
        area_sum, stat_sum = Total(p, refs[:7]), Total(p, refs[7:14])
        refs = refs[14:]
        for chunk in self.chunks:
            many = len(chunk.scratch())
            chunk.bind(p, refs[:many])
            refs = refs[many:]

        def weight_rows(i, col):
            which = WIRE[i]
            whole = v.wib if which == "in" else v.wob if which == "out" else v.wlb.at[which]
            return whole.at[ds(col * SH, SH), :]

        def w_copy(i, j, d=0):
            rows = weight_rows(i, 2 * p.to("x", -d) + p.k if j == 2 else p.col)
            at = (0, d, X - 1 + d)[j]
            device = p.peer("x", d) if j == 1 else p.peer("k", 1)
            return remote(rows, rows, v.w_ss.at[i, at], v.w_rs.at[i, at], device)

        hops = range(1, X)

        def w_forward(i):
            for d in hops:
                w_copy(i, 1, d).wait_recv()
                w_copy(i, 2, d).start()

        def w_get(i):
            w_copy(i, 0).wait_recv()
            for d in hops:
                w_copy(i, 2, d).wait_recv()

        W = lambda which: v.wlb[which]
        barrier = p.greet()
        own = ds(p.col * SH, SH)
        loads = [pltpu.make_async_copy(wl.at[m], v.fp.at[m * SH : (m + 1) * SH, :], v.l_sem.at[m]) for m in range(6)]
        for load in loads:
            load.start()

        def turned(ref, n):
            v.tmp[0:n, 0:SH] = jnp.zeros((n, SH), f32)
            v.tmp[0 : ref.shape[0], 0:SH] = ref[...]
            return jnp.transpose(v.tmp[0:n, 0:SH])

        v.wib[own, :] = turned(wi, N_IN).astype(bf16)
        v.wob[own, :] = turned(wo, N_OUT).astype(bf16)
        for m, load in enumerate(loads):
            load.wait()
            v.wlb[m, own, :] = v.fp[m * SH : (m + 1) * SH, :].astype(bf16)
        used = count[0]
        area_row = area[...].reshape(1, C) * (lax.broadcasted_iota(jnp.int32, (1, C), 1) < used).astype(f32)
        area_sum.value[...] = jnp.broadcast_to(jnp.sum(area_row), (8, 128))
        pl.semaphore_wait(*barrier)


        def w_depart(*items):
            for i in items:
                w_copy(i, 0).start()
                for d in hops:
                    w_copy(i, 1, d).start()

        w_depart(0, 1, 2, 3)
        area_sum.start("y")

        node_row = node[...].reshape(1, C)
        match = (lax.broadcasted_iota(jnp.int32, (N, C), 0) == node_row).astype(f32)
        v.nm[...] = match.astype(bf16)
        match = match * (lax.broadcasted_iota(jnp.int32, (N, C), 1) < used).astype(f32)
        v.nv[...] = match.astype(bf16)
        v.cnt[...] = jnp.broadcast_to(jnp.maximum(jnp.sum(match, axis=1, keepdims=True), 1.0), (N, 128))
        node_col = jnp.transpose(jnp.broadcast_to(node_row, (128, C)))
        v.cw[...] = jnp.transpose(jnp.broadcast_to(area_row, (128, C)))
        match = (lax.broadcasted_iota(jnp.int32, (C, 128), 1) == node_col).astype(f32)
        v.cm[...] = match[:, :N].astype(bf16)
        match = match * (lax.broadcasted_iota(jnp.int32, (C, 128), 0) < used).astype(f32)
        v.cmv[...] = match[:, :N].astype(bf16)

        def table(index, base, rows):
            def down(at):
                hit = lax.broadcasted_iota(jnp.int32, (128, E), 0) + at == index
                v.oht[pl.ds(pl.multiple_of(base + at, 128), 128), :] = hit.astype(f32).astype(bf16)

            by_rows(rows, 128, down)
            column = jnp.transpose(jnp.broadcast_to(index, (128, E)))
            for at in range(0, rows, 128):
                hit = lax.broadcasted_iota(jnp.int32, (E, 128), 1) + at == column
                v.oh[:, base + at : base + at + 128] = hit.astype(f32).astype(bf16)

        table(snd[...], 0, R)
        table(rcv[...], R, Q)
        v.dp[...] = jnp.zeros((S * C, N_OUT), bf16)
        v.loss[...] = jnp.zeros((8, 128), f32)

        w_forward(0)
        w_get(0)

        def encode(s, carry):
            at = ds(s * C, C)
            pre = mm_nt(x[s], v.wib[:, : self.c_in])
            v.fp[at, :] = pre
            v.gl[at, :] = silu(pre).astype(bf16)
            here = ds(s * N, N)
            v.av[here, :] = (mm(v.nv[...], v.gl[at, :]) / v.cnt[:, 0:1]).astype(bf16)
            return carry

        lax.fori_loop(0, S, encode, 0)
        area_sum.finish("y")
        area_sum.start("z")
        w_forward(1)
        w_get(1)
        pre = mm(v.av[...], W(0))
        v.sp[...] = pre
        v.mlb[...] = silu(pre).astype(bf16)

        def mz(s, d):
            rows = v.sr.at[s, ds(p.row * N, N), :]
            return remote(rows, rows, v.mz_ss.at[s, d - 1], v.mz_rs.at[s, d - 1], p.peer("z", d))

        def my(s, d, e):
            rows = v.sr.at[s, ds((p.to("z", -e) * Y + p.y) * N, N), :]
            return remote(rows, rows, v.my_ss.at[s, d - 1, e], v.my_rs.at[s, d - 1, e], p.peer("y", d))

        def mr(s, j, d=0):
            col = 2 * p.to("x", -d) + p.k if j == 2 else p.col
            rows = v.sr.at[s, ds(R + col * N, N), :]
            at = (0, d, X - 1 + d)[j]
            return remote(rows, rows, v.mr_ss.at[s, at], v.mr_rs.at[s, at], p.peer("x", d) if j == 1 else p.peer("k", 1))

        for s in range(S):
            v.sr[s, ds(p.row * N, N), :] = v.mlb[s * N : (s + 1) * N, :]
            v.sr[s, ds(R + p.col * N, N), :] = v.mlb[s * N : (s + 1) * N, :]

        def depart(s):
            for d in range(1, Z):
                mz(s, d).start()

        depart(0)
        for s in range(S):
            for d in range(1, Y):
                my(s, d, 0).start()
            mr(s, 0).start()
            for d in hops:
                mr(s, 1, d).start()
            if s == 1:
                w_depart(4)
        w_depart(5, 6, 7)
        w_forward(2)
        w_forward(3)
        depart(1)
        area_sum.finish("z")
        area_sum.start("x")
        w_get(2)
        w_get(3)

        def skip(at):
            v.tp[pl.ds(at, 512), :] = mm(v.gl[pl.ds(at, 512), :], W(5))

        def pk(t, s, xx):
            rows = v.part.at[s, ds((2 * xx + 1 - p.k) * N, N), :]
            return remote(rows, v.pcr.at[s, xx], v.pk_ss.at[t, s, xx], v.pk_rs.at[t, s, xx], p.peer("k", 1))

        def px(t, s, d):
            return remote(v.pxs.at[s, d - 1], v.pxr.at[s, d - 1], v.px_ss.at[t, s, d - 1], v.px_rs.at[t, s, d - 1], p.peer("x", d))

        def col_second(t, s):
            for xx in range(X):
                pk(t, s, xx).wait_recv()
            for d in hops:
                px_to = p.to("x", d)
                mine = v.part[s, ds((2 * px_to + p.k) * N, N), :]
                v.pxs[s, d - 1] = (mine + v.pcr[s, px_to]).astype(bf16)
                px(t, s, d).start()

        def col_last(t, s):
            total = v.part[s, ds(p.col * N, N), :] + v.pcr[s, p.x]
            for d in hops:
                px(t, s, d).wait_recv()
                total = total + v.pxr[s, d - 1].astype(f32)
            return total

        def nearest(j):
            steps = [(n + 1) // 2 * (1 if n % 2 else -1) for n in range(1, 2 * Z - 1)]
            taken, found = jnp.int32(0), jnp.int32(0)
            for step in steps:
                inside = ((p.z - step >= 0) & (p.z - step < Z)).astype(jnp.int32)
                found = found + jnp.where((taken == j) & (inside == 1), step, 0)
                taken = taken + inside
            return (found + Z) % Z

        def arrive(s):
            for j in range(Z - 1):
                d = nearest(j)
                mz(s, d).wait_recv()
                for b in range(1, Y):
                    my(s, b, d).start()
            for d in hops:
                mr(s, 1, d).wait_recv()
                mr(s, 2, d).start()

        def edges(s):
            for b in range(1, Y):
                for e in range(Z):
                    my(s, b, e).wait_recv()
            mr(s, 0).wait_recv()
            for d in hops:
                mr(s, 2, d).wait_recv()
            for d in range(1, Z):
                mz(s, d).wait_send()
            for b in range(1, Y):
                for e in range(Z):
                    my(s, b, e).wait_send()
            mr(s, 0).wait_send()
            for d in hops:
                mr(s, 1, d).wait_send()
                mr(s, 2, d).wait_send()
            v.sr[s, 0:R, :] = mm(v.sr[s, 0:R, :], W(1)).astype(bf16)
            v.sr[s, R : R + Q, :] = mm(v.sr[s, R : R + Q, :], W(2)).astype(bf16)

            def pick(at):
                pre = mm(v.oh[pl.ds(at, 512), :], v.sr[s])
                v.ep[s, pl.ds(at, 512), :] = pre
                v.ac[pl.ds(at, 512), :] = silu(pre).astype(bf16)

            by_rows(E, 512, pick)
            v.part[s] = mm(v.oht[R:, :], v.ac[...])
            for xx in range(X):
                pk(0, s, xx).start()

        def ac(s, j, d=0):
            col = 2 * p.to("x", -d) + p.k if j == 2 else p.col
            rows = v.da.at[s, ds(col * N, N), :]
            at = (0, d, X - 1 + d)[j]
            return remote(rows, rows, v.a_ss.at[s, at], v.a_rs.at[s, at], p.peer("x", d) if j == 1 else p.peer("k", 1))

        def decode(s):
            at, here = ds(s * C, C), ds(s * N, N)
            v.agb[here, :] = (col_last(0, s) * (1.0 / DEG)).astype(bf16)
            v.mnb[here, :] = (silu(v.sp[here, :]) + mm(v.agb[here, :], W(3))).astype(bf16)
            scale = 1.0 / (C_OUT * S * area_sum.value[0:1, 0:1])
            rows = mm(v.cm[...], v.mnb[here, :]).astype(bf16)
            pre = mm(rows, W(4)) + v.tp[at, :]
            v.tp[at, :] = pre
            v.go[at, :] = silu(pre).astype(bf16)
            error = mm(v.go[at, :], v.wob[...])[:, :C_OUT] - tgt[s].astype(f32)
            weighted = v.cw[:, :C_OUT] * error
            v.loss[0:1, 0:C_OUT] = v.loss[0:1, 0:C_OUT] + jnp.sum(weighted * error, axis=0, keepdims=True)
            v.dp[at, 0:C_OUT] = (2.0 * weighted * scale).astype(bf16)
            v.dt[at, :] = (silu_slope(v.tp[at, :]) * mm_nt(v.dp[at, :], v.wob[...])).astype(bf16)
            grad = mm(v.nm[...], v.dt[at, :])
            v.sg[here, :] = grad
            grad = mm_nt(jnp.concatenate(high_low(grad), axis=0), W(4))
            grad = grad[:N] + grad[N:]
            v.dmn[here, :] = grad
            v.da[s, ds(p.col * N, N), :] = mm_nt(grad.astype(bf16), W(3)).astype(bf16)
            ac(s, 0).start()
            for d in hops:
                ac(s, 1, d).start()

        def dy(s, d, e):
            return remote(v.dys.at[s, d - 1, e], v.dyr.at[s, d - 1, e], v.dy_ss.at[s, d - 1, e], v.dy_rs.at[s, d - 1, e], p.peer("y", d))

        def dz(s, d):
            return remote(v.dzs.at[s, d - 1], v.dzr.at[s, d - 1], v.dz_ss.at[s, d - 1], v.dz_rs.at[s, d - 1], p.peer("z", d))

        def pass_on(s):
            for d in hops:
                ac(s, 1, d).wait_recv()
                ac(s, 2, d).start()

        def edges_back(s):
            ac(s, 0).wait_recv()
            for d in hops:
                ac(s, 2, d).wait_recv()
            for xx in range(X):
                pk(0, s, xx).wait_send()
            for d in hops:
                px(0, s, d).wait_send()

            def pick(at):
                grad = mm(v.oh[pl.ds(at, 512), R:], v.da[s])
                v.ac[pl.ds(at, 512), :] = (silu_slope(v.ep[s, pl.ds(at, 512), :]) * grad * (1.0 / DEG)).astype(bf16)

            by_rows(E, 512, pick)
            v.tmp[...] = mm(v.oht[...], v.ac[...])
            for e in (*range(1, Z), 0):
                to = p.to("z", e)
                for d in range(1, Y):
                    v.dys[s, d - 1, e] = v.tmp[ds((to * Y + p.to("y", d)) * N, N), :].astype(bf16)
                    dy(s, d, e).start()
                v.down[s, e] = v.tmp[ds((to * Y + p.y) * N, N), :]
            v.part[s] = v.tmp[R:, :]
            for xx in range(X):
                pk(1, s, xx).start()

        def row_sum(s, e):
            total = v.down[s, e]
            for d in range(1, Y):
                dy(s, d, e).wait_recv()
                total = total + v.dyr[s, d - 1, e].astype(f32)
            return total

        def row_second(s):
            for e in range(1, Z):
                v.dzs[s, e - 1] = row_sum(s, e).astype(bf16)
                dz(s, e).start()

        def encode_back(s):
            at, here = ds(s * C, C), ds(s * N, N)
            v.drb[here, :] = col_last(1, s).astype(bf16)
            total = row_sum(s, 0)
            for d in range(1, Z):
                dz(s, d).wait_recv()
                total = total + v.dzr[s, d - 1].astype(f32)
            v.dsb[here, :] = total.astype(bf16)
            whole = v.dmn[here, :] + mm_nt(v.dsb[here, :], W(1)) + mm_nt(v.drb[here, :], W(2))
            v.d2b[here, :] = (silu_slope(v.sp[here, :]) * whole).astype(bf16)
            high, low = high_low(mm_nt(v.d2b[here, :], W(0)) / v.cnt[:, 0:1])
            grad = v.tp[at, :] + mm(v.cmv[...], high) + mm(v.cmv[...], low)
            v.dt[at, :] = (silu_slope(v.fp[at, :]) * grad).astype(bf16)

        skips, decoders, senders, receivers, encoders, inputs = self.chunks

        def decoder_gradients():
            skips.full[:, 0:D] = mm_tn(v.gl[...], v.dt[...])
            skips.full[:, D : D + N_OUT] = mm_tn(v.go[...], v.dp[...])
            skips.stage(0)
            high, low = high_low(v.sg[...])
            decoders.full[:, 0:D] = mm_tn(v.mnb[...], high) + mm_tn(v.mnb[...], low)
            decoders.full[:, D : 2 * D] = mm_tn(v.agb[...], v.dmn[...].astype(bf16))
            decoders.stage(0)

        def skip_back():
            def one(at):
                v.tp[pl.ds(at, 512), :] = mm_nt(v.dt[pl.ds(at, 512), :], W(5))

            by_rows(S * C, 512, one)

        def weights_rest():
            for i in (5, 6, 7):
                w_forward(i)
            area_sum.finish("x")
            area_sum.start("k")
            for i in (5, 6, 7):
                w_get(i)
            area_sum.finish("k")

        def partials_back(s):
            col_second(1, s)
            row_second(s)

        stage = lambda chunk, n: functools.partial(chunk.stage, n)
        line = [
            (edges_back, 3),
            (stage(decoders, 1), S + 2, None),
            (edges, 0),
            (arrive, -2),
            (weights_rest, 1, None),
            (decoder_gradients, S + 1, None),
            (partials_back, 4),
            (pass_on, 2),
            (stage(skips, 1), S + 1, None),
            (skip_back, S + 2, None),
            (decode, 1),
            (functools.partial(col_second, 0), 0),
            (stage(skips, 3), S + 5, None),
            (encode_back, 6),
            (stage(skips, 2), S + 3, None),
            (stage(decoders, 2), S + 3, None),
        ]
        arrive(0)
        depart(2)
        w_forward(4)
        w_get(4)
        by_rows(S * C, 512, skip)
        arrive(1)
        depart(3)

        def turn(i, carry):
            for todo, behind, *once in line:
                if once:
                    pl.when(i == behind)(todo)
                else:
                    pl.when((i >= max(behind, 0)) & (i < S + behind))(functools.partial(todo, i - behind))
            return carry

        lax.fori_loop(0, S + 6, turn, 0)
        states = [
            pltpu.make_async_copy(a.at[m], v.ep.at[j, m * SH : (m + 1) * SH, :], v.l_sem.at[6 + 6 * j + m])
            for j, a in enumerate((wl, mal, sal))
            for m in range(6)
        ]
        for load in states:
            load.start()
        decoders.lend()
        skips.lend()
        senders.full[...] = mm_tn(v.mlb[...], v.dsb[...])
        senders.stage(0)
        receivers.full[...] = mm_tn(v.mlb[...], v.drb[...])
        receivers.stage(0)
        encoders.full[...] = mm_tn(v.av[...], v.d2b[...])
        encoders.stage(0)
        inputs.full[:, self.c_in :] = jnp.zeros((D, N_IN - self.c_in), f32)
        for s in range(S):
            grad = mm_tn(v.dt[s * C : (s + 1) * C, :], x[s])
            if s:
                grad = grad + inputs.full[:, : self.c_in]
            inputs.full[:, : self.c_in] = grad
        inputs.stage(0)
        senders.stage(1)
        encoders.stage(1)
        receivers.stage(1)
        inputs.stage(1)
        decoders.stage(3)

        for load in states:
            load.wait()
        spare = v.ep.at[3]
        for j, (a, b) in enumerate(((wi, wo), (mi, mo), (si, so))):
            spare[j * SH : (j + 1) * SH, 0:N_IN] = turned(a, N_IN)
            spare[j * SH : (j + 1) * SH, N_IN : N_IN + N_OUT] = turned(b, N_OUT)
        lane = lax.broadcasted_iota(jnp.int32, (8, 128), 1)
        row = lax.broadcasted_iota(jnp.int32, (8, 128), 0)
        stat_sum.value[...] = jnp.where(row == 2, jnp.sum(v.loss[...]), 0.0)

        def note(j, gradient, at, lanes):
            held = [buf[pl.ds(pl.multiple_of(start + p.y * (SH // Y) + p.z * (SH // Y // Z), 16), SH // Y // Z), lanes] for buf, start in at]
            _, _, update = adam_parts(held[0], gradient, held[1], held[2])
            for i, what in enumerate((held[0], update)):
                stat_sum.value[...] += jnp.where((row == i) & (lane == j), jnp.sum(what * what), 0.0)

        def note_latent(m, gradient):
            note(1 + m, gradient, [(v.ep.at[j], m * SH) for j in range(3)], slice(None))

        edge = [(spare, j * SH) for j in range(3)]
        skips.stage(4)
        note_latent(5, skips.piece[:, 0:D])
        note(7, skips.piece[:, D : D + N_OUT], edge, slice(N_IN, N_IN + N_OUT))
        senders.stage(2)
        encoders.stage(2)
        decoders.stage(4)
        note_latent(4, decoders.piece[:, 0:D])
        note_latent(3, decoders.piece[:, D : 2 * D])
        receivers.stage(2)
        inputs.stage(2)
        skips.stage(5)
        senders.stage(3)
        encoders.stage(3)
        receivers.stage(3)
        inputs.stage(3)
        decoders.stage(5)
        senders.stage(4)
        note_latent(1, senders.piece[...])
        encoders.stage(4)
        note_latent(0, encoders.piece[...])
        receivers.stage(4)
        note_latent(2, receivers.piece[...])
        inputs.stage(4)
        note(0, inputs.piece[...], edge, slice(0, N_IN))
        stat_sum.start("k")
        skips.stage(6)
        g_skip[...] = skips.out[:, :D]
        g_out[...] = jnp.transpose(skips.out[:, D : D + N_OUT])[: g_out.shape[0], :]
        stat_sum.finish("k")
        stat_sum.start("x")
        decoders.stage(6)
        g_two[...] = decoders.out[...]
        senders.stage(5)
        encoders.stage(5)
        stat_sum.finish("x")
        stat_sum.start("z")
        receivers.stage(5)
        inputs.stage(5)
        senders.stage(6)
        g_three[:, 0:D] = senders.out[...]
        encoders.stage(6)
        g_four[...] = encoders.out[...]
        stat_sum.finish("z")
        stat_sum.start("y")
        receivers.stage(6)
        g_three[:, D : 2 * D] = receivers.out[...]
        inputs.stage(6)
        g_in[...] = jnp.transpose(inputs.out[...])[: g_in.shape[0], :]
        stat_sum.finish("y")
        stats[...] = jnp.where(row < 2, stat_sum.value[...], stat_sum.value[...] / (C_OUT * S * area_sum.value[...]))

        for i in range(8):
            w_copy(i, 0).wait_send()
            for d in hops:
                w_copy(i, 1, d).wait_send()
                w_copy(i, 2, d).wait_send()
        for s in range(S):
            for d in range(1, Z):
                dz(s, d).wait_send()
            for d in range(1, Y):
                for e in range(Z):
                    dy(s, d, e).wait_send()
            ac(s, 0).wait_send()
            for d in hops:
                ac(s, 1, d).wait_send()
                ac(s, 2, d).wait_send()
            for xx in range(X):
                pk(1, s, xx).wait_send()
            for d in hops:
                px(1, s, d).wait_send()
        area_sum.drain("kxyz")
        stat_sum.drain("kxyz")
        for chunk in self.chunks:
            chunk.drain()

    def __call__(self, count, x, tgt, area, node, snd, rcv, *states):
        vm, hbm = pl.BlockSpec(memory_space=pltpu.VMEM), pl.BlockSpec(memory_space=pl.ANY)
        D, SH = self.D, self.SH
        outs = [(states[0].shape, f32), (states[2].shape, f32), ((SH, D), f32), ((SH, 2 * D), bf16), ((SH, 2 * D), bf16), ((SH, D), bf16), ((8, 128), f32)]
        return pl.pallas_call(
            self.kernel,
            out_shape=[jax.ShapeDtypeStruct(*o) for o in outs],
            in_specs=[pl.BlockSpec(memory_space=pltpu.SMEM)] + [vm] * 6 + [vm, hbm, vm] * 3,
            out_specs=[vm] * 7,
            scratch_shapes=self.scratch(),
            name="train_step",
            compiler_params=pltpu.CompilerParams(collective_id=0, has_side_effects=True, vmem_limit_bytes=67043328),
        )(count, x, tgt, area, node, snd, rcv, *states)


def update_kernel(g_in, g_out, g_skip, g_two, g_three, g_four, stats, wi, wl, wo, mi, mal, mo, si, sal, so, *refs):
    loss, *outs, norms = refs[:17]
    in_buf, out_buf, low_buf, in_sem, out_sem = refs[17:]
    SH, D = g_skip.shape
    loads = [[pltpu.make_async_copy(a.at[m], in_buf.at[j, m], in_sem.at[j, m]) for j, a in enumerate((wl, mal, sal))] for m in range(6)]
    order = (5, 4, 3, 2, 1, 0)
    for m in order:
        for load in loads[m]:
            load.start()
    root = jnp.sqrt(stats[...])
    norms[...] = root[0:2, 0:8]
    loss[...] = stats[2:3, 0:1]

    def step(j, weight, gradient, mean, square):
        first, second, update = adam_parts(weight, gradient, mean, square)
        ratio = root[0:1, j : j + 1] / (root[1:2, j : j + 1] + trust_epsilon)
        master = weight - learn_rate * ratio * update
        return gradient, first, second, master, master.astype(bf16)

    grads = {5: (g_skip, 0), 4: (g_two, 0), 3: (g_two, D), 2: (g_three, D), 1: (g_three, 0), 0: (g_four, 0)}
    stores = []
    for m in order:
        for load in loads[m]:
            load.wait()
        ref, at = grads[m]
        results = step(1 + m, in_buf[0, m], ref[:, at : at + D].astype(f32), in_buf[1, m], in_buf[2, m])
        for j, result in enumerate(results):
            buf = low_buf.at[m] if j == 4 else out_buf.at[j, m]
            buf[...] = result
            stores.append(pltpu.make_async_copy(buf, outs[3 * j + 1].at[m], out_sem.at[j, m]))
            stores[-1].start()
    for j, result in enumerate(step(0, wi[...], g_in[...], mi[...], si[...])):
        outs[3 * j][...] = result
    for j, result in enumerate(step(7, wo[...], g_out[...], mo[...], so[...])):
        outs[3 * j + 2][...] = result
    for store in stores:
        store.wait()


def update_all(grads, states):
    vm, hbm = pl.BlockSpec(memory_space=pltpu.VMEM), pl.BlockSpec(memory_space=pl.ANY)
    kinds = [f32] * 4 + [bf16]
    shapes = [states[0].shape, states[1].shape, states[2].shape]
    n, SH, D = states[1].shape
    return pl.pallas_call(
        update_kernel,
        out_shape=[jax.ShapeDtypeStruct((1, 1), f32)]
        + [jax.ShapeDtypeStruct(s, k) for k in kinds for s in shapes]
        + [jax.ShapeDtypeStruct((2, 8), f32)],
        in_specs=[vm] * 7 + [vm, hbm, vm] * 3,
        out_specs=[vm] + [vm, hbm, vm] * 5 + [vm],
        scratch_shapes=[
            pltpu.VMEM((3, n, SH, D), f32),
            pltpu.VMEM((4, n, SH, D), f32),
            pltpu.VMEM((n, SH, D), bf16),
            pltpu.SemaphoreType.DMA((3, n)),
            pltpu.SemaphoreType.DMA((5, n)),
        ],
        name="lamb",
        compiler_params=pltpu.CompilerParams(vmem_limit_bytes=67043328),
    )(*grads, *states)


def kernel_body(mesh, step, inputs, targets, cell_area, cell_count, cell_node, edge_senders, edge_receivers, *states):
    states = [a.T if i % 3 == 2 else a for i, a in enumerate(states)]
    grads = step(cell_count, inputs, targets, cell_area, cell_node, edge_senders[None, :], edge_receivers[None, :], *states)
    loss, *outs, norms = update_all(grads, states)
    outs = [a.T if i % 3 == 2 else a for i, a in enumerate(outs)]
    return (loss[0, 0], *outs, norms)


def native_gradients(
    inputs,
    targets,
    cell_area,
    cell_count,
    cell_node,
    edge_senders,
    edge_receivers,
    weight_input,
    weight_latent,
    weight_output,
):
    full_input, complete_latent, full_output = (
        lax.all_gather(weight_input.astype(jnp.bfloat16), "col", axis=1, tiled=True),
        lax.all_gather(weight_latent.astype(jnp.bfloat16), "col", axis=1, tiled=True),
        lax.all_gather(weight_output.astype(jnp.bfloat16), "col", axis=0, tiled=True),
    )
    samples = inputs.shape[0]
    slots = inputs.shape[1]
    valid = (jnp.arange(slots, dtype=jnp.int32) < cell_count[0]).astype(jnp.float32)
    cell_weight = cell_area * valid
    area_total = lax.psum(jnp.sum(cell_weight), ("row", "col"))
    first_pre = reduced_matmul("sci,id->scd", inputs, full_input)
    grid_latent = jax.nn.silu(first_pre).astype(jnp.bfloat16)
    node_match = (cell_node[None, :] == jnp.arange(MESH_DEV, dtype=jnp.int32)[:, None]).astype(
        jnp.float32
    )
    node_match_low = node_match.astype(jnp.bfloat16)
    cell_match = node_match_low.T
    node_valid = node_match * valid[None, :]
    node_sum = reduced_matmul("nc,scd->snd", node_valid.astype(jnp.bfloat16), grid_latent)
    node_lower_limit = jnp.maximum(jnp.sum(node_valid, axis=1), 1.0)
    node_average = node_sum / node_lower_limit[None, :, None]
    average_reduced = node_average.astype(jnp.bfloat16)
    second_activation_input = reduced_matmul("kaj,jz->kaz", average_reduced, complete_latent[0])
    mesh_latent = jax.nn.silu(second_activation_input)
    mesh_state_reduced = mesh_latent.astype(jnp.bfloat16)
    receiver_local_part = reduced_matmul("kaj,jz->kaz", mesh_state_reduced, complete_latent[2])
    receiver_block = lax.all_gather(receiver_local_part, "col", axis=1, tiled=True)
    sender_block = reduced_matmul(
        "kaj,jz->kaz",
        lax.all_gather(mesh_state_reduced, "row", axis=1, tiled=True),
        complete_latent[1],
    )
    receiver_rows = receiver_block.shape[1]
    sender_rows = sender_block.shape[1]
    sender_match = one_hot_table(edge_senders, sender_rows)
    receiver_match = one_hot_table(edge_receivers, receiver_rows)
    edge_pre = pick_rows(sender_match, sender_block) + pick_rows(receiver_match, receiver_block)
    partial_sums = add_into_rows(receiver_match, jax.nn.silu(edge_pre))
    message_total = lax.psum_scatter(partial_sums, "col", scatter_dimension=1, tiled=True) / DEG
    message_total_reduced = message_total.astype(jnp.bfloat16)
    residual_branch = reduced_matmul("kaj,jz->kaz", message_total_reduced, complete_latent[3])
    mesh_next = mesh_latent + residual_branch
    decode_rows = reduced_matmul("cn,snd->scd", cell_match, mesh_next.astype(jnp.bfloat16)).astype(
        jnp.bfloat16
    )
    third_pre = reduced_matmul("scd,de->sce", decode_rows, complete_latent[4]) + reduced_matmul(
        "scd,de->sce", grid_latent, complete_latent[5]
    )
    grid_out = jax.nn.silu(third_pre).astype(jnp.bfloat16)
    predict = reduced_matmul("scd,do->sco", grid_out, full_output)
    error = predict - targets.astype(jnp.float32)
    denominator = C_OUT * samples * area_total
    weighted = cell_weight[None, :, None] * error
    loss_value = lax.psum(jnp.sum(weighted * error), ("row", "col")) / denominator
    d_predict = (2.0 * weighted / denominator).astype(jnp.bfloat16)
    grad_output_local = reduced_matmul("scd,sco->do", grid_out, d_predict)
    d_grid_out = reduced_matmul("sco,do->scd", d_predict, full_output)
    d_third = silu_grad(third_pre, d_grid_out).astype(jnp.bfloat16)
    grad_decode = reduced_matmul("scd,sce->de", decode_rows, d_third)
    grad_skip = reduced_matmul("scd,sce->de", grid_latent, d_third)
    d_decode = reduced_matmul("sce,de->scd", d_third, complete_latent[4])
    d_skip = reduced_matmul("sce,de->scd", d_third, complete_latent[5])
    d_mesh_next = jnp.einsum("nc,scd->snd", node_match, d_decode, precision=highest)
    residual_branch_gradient = d_mesh_next.astype(jnp.bfloat16)
    branch_gradient_sum = reduced_matmul(
        "lhg,lhj->gj", message_total_reduced, residual_branch_gradient
    )
    message_total_gradient = reduced_matmul(
        "pyk,ck->pyc", residual_branch_gradient, complete_latent[3]
    ).astype(jnp.bfloat16)
    d_block = lax.all_gather(message_total_gradient, "col", axis=1, tiled=True)
    d_edge_message = reduced_matmul("es,ksd->ked", receiver_match, d_block)
    d_edge_pre = silu_grad(edge_pre, d_edge_message / DEG)
    d_sender_part = add_into_rows(sender_match, d_edge_pre)
    d_receiver_part = add_into_rows(receiver_match, d_edge_pre)
    sender_gradient = lax.psum_scatter(
        d_sender_part.astype(jnp.bfloat16), "row", scatter_dimension=1, tiled=True
    )
    receiver_gradient = lax.psum_scatter(
        d_receiver_part.astype(jnp.bfloat16), "col", scatter_dimension=1, tiled=True
    )
    sender_weight_gradient = reduced_matmul("lhg,lhj->gj", mesh_state_reduced, sender_gradient)
    receiver_weight_gradient = reduced_matmul("lhg,lhj->gj", mesh_state_reduced, receiver_gradient)
    d_mesh = (
        d_mesh_next
        + reduced_matmul("pyk,ck->pyc", sender_gradient, complete_latent[1])
        + reduced_matmul("pyk,ck->pyc", receiver_gradient, complete_latent[2])
    )
    hidden_second_gradient = silu_grad(second_activation_input, d_mesh).astype(jnp.bfloat16)
    encoder_gradient = reduced_matmul("lhg,lhj->gj", average_reduced, hidden_second_gradient)
    node_average_gradient = (
        reduced_matmul("pyk,ck->pyc", hidden_second_gradient, complete_latent[0])
        / node_lower_limit[None, :, None]
    )
    d_grid = d_skip + valid[None, :, None] * pick_rows(cell_match, node_average_gradient)
    d_first = silu_grad(first_pre, d_grid).astype(jnp.bfloat16)
    grad_input_local = reduced_matmul("sci,scd->id", inputs, d_first)
    grad_latent_local = jnp.stack(
        [
            encoder_gradient,
            sender_weight_gradient,
            receiver_weight_gradient,
            branch_gradient_sum,
            grad_decode,
            grad_skip,
        ]
    )
    local_terms = (grad_input_local, grad_latent_local, grad_output_local)
    whole_input, whole_latent, whole_output = lax.psum(
        (local_terms[0], local_terms[1], local_terms[2]), ("row", "col")
    )
    column = lax.axis_index("col")
    width_input = weight_input.shape[1]
    width_latent = weight_latent.shape[1]
    width_output = weight_output.shape[0]
    gradient_input = lax.dynamic_slice_in_dim(whole_input, column * width_input, width_input, 1)
    gradient_latent = lax.dynamic_slice_in_dim(whole_latent, column * width_latent, width_latent, 1)
    gradient_output = lax.dynamic_slice_in_dim(whole_output, column * width_output, width_output, 0)
    return loss_value, gradient_input, gradient_latent, gradient_output


def body(
    mesh,
    inputs,
    targets,
    cell_area,
    cell_count,
    cell_node,
    edge_senders,
    edge_receivers,
    weight_input,
    weight_latent,
    weight_output,
    mean_input,
    mean_latent,
    mean_output,
    square_input,
    square_latent,
    square_output,
):
    given = (inputs, targets, cell_area, cell_count, cell_node, edge_senders, edge_receivers, weight_input, weight_latent, weight_output)
    states = (mean_input, mean_latent, mean_output, square_input, square_latent, square_output)
    step = Step(mesh, inputs.shape[0], inputs.shape[1], weight_latent.shape[2], edge_senders.shape[0], inputs.shape[2])
    if step.fits():
        return kernel_body(mesh, step, *given, *states)
    loss_value, gradient_input, gradient_latent, gradient_output = native_gradients(*given)
    first_input, second_input, update_input = adam_parts(
        weight_input, gradient_input, mean_input, square_input
    )
    first_latent, second_latent, update_latent = adam_parts(
        weight_latent, gradient_latent, mean_latent, square_latent
    )
    first_output, second_output, update_output = adam_parts(
        weight_output, gradient_output, mean_output, square_output
    )
    weight_sums = jnp.concatenate(
        [
            jnp.sum(weight_input * weight_input)[None],
            jnp.sum(weight_latent * weight_latent, axis=(1, 2)),
            jnp.sum(weight_output * weight_output)[None],
        ]
    )
    update_sums = jnp.concatenate(
        [
            jnp.sum(update_input * update_input)[None],
            jnp.sum(update_latent * update_latent, axis=(1, 2)),
            jnp.sum(update_output * update_output)[None],
        ]
    )
    norm_sums = lax.psum(jnp.stack([weight_sums, update_sums]), "col")
    trust_norms = jnp.sqrt(norm_sums)
    ratio = trust_norms[0] / (trust_norms[1] + trust_epsilon)
    master_input = weight_input - learn_rate * ratio[0] * update_input
    master_latent = weight_latent - learn_rate * ratio[1:7][:, None, None] * update_latent
    master_output = weight_output - learn_rate * ratio[7] * update_output
    return (
        loss_value,
        gradient_input,
        gradient_latent,
        gradient_output,
        first_input,
        first_latent,
        first_output,
        second_input,
        second_latent,
        second_output,
        master_input,
        master_latent,
        master_output,
        master_input.astype(jnp.bfloat16),
        master_latent.astype(jnp.bfloat16),
        master_output.astype(jnp.bfloat16),
        trust_norms,
    )


def solution(mesh):
    placed = (
        P(None, ("row", "col"), None),
        P(None, ("row", "col"), None),
        P(("row", "col")),
        P(("row", "col")),
        P(("row", "col")),
        P(("row", "col")),
        P(("row", "col")),
        P(None, "col"),
        P(None, "col", None),
        P("col", None),
        P(None, "col"),
        P(None, "col", None),
        P("col", None),
        P(None, "col"),
        P(None, "col", None),
        P("col", None),
    )
    return jax.shard_map(
        functools.partial(body, mesh),
        mesh=mesh,
        in_specs=placed,
        out_specs=(
            P(),
            P(None, "col"),
            P(None, "col", None),
            P("col", None),
            P(None, "col"),
            P(None, "col", None),
            P("col", None),
            P(None, "col"),
            P(None, "col", None),
            P("col", None),
            P(None, "col"),
            P(None, "col", None),
            P("col", None),
            P(None, "col"),
            P(None, "col", None),
            P("col", None),
            P(),
        ),
        check_vma=False,
    )
```

```python
import functools
import types

import jax
import jax.numpy as jnp
from jax import lax
from jax.experimental import pallas as pl
from jax.experimental.pallas import tpu as pltpu
from jax.sharding import PartitionSpec as P

C_OUT = 83
DEG = 16
MESH_DEV = 64


highest = lax.Precision.HIGHEST
beta_first = 0.5
beta_second = 0.5
adam_epsilon = 1e-08
trust_epsilon = 1e-06
weight_decay = 0.01
learn_rate = 0.1


def silu_grad(pre_act, grad_out):
    sigma = jax.nn.sigmoid(pre_act)
    return grad_out * sigma * (1.0 + pre_act * (1.0 - sigma))


def reduced_matmul(form, left, right):
    return jnp.einsum(form, left, right, preferred_element_type=jnp.float32)


def split_parts(values):
    upper = values.astype(jnp.bfloat16)
    rest = values - upper.astype(jnp.float32)
    middle = rest.astype(jnp.bfloat16)
    lower = (rest - middle.astype(jnp.float32)).astype(jnp.bfloat16)
    return (upper, middle, lower)


def pick_rows(match, values):
    upper, middle, lower = split_parts(values)
    total = reduced_matmul("es,ksd->ked", match, upper)
    total = total + reduced_matmul("es,ksd->ked", match, middle)
    return total + reduced_matmul("es,ksd->ked", match, lower)


def add_into_rows(match, values):
    upper, middle, lower = split_parts(values)
    total = reduced_matmul("es,ked->ksd", match, upper)
    total = total + reduced_matmul("es,ked->ksd", match, middle)
    return total + reduced_matmul("es,ked->ksd", match, lower)


def one_hot_table(indices, count):
    return (indices[:, None] == jnp.arange(count, dtype=jnp.int32)[None, :]).astype(jnp.bfloat16)


def adam_parts(weight, gradient, first, second):
    new_first = beta_first * first + (1.0 - beta_first) * gradient
    new_second = beta_second * second + (1.0 - beta_second) * gradient * gradient
    update = new_first / (jnp.sqrt(new_second) + adam_epsilon) + weight_decay * weight
    return (new_first, new_second, update)


MESH = pl.DeviceIdType.MESH
bf16 = jnp.bfloat16
f32 = jnp.float32
VMEM_ROOM = 63 * 2**20
N_IN = 256
N_OUT = 128
WIRE = ("in", 0, 1, 2, 5, 3, 4, "out")


def sizes_of(n_row, n_col):
    X = n_col // 2
    Y = X if n_row % X == 0 else 1
    return X, Y, n_row // Y


class Place:
    def __init__(self, n_row, n_col):
        self.K = 2
        self.X, self.Y, self.Z = sizes_of(n_row, n_col)
        self.row, self.col = lax.axis_index("row"), lax.axis_index("col")
        self.z, self.y = self.row // self.Y, self.row % self.Y
        self.x, self.k = self.col // 2, self.col % 2

    def to(self, axis, d):
        n = getattr(self, axis.upper())
        return (getattr(self, axis) + d) % n

    def peer(self, axis, d):
        at = {a: getattr(self, a) for a in "zyxk"}
        at[axis] = self.to(axis, d)
        return (at["z"] * self.Y + at["y"], at["x"] * 2 + at["k"])

    def others(self, axis):
        if axis == "col":
            return [(self.row, (self.col + d) % (2 * self.X)) for d in range(1, 2 * self.X)]
        return [((self.row + d) % (self.Y * self.Z), self.col) for d in range(1, self.Y * self.Z)]

    def greet(self):
        sem = pltpu.get_barrier_semaphore()
        peers = self.others("col") + self.others("row")
        for peer in peers:
            pl.semaphore_signal(sem, inc=1, device_id=peer, device_id_type=MESH)
        return sem, len(peers)


def remote(src, dst, send_sem, recv_sem, device):
    return pltpu.make_async_remote_copy(
        src_ref=src,
        dst_ref=dst,
        send_sem=send_sem,
        recv_sem=recv_sem,
        device_id=device,
        device_id_type=MESH,
    )


def ds(start, size):
    if isinstance(start, int):
        return pl.ds(start, size)
    return pl.ds(pl.multiple_of(start, size if size % 128 else 128), size)


def by_rows(count, step, todo):
    def one(i, carry):
        todo(pl.multiple_of(i * step, step))
        return carry

    lax.fori_loop(0, count // step, one, 0)


def mm(a, b):
    return jnp.dot(a, b, preferred_element_type=f32)


def mm_nt(a, b):
    return lax.dot_general(a, b, (((1,), (1,)), ((), ())), preferred_element_type=f32)


def mm_tn(a, b):
    return lax.dot_general(a, b, (((0,), (0,)), ((), ())), preferred_element_type=f32)


def sigmoid(v):
    return 0.5 * jnp.tanh(0.5 * v) + 0.5


def silu(v):
    return v * sigmoid(v)


def silu_slope(v):
    s = sigmoid(v)
    return s * (1.0 + v * (1.0 - s))


def high_low(v):
    high = v.astype(bf16)
    return high, (v - high.astype(f32)).astype(bf16)


class Total:
    AXES = ("col", "row")

    @staticmethod
    def scratch(X, Y, Z):
        many = 2 * X - 1 + Y * Z - 1
        return [pltpu.VMEM((2 * X, 8, 128), f32), pltpu.VMEM((Y * Z, 8, 128), f32)] + [
            pltpu.VMEM((8, 128), f32),
            pltpu.SemaphoreType.DMA((many,)),
            pltpu.SemaphoreType.DMA((many,)),
        ]

    def __init__(self, place, refs):
        self.p, self.bufs, (self.value, self.ss, self.rs) = place, dict(zip(self.AXES, refs[:2])), refs[2:]

    def _copies(self, axis):
        p = self.p
        base = 0 if axis == "col" else 2 * p.X - 1
        here = self.bufs[axis].at[getattr(p, axis)]
        return [remote(here, here, self.ss.at[base + i], self.rs.at[base + i], to) for i, to in enumerate(p.others(axis))]

    def start(self, axis):
        self.bufs[axis][getattr(self.p, axis)] = self.value[...]
        for copy in self._copies(axis):
            copy.start()

    def finish(self, axis):
        for copy in self._copies(axis):
            copy.wait_recv()
        buf = self.bufs[axis]
        value = buf[0]
        for i in range(1, buf.shape[0]):
            value = value + buf[i]
        self.value[...] = value

    def drain(self):
        for axis in self.AXES:
            for copy in self._copies(axis):
                copy.wait_send()


class Reduce:
    def __init__(self, grid, dim, n_col, width, late, order, lender=None, lanes=0):
        self.X, self.Y, self.Z = grid
        self.dim, self.shard, self.late, self.order = dim, dim // n_col, late, order
        self.ry = self.shard // self.Y
        self.rz = self.ry // self.Z
        self.w = width
        self.lender, self.lanes, self.lent = lender, lanes, False

    def scratch(self):
        X, Y, Z, w = self.X, self.Y, self.Z, self.w
        many = X + (X - 1) + 2 * (Y - 1) + 2 * (Z - 1)
        along_x = (X - 1, 1, self.shard, w) if self.order == "xy" else (X - 1, 1, self.ry, w)
        along_y = (Y - 1, 1, self.ry, w) if self.order == "xy" else (Y - 1, X, self.ry, w)
        return [
            *([] if self.lender else [pltpu.VMEM((self.dim, w), f32)]),
            pltpu.VMEM((X, self.shard, w), f32),
            pltpu.VMEM(along_x, bf16),
            pltpu.VMEM(along_x, bf16),
            pltpu.VMEM(along_y, bf16),
            pltpu.VMEM(along_y, bf16),
            pltpu.VMEM((Z - 1, self.rz, w), self.late),
            pltpu.VMEM((Z - 1, self.rz, w), self.late),
            pltpu.VMEM((self.rz, w), f32),
            pltpu.VMEM((self.shard, w), self.late),
            pltpu.SemaphoreType.DMA((many,)),
            pltpu.SemaphoreType.DMA((many,)),
        ]

    def bind(self, place, refs):
        if self.lender:
            refs = (self.lender.full.at[:, self.lanes : self.lanes + self.w], *refs)
        (self.full, self.cr, self.xs, self.xr, self.ys, self.yr, self.zs, self.zin, self.piece, self.out, self.ss, self.rs) = refs
        self.p = place

    def lend(self):
        for copy in self.copies(0):
            copy.wait_send()

    def rows_of(self, x, k):
        return (2 * x + k) * self.shard

    def place_z(self):
        return pl.ds(pl.multiple_of(self.p.y * self.ry + self.p.z * self.rz, 16), self.rz)

    def copies(self, stage):
        p, X, Y, Z = self.p, self.X, self.Y, self.Z
        first_x = self.order == "xy"
        x_base, y_base = (X, 2 * X - 1) if first_x else (X + Y - 1, X)
        base = (0, x_base if first_x else y_base, y_base if first_x else x_base, 2 * X + Y - 2, 2 * X + Y + Z - 3, 2 * X + Y + 2 * Z - 4)[stage]
        if stage == 0:
            many = [(self.full.at[ds(self.rows_of(x, 1 - p.k), self.shard), :], self.cr.at[x], p.peer("k", 1)) for x in range(X)]
        elif stage == (1 if first_x else 2):
            many = [(self.xs.at[d - 1], self.xr.at[d - 1], p.peer("x", d)) for d in range(1, X)]
        elif stage == (2 if first_x else 1):
            many = [(self.ys.at[d - 1], self.yr.at[d - 1], p.peer("y", d)) for d in range(1, Y)]
        elif stage == 3:
            many = [(self.zs.at[d - 1], self.zin.at[d - 1], p.peer("z", d)) for d in range(1, Z)]
        elif stage == 4:
            here = self.out.at[self.place_z(), :]
            many = [(here, here, p.peer("z", d)) for d in range(1, Z)]
        else:
            here = self.out.at[pl.ds(pl.multiple_of(p.y * self.ry, 16), self.ry), :]
            many = [(here, here, p.peer("y", d)) for d in range(1, Y)]
        return [remote(src, dst, self.ss.at[base + i], self.rs.at[base + i], to) for i, (src, dst, to) in enumerate(many)]

    def sum_core(self, x, at, n=16):
        mine = self.full[pl.ds(pl.multiple_of(self.rows_of(x, self.p.k) + at, 16), n), :]
        return mine + self.cr[x, pl.ds(at, n), :]

    def sum_first(self, x, y, at):
        rows = pl.multiple_of(y * self.ry + at, 16)
        value = self.sum_core(x, rows)
        if self.order == "xy":
            for d in range(1, self.X):
                value = value + self.xr[d - 1, 0, pl.ds(rows, 16), :].astype(f32)
        else:
            for d in range(1, self.Y):
                value = value + self.yr[d - 1, x, pl.ds(at, 16), :].astype(f32)
        return value

    def stage(self, s):
        p, X, Y, Z = self.p, self.X, self.Y, self.Z
        if s:
            for copy in self.copies(s - 1):
                copy.wait_recv()
        if s == 1 and self.order == "xy":
            for d in range(1, X):
                to = p.to("x", d)

                def one(at, to=to, d=d):
                    self.xs[d - 1, 0, pl.ds(at, 16), :] = self.sum_core(to, at).astype(bf16)

                by_rows(self.shard, 16, one)
        elif s == 1:
            for d in range(1, Y):
                base = p.to("y", d) * self.ry

                def one(at, base=base, d=d):
                    for x in range(X):
                        self.ys[d - 1, x, pl.ds(at, 16), :] = self.sum_core(x, pl.multiple_of(base + at, 16)).astype(bf16)

                by_rows(self.ry, 16, one)
        elif s == 2:
            if self.order == "xy":
                for d in range(1, Y):

                    def one(at, to=p.to("y", d), d=d):
                        self.ys[d - 1, 0, pl.ds(at, 16), :] = self.sum_first(p.x, to, at).astype(bf16)

                    by_rows(self.ry, 16, one)
            else:
                for d in range(1, X):

                    def one(at, to=p.to("x", d), d=d):
                        self.xs[d - 1, 0, pl.ds(at, 16), :] = self.sum_first(to, p.y, at).astype(bf16)

                    by_rows(self.ry, 16, one)

            def mine(at):
                self.cr[p.x, pl.ds(pl.multiple_of(p.y * self.ry + at, 16), 16), :] = self.sum_first(p.x, p.y, at)

            by_rows(self.ry, 16, mine)
        elif s == 3:

            def total(z):
                rows = pl.multiple_of(z * self.rz, 16)
                value = self.cr[p.x, pl.ds(pl.multiple_of(p.y * self.ry + rows, 16), self.rz), :]
                arrived = self.yr if self.order == "xy" else self.xr
                for d in range(1, Y if self.order == "xy" else X):
                    value = value + arrived[d - 1, 0, pl.ds(rows, self.rz), :].astype(f32)
                return value

            for d in range(1, Z):
                self.zs[d - 1] = total(p.to("z", d)).astype(self.late)
            self.piece[...] = total(p.z)
        elif s == 4:
            value = self.piece[...]
            for d in range(1, Z):
                value = value + self.zin[d - 1].astype(f32)
            self.piece[...] = value
            self.out[self.place_z(), :] = value.astype(self.late)
        if s < STAGES - 1:
            for copy in self.copies(s):
                copy.start()

    def drain(self):
        for s in range(1 if self.lent else 0, STAGES - 1):
            for copy in self.copies(s):
                copy.wait_send()


STAGES = 7


class Step:
    def __init__(self, mesh, samples, slots, dim, edges, c_in):
        self.n_row, self.n_col = mesh.shape["row"], mesh.shape["col"]
        self.grid = sizes_of(self.n_row, self.n_col)
        self.S, self.C, self.D, self.E, self.c_in = samples, slots, dim, edges, c_in
        self.N = MESH_DEV
        self.SH = dim // self.n_col
        self.R, self.Q = self.n_row * self.N, self.n_col * self.N
        chunk = functools.partial(Reduce, self.grid, dim, self.n_col)
        skips, decoders = chunk(dim + N_OUT, f32, "xy"), chunk(2 * dim, bf16, "xy")
        skips.lent = decoders.lent = True
        self.chunks = [
            skips,
            decoders,
            chunk(dim, bf16, "xy", decoders, 0),
            chunk(dim, bf16, "xy", decoders, dim),
            chunk(dim, bf16, "yx", skips, 0),
            chunk(N_IN, f32, "yx"),
        ]
        X, Y, Z = self.grid
        S, C, D, E, N, R, Q = self.S, self.C, self.D, self.E, self.N, self.R, self.Q
        vm = pltpu.VMEM
        dma = lambda *shape: pltpu.SemaphoreType.DMA(shape)
        self.shapes = dict(
            wib=vm((D, N_IN), bf16),
            wlb=vm((6, D, D), bf16),
            wob=vm((D, N_OUT), bf16),
            nm=vm((N, C), bf16),
            nv=vm((N, C), bf16),
            cm=vm((C, N), bf16),
            cmv=vm((C, N), bf16),
            cw=vm((C, 128), f32),
            cnt=vm((N, 128), f32),
            fx=vm((N_IN, S, C), f32),
            xb=vm((S * C, N_IN), bf16),
            tb=vm((S * C, N_OUT), bf16),
            fp=vm((S * C, D), f32),
            gl=vm((S * C, D), bf16),
            tp=vm((S * C, D), f32),
            go=vm((S * C, D), bf16),
            dp=vm((S * C, N_OUT), bf16),
            dt=vm((S * C, D), bf16),
            av=vm((S * N, D), bf16),
            sp=vm((S * N, D), f32),
            mlb=vm((S * N, D), bf16),
            agb=vm((S * N, D), bf16),
            mnb=vm((S * N, D), bf16),
            sg=vm((S * N, D), f32),
            dmn=vm((S * N, D), f32),
            dsb=vm((S * N, D), bf16),
            drb=vm((S * N, D), bf16),
            d2b=vm((S * N, D), bf16),
            sr=vm((S, R + Q, D), bf16),
            oh=vm((E, R + Q), bf16),
            oht=vm((R + Q, E), bf16),
            ep=vm((S, E, D), f32),
            ac=vm((E, D), bf16),
            tmp=vm((R + Q, D), f32),
            part=vm((S, Q, D), f32),
            pcr=vm((S, X, N, D), f32),
            pxs=vm((S, X - 1, N, D), bf16),
            pxr=vm((S, X - 1, N, D), bf16),
            da=vm((S, Q, D), bf16),
            down=vm((S, Z, N, D), f32),
            dys=vm((S, Y - 1, Z, N, D), bf16),
            dyr=vm((S, Y - 1, Z, N, D), bf16),
            dzs=vm((S, Z - 1, N, D), bf16),
            dzr=vm((S, Z - 1, N, D), bf16),
            loss=vm((8, 128), f32),
            l_sem=dma(24),
            w_ss=dma(8, 1 + 2 * (X - 1)),
            w_rs=dma(8, 1 + 2 * (X - 1)),
            mz_ss=dma(S, Z - 1),
            mz_rs=dma(S, Z - 1),
            my_ss=dma(S, Y - 1, Z),
            my_rs=dma(S, Y - 1, Z),
            mr_ss=dma(S, 1 + 2 * (X - 1)),
            mr_rs=dma(S, 1 + 2 * (X - 1)),
            pk_ss=dma(2, S, X),
            pk_rs=dma(2, S, X),
            px_ss=dma(2, S, X - 1),
            px_rs=dma(2, S, X - 1),
            a_ss=dma(S, 1 + 2 * (X - 1)),
            a_rs=dma(S, 1 + 2 * (X - 1)),
            dy_ss=dma(S, Y - 1, Z),
            dy_rs=dma(S, Y - 1, Z),
            dz_ss=dma(S, Z - 1),
            dz_rs=dma(S, Z - 1),
        )

    def fits(self):
        X, Y, Z = self.grid
        return self.SH % (16 * Y * Z) == 0 and self.SH % 128 == 0 and self.vmem_bytes() < VMEM_ROOM

    def vmem_bytes(self):
        total = 0
        for s in [*self.shapes.values(), *[s for c in self.chunks for s in c.scratch()]]:
            dtype = getattr(s, "dtype", None)
            if dtype in (jnp.dtype(f32), jnp.dtype(bf16)):
                size = jnp.dtype(dtype).itemsize
                for n in s.shape[:-1]:
                    size *= n
                total += size * -(-s.shape[-1] // 128) * 128
        return total

    def scratch(self):
        total = Total.scratch(*self.grid)
        return [*self.shapes.values(), *total * 2, *[s for c in self.chunks for s in c.scratch()]]

    def kernel(self, count, x, tgt, area, node, snd, rcv, wi, wl, wo, mi, mal, mo, si, sal, so, *refs):
        S, C, D, E, N, R, Q, SH = self.S, self.C, self.D, self.E, self.N, self.R, self.Q, self.SH
        X, Y, Z = self.grid
        (g_in, g_out, g_skip, g_two, g_three, g_four, stats), refs = refs[:7], refs[7:]
        v = types.SimpleNamespace(**dict(zip(self.shapes, refs)))
        refs = refs[len(self.shapes) :]
        p = Place(self.n_row, self.n_col)
        area_sum, stat_sum = Total(p, refs[:5]), Total(p, refs[5:10])
        refs = refs[10:]
        for chunk in self.chunks:
            many = len(chunk.scratch())
            chunk.bind(p, refs[:many])
            refs = refs[many:]

        def weight_rows(i, col):
            which = WIRE[i]
            whole = v.wib if which == "in" else v.wob if which == "out" else v.wlb.at[which]
            return whole.at[ds(col * SH, SH), :]

        def w_copy(i, j, d=0):
            rows = weight_rows(i, 2 * p.to("x", -d) + p.k if j == 2 else p.col)
            at = (0, d, X - 1 + d)[j]
            device = p.peer("x", d) if j == 1 else p.peer("k", 1)
            return remote(rows, rows, v.w_ss.at[i, at], v.w_rs.at[i, at], device)

        hops = range(1, X)

        def w_forward(i):
            for d in hops:
                w_copy(i, 1, d).wait_recv()
                w_copy(i, 2, d).start()

        def w_get(i):
            w_copy(i, 0).wait_recv()
            for d in hops:
                w_copy(i, 2, d).wait_recv()

        W = lambda which: v.wlb[which]
        barrier = p.greet()
        own = ds(p.col * SH, SH)
        latents = [w for w in WIRE if isinstance(w, int)]
        loads = {m: pltpu.make_async_copy(wl.at[m], v.fp.at[m * SH : (m + 1) * SH, :], v.l_sem.at[m]) for m in latents}
        for load in loads.values():
            load.start()

        def turned(ref, n):
            v.tmp[0:n, 0:SH] = jnp.zeros((n, SH), f32)
            v.tmp[0 : ref.shape[0], 0:SH] = ref[...]
            return jnp.transpose(v.tmp[0:n, 0:SH])

        def w_ready(i):
            m = WIRE[i]
            if m == "in":
                v.wib[own, :] = turned(wi, N_IN).astype(bf16)
            elif m == "out":
                v.wob[own, :] = turned(wo, N_OUT).astype(bf16)
            else:
                loads[m].wait()
                v.wlb[m, own, :] = v.fp[m * SH : (m + 1) * SH, :].astype(bf16)

        def w_depart(*items):
            for i in items:
                w_copy(i, 0).start()
                for d in hops:
                    w_copy(i, 1, d).start()

        w_ready(0)
        w_ready(1)
        pl.semaphore_wait(*barrier)
        w_depart(0, 1)
        for i in range(2, 8):
            w_ready(i)
            if i < 4:
                w_depart(i)
        used = count[0]
        area_row = area[...].reshape(1, C) * (lax.broadcasted_iota(jnp.int32, (1, C), 1) < used).astype(f32)
        area_sum.value[...] = jnp.broadcast_to(jnp.sum(area_row), (8, 128))
        area_sum.start("col")

        def by_cell(ref, n, out):
            have = ref.shape[0]
            v.fx[0:have] = ref[...].astype(f32)
            v.fx[have:n] = jnp.zeros((n - have, S, C), f32)
            for s in range(S):
                out[s * C : (s + 1) * C, :] = jnp.transpose(v.fx[0:n, s, :]).astype(bf16)

        by_cell(x, N_IN, v.xb)

        node_row = node[...].reshape(1, C)
        match = (lax.broadcasted_iota(jnp.int32, (N, C), 0) == node_row).astype(f32)
        v.nm[...] = match.astype(bf16)
        match = match * (lax.broadcasted_iota(jnp.int32, (N, C), 1) < used).astype(f32)
        v.nv[...] = match.astype(bf16)
        v.cnt[...] = jnp.broadcast_to(jnp.maximum(jnp.sum(match, axis=1, keepdims=True), 1.0), (N, 128))
        node_col = jnp.transpose(jnp.broadcast_to(node_row, (128, C)))
        v.cw[...] = jnp.transpose(jnp.broadcast_to(area_row, (128, C)))
        match = (lax.broadcasted_iota(jnp.int32, (C, 128), 1) == node_col).astype(f32)
        v.cm[...] = match[:, :N].astype(bf16)
        match = match * (lax.broadcasted_iota(jnp.int32, (C, 128), 0) < used).astype(f32)
        v.cmv[...] = match[:, :N].astype(bf16)

        def table(index, base, rows):
            def down(at):
                hit = lax.broadcasted_iota(jnp.int32, (128, E), 0) + at == index
                v.oht[pl.ds(pl.multiple_of(base + at, 128), 128), :] = hit.astype(f32).astype(bf16)

            by_rows(rows, 128, down)
            column = jnp.transpose(jnp.broadcast_to(index, (128, E)))
            for at in range(0, rows, 128):
                hit = lax.broadcasted_iota(jnp.int32, (E, 128), 1) + at == column
                v.oh[:, base + at : base + at + 128] = hit.astype(f32).astype(bf16)

        v.dp[...] = jnp.zeros((S * C, N_OUT), bf16)
        v.loss[...] = jnp.zeros((8, 128), f32)

        def encode(xx, s):
            at, here, lanes = ds(s * C, C), ds(s * N, N), ds(xx * 2 * SH, 2 * SH)
            pre = mm_nt(v.xb[at, :], v.wib[lanes, :])
            v.fp[at, lanes] = pre
            v.gl[at, lanes] = silu(pre).astype(bf16)
            v.av[here, lanes] = (mm(v.nv[...], v.gl[at, lanes]) / v.cnt[:, 0:1]).astype(bf16)

        def encode_all(xx):
            def one(s, carry):
                encode(xx, s)
                return carry

            lax.fori_loop(0, S, one, 0)

        w_copy(0, 0).wait_recv()
        encode_all(p.x)
        w_forward(0)
        by_cell(tgt, N_OUT, v.tb)
        table(snd[...], 0, R)
        table(rcv[...], R, Q)
        for d in hops:
            w_copy(0, 2, d).wait_recv()
            encode_all(p.to("x", -d))
        w_forward(1)
        w_get(1)
        pre = mm(v.av[...], W(0))
        v.sp[...] = pre
        v.mlb[...] = silu(pre).astype(bf16)

        def mz(s, d):
            rows = v.sr.at[s, ds(p.row * N, N), :]
            return remote(rows, rows, v.mz_ss.at[s, d - 1], v.mz_rs.at[s, d - 1], p.peer("z", d))

        def my(s, d, e):
            rows = v.sr.at[s, ds((p.to("z", -e) * Y + p.y) * N, N), :]
            return remote(rows, rows, v.my_ss.at[s, d - 1, e], v.my_rs.at[s, d - 1, e], p.peer("y", d))

        def mr(s, j, d=0):
            col = 2 * p.to("x", -d) + p.k if j == 2 else p.col
            rows = v.sr.at[s, ds(R + col * N, N), :]
            at = (0, d, X - 1 + d)[j]
            return remote(rows, rows, v.mr_ss.at[s, at], v.mr_rs.at[s, at], p.peer("x", d) if j == 1 else p.peer("k", 1))

        for s in range(S):
            v.sr[s, ds(p.row * N, N), :] = v.mlb[s * N : (s + 1) * N, :]
            v.sr[s, ds(R + p.col * N, N), :] = v.mlb[s * N : (s + 1) * N, :]

        def depart(s):
            for d in range(1, Z):
                mz(s, d).start()

        depart(0)
        for s in range(S):
            for d in range(1, Y):
                my(s, d, 0).start()
            mr(s, 0).start()
            for d in hops:
                mr(s, 1, d).start()
            if s == 1:
                w_depart(4)
        w_depart(5, 6, 7)
        w_forward(2)
        w_forward(3)
        depart(1)
        w_get(2)
        w_get(3)

        def skip(at):
            v.tp[pl.ds(at, 512), :] = mm(v.gl[pl.ds(at, 512), :], W(5))

        def pk(t, s, xx):
            rows = v.part.at[s, ds((2 * xx + 1 - p.k) * N, N), :]
            return remote(rows, v.pcr.at[s, xx], v.pk_ss.at[t, s, xx], v.pk_rs.at[t, s, xx], p.peer("k", 1))

        def px(t, s, d):
            return remote(v.pxs.at[s, d - 1], v.pxr.at[s, d - 1], v.px_ss.at[t, s, d - 1], v.px_rs.at[t, s, d - 1], p.peer("x", d))

        def col_second(t, s):
            for xx in range(X):
                pk(t, s, xx).wait_recv()
            for d in hops:
                px_to = p.to("x", d)
                mine = v.part[s, ds((2 * px_to + p.k) * N, N), :]
                v.pxs[s, d - 1] = (mine + v.pcr[s, px_to]).astype(bf16)
                px(t, s, d).start()

        def col_last(t, s):
            total = v.part[s, ds(p.col * N, N), :] + v.pcr[s, p.x]
            for d in hops:
                px(t, s, d).wait_recv()
                total = total + v.pxr[s, d - 1].astype(f32)
            return total

        def nearest(j):
            steps = [(n + 1) // 2 * (1 if n % 2 else -1) for n in range(1, 2 * Z - 1)]
            taken, found = jnp.int32(0), jnp.int32(0)
            for step in steps:
                inside = ((p.z - step >= 0) & (p.z - step < Z)).astype(jnp.int32)
                found = found + jnp.where((taken == j) & (inside == 1), step, 0)
                taken = taken + inside
            return (found + Z) % Z

        def arrive(s):
            for j in range(Z - 1):
                d = nearest(j)
                mz(s, d).wait_recv()
                for b in range(1, Y):
                    my(s, b, d).start()
            for d in hops:
                mr(s, 1, d).wait_recv()
                mr(s, 2, d).start()

        def edges(s):
            for b in range(1, Y):
                for e in range(Z):
                    my(s, b, e).wait_recv()
            mr(s, 0).wait_recv()
            for d in hops:
                mr(s, 2, d).wait_recv()
            for d in range(1, Z):
                mz(s, d).wait_send()
            for b in range(1, Y):
                for e in range(Z):
                    my(s, b, e).wait_send()
            mr(s, 0).wait_send()
            for d in hops:
                mr(s, 1, d).wait_send()
                mr(s, 2, d).wait_send()
            v.sr[s, 0:R, :] = mm(v.sr[s, 0:R, :], W(1)).astype(bf16)
            v.sr[s, R : R + Q, :] = mm(v.sr[s, R : R + Q, :], W(2)).astype(bf16)

            def pick(at):
                pre = mm(v.oh[pl.ds(at, 512), :], v.sr[s])
                v.ep[s, pl.ds(at, 512), :] = pre
                v.ac[pl.ds(at, 512), :] = silu(pre).astype(bf16)

            by_rows(E, 512, pick)
            v.part[s] = mm(v.oht[R:, :], v.ac[...])
            for xx in range(X):
                pk(0, s, xx).start()

        def ac(s, j, d=0):
            col = 2 * p.to("x", -d) + p.k if j == 2 else p.col
            rows = v.da.at[s, ds(col * N, N), :]
            at = (0, d, X - 1 + d)[j]
            return remote(rows, rows, v.a_ss.at[s, at], v.a_rs.at[s, at], p.peer("x", d) if j == 1 else p.peer("k", 1))

        def decode(s):
            at, here = ds(s * C, C), ds(s * N, N)
            v.agb[here, :] = (col_last(0, s) * (1.0 / DEG)).astype(bf16)
            v.mnb[here, :] = (silu(v.sp[here, :]) + mm(v.agb[here, :], W(3))).astype(bf16)
            pl.when(s == 0)(functools.partial(area_sum.finish, "row"))
            scale = 1.0 / (C_OUT * S * area_sum.value[0:1, 0:1])
            rows = mm(v.cm[...], v.mnb[here, :]).astype(bf16)
            pre = mm(rows, W(4)) + v.tp[at, :]
            v.tp[at, :] = pre
            v.go[at, :] = silu(pre).astype(bf16)
            error = mm(v.go[at, :], v.wob[...])[:, :C_OUT] - v.tb[at, 0:C_OUT].astype(f32)
            weighted = v.cw[:, :C_OUT] * error
            v.loss[0:1, 0:C_OUT] = v.loss[0:1, 0:C_OUT] + jnp.sum(weighted * error, axis=0, keepdims=True)
            v.dp[at, 0:C_OUT] = (2.0 * weighted * scale).astype(bf16)
            v.dt[at, :] = (silu_slope(v.tp[at, :]) * mm_nt(v.dp[at, :], v.wob[...])).astype(bf16)
            grad = mm(v.nm[...], v.dt[at, :])
            v.sg[here, :] = grad
            grad = mm_nt(jnp.concatenate(high_low(grad), axis=0), W(4))
            grad = grad[:N] + grad[N:]
            v.dmn[here, :] = grad
            v.da[s, ds(p.col * N, N), :] = mm_nt(grad.astype(bf16), W(3)).astype(bf16)
            ac(s, 0).start()
            for d in hops:
                ac(s, 1, d).start()

        def dy(s, d, e):
            return remote(v.dys.at[s, d - 1, e], v.dyr.at[s, d - 1, e], v.dy_ss.at[s, d - 1, e], v.dy_rs.at[s, d - 1, e], p.peer("y", d))

        def dz(s, d):
            return remote(v.dzs.at[s, d - 1], v.dzr.at[s, d - 1], v.dz_ss.at[s, d - 1], v.dz_rs.at[s, d - 1], p.peer("z", d))

        def pass_on(s):
            for d in hops:
                ac(s, 1, d).wait_recv()
                ac(s, 2, d).start()

        def edges_back(s):
            ac(s, 0).wait_recv()
            for d in hops:
                ac(s, 2, d).wait_recv()
            for xx in range(X):
                pk(0, s, xx).wait_send()
            for d in hops:
                px(0, s, d).wait_send()

            def pick(at):
                grad = mm(v.oh[pl.ds(at, 512), R:], v.da[s])
                v.ac[pl.ds(at, 512), :] = (silu_slope(v.ep[s, pl.ds(at, 512), :]) * grad * (1.0 / DEG)).astype(bf16)

            by_rows(E, 512, pick)
            v.tmp[...] = mm(v.oht[...], v.ac[...])
            for e in (*range(1, Z), 0):
                to = p.to("z", e)
                for d in range(1, Y):
                    v.dys[s, d - 1, e] = v.tmp[ds((to * Y + p.to("y", d)) * N, N), :].astype(bf16)
                    dy(s, d, e).start()
                v.down[s, e] = v.tmp[ds((to * Y + p.y) * N, N), :]
            v.part[s] = v.tmp[R:, :]
            for xx in range(X):
                pk(1, s, xx).start()

        def row_sum(s, e):
            total = v.down[s, e]
            for d in range(1, Y):
                dy(s, d, e).wait_recv()
                total = total + v.dyr[s, d - 1, e].astype(f32)
            return total

        def row_second(s):
            for e in range(1, Z):
                v.dzs[s, e - 1] = row_sum(s, e).astype(bf16)
                dz(s, e).start()

        def encode_back(s):
            at, here = ds(s * C, C), ds(s * N, N)
            v.drb[here, :] = col_last(1, s).astype(bf16)
            total = row_sum(s, 0)
            for d in range(1, Z):
                dz(s, d).wait_recv()
                total = total + v.dzr[s, d - 1].astype(f32)
            v.dsb[here, :] = total.astype(bf16)
            whole = v.dmn[here, :] + mm_nt(v.dsb[here, :], W(1)) + mm_nt(v.drb[here, :], W(2))
            v.d2b[here, :] = (silu_slope(v.sp[here, :]) * whole).astype(bf16)
            high, low = high_low(mm_nt(v.d2b[here, :], W(0)) / v.cnt[:, 0:1])
            grad = v.tp[at, :] + mm(v.cmv[...], high) + mm(v.cmv[...], low)
            v.dt[at, :] = (silu_slope(v.fp[at, :]) * grad).astype(bf16)

        skips, decoders, senders, receivers, encoders, inputs = self.chunks

        def decoder_gradients():
            skips.full[:, 0:D] = mm_tn(v.gl[...], v.dt[...])
            skips.full[:, D : D + N_OUT] = mm_tn(v.go[...], v.dp[...])
            skips.stage(0)
            high, low = high_low(v.sg[...])
            decoders.full[:, 0:D] = mm_tn(v.mnb[...], high) + mm_tn(v.mnb[...], low)
            decoders.full[:, D : 2 * D] = mm_tn(v.agb[...], v.dmn[...].astype(bf16))
            decoders.stage(0)

        def skip_back():
            def one(at):
                v.tp[pl.ds(at, 512), :] = mm_nt(v.dt[pl.ds(at, 512), :], W(5))

            by_rows(S * C, 512, one)

        def weights_rest():
            for i in (5, 6, 7):
                w_forward(i)
            area_sum.finish("col")
            area_sum.start("row")
            for i in (5, 6, 7):
                w_get(i)

        def partials_back(s):
            col_second(1, s)
            row_second(s)

        stage = lambda chunk, n: functools.partial(chunk.stage, n)
        line = [
            (edges, 0),
            (edges_back, 3),
            (stage(skips, 1), S + 2, None),
            (stage(decoders, 1), S + 2, None),
            (arrive, -2),
            (functools.partial(col_second, 0), 0),
            (weights_rest, 1, None),
            (decoder_gradients, S + 1, None),
            (lambda s: pl.when(s < S // 2)(functools.partial(pass_on, s)), 2),
            (decode, 1),
            (lambda s: pl.when(s >= S // 2)(functools.partial(pass_on, s)), 2),
            (partials_back, 4),
            (skip_back, S + 2, None),
            (stage(skips, 3), S + 5, None),
            (encode_back, 6),
            (stage(skips, 2), S + 3, None),
            (stage(decoders, 2), S + 3, None),
        ]
        arrive(0)
        depart(2)
        w_forward(4)
        w_get(4)
        by_rows(S * C, 512, skip)
        arrive(1)
        depart(3)

        def turn(i, carry):
            for todo, behind, *once in line:
                if once:
                    pl.when(i == behind)(todo)
                else:
                    pl.when((i >= max(behind, 0)) & (i < S + behind))(functools.partial(todo, i - behind))
            return carry

        lax.fori_loop(0, S + 6, turn, 0)
        states = [
            pltpu.make_async_copy(a.at[m], v.ep.at[j, m * SH : (m + 1) * SH, :], v.l_sem.at[6 + 6 * j + m])
            for j, a in enumerate((wl, mal, sal))
            for m in range(6)
        ]
        for load in states:
            load.start()
        decoders.lend()
        skips.lend()
        senders.full[...] = mm_tn(v.mlb[...], v.dsb[...])
        senders.stage(0)
        receivers.full[...] = mm_tn(v.mlb[...], v.drb[...])
        receivers.stage(0)
        encoders.full[...] = mm_tn(v.av[...], v.d2b[...])
        encoders.stage(0)
        inputs.full[...] = mm_tn(v.dt[...], v.xb[...])
        inputs.stage(0)
        senders.stage(1)
        encoders.stage(1)
        receivers.stage(1)
        inputs.stage(1)
        decoders.stage(3)

        for load in states:
            load.wait()
        spare = v.ep.at[3]
        for j, (a, b) in enumerate(((wi, wo), (mi, mo), (si, so))):
            spare[j * SH : (j + 1) * SH, 0:N_IN] = turned(a, N_IN)
            spare[j * SH : (j + 1) * SH, N_IN : N_IN + N_OUT] = turned(b, N_OUT)
        lane = lax.broadcasted_iota(jnp.int32, (8, 128), 1)
        row = lax.broadcasted_iota(jnp.int32, (8, 128), 0)
        stat_sum.value[...] = jnp.where(row == 2, jnp.sum(v.loss[...]), 0.0)

        def note(j, gradient, at, lanes):
            held = [buf[pl.ds(pl.multiple_of(start + p.y * (SH // Y) + p.z * (SH // Y // Z), 16), SH // Y // Z), lanes] for buf, start in at]
            _, _, update = adam_parts(held[0], gradient, held[1], held[2])
            for i, what in enumerate((held[0], update)):
                stat_sum.value[...] += jnp.where((row == i) & (lane == j), jnp.sum(what * what), 0.0)

        def note_latent(m, gradient):
            note(1 + m, gradient, [(v.ep.at[j], m * SH) for j in range(3)], slice(None))

        edge = [(spare, j * SH) for j in range(3)]
        skips.stage(4)
        note_latent(5, skips.piece[:, 0:D])
        note(7, skips.piece[:, D : D + N_OUT], edge, slice(N_IN, N_IN + N_OUT))
        senders.stage(2)
        encoders.stage(2)
        receivers.stage(2)
        inputs.stage(2)
        senders.stage(3)
        encoders.stage(3)
        decoders.stage(4)
        note_latent(4, decoders.piece[:, 0:D])
        note_latent(3, decoders.piece[:, D : 2 * D])
        inputs.stage(3)
        receivers.stage(3)
        skips.stage(5)
        senders.stage(4)
        note_latent(1, senders.piece[...])
        encoders.stage(4)
        note_latent(0, encoders.piece[...])
        inputs.stage(4)
        note(0, inputs.piece[...], edge, slice(0, N_IN))
        receivers.stage(4)
        note_latent(2, receivers.piece[...])
        stat_sum.start("col")
        decoders.stage(5)
        skips.stage(6)
        g_skip[...] = skips.out[:, :D]
        g_out[...] = jnp.transpose(skips.out[:, D : D + N_OUT])[: g_out.shape[0], :]
        senders.stage(5)
        encoders.stage(5)
        stat_sum.finish("col")
        stat_sum.start("row")
        inputs.stage(5)
        receivers.stage(5)
        decoders.stage(6)
        g_two[...] = decoders.out[...]
        senders.stage(6)
        g_three[:, 0:D] = senders.out[...]
        encoders.stage(6)
        g_four[...] = encoders.out[...]
        inputs.stage(6)
        g_in[...] = jnp.transpose(inputs.out[...])[: g_in.shape[0], :]
        receivers.stage(6)
        g_three[:, D : 2 * D] = receivers.out[...]
        stat_sum.finish("row")
        stats[...] = jnp.where(row < 2, stat_sum.value[...], stat_sum.value[...] / (C_OUT * S * area_sum.value[...]))

        for i in range(8):
            w_copy(i, 0).wait_send()
            for d in hops:
                w_copy(i, 1, d).wait_send()
                w_copy(i, 2, d).wait_send()
        for s in range(S):
            for d in range(1, Z):
                dz(s, d).wait_send()
            for d in range(1, Y):
                for e in range(Z):
                    dy(s, d, e).wait_send()
            ac(s, 0).wait_send()
            for d in hops:
                ac(s, 1, d).wait_send()
                ac(s, 2, d).wait_send()
            for xx in range(X):
                pk(1, s, xx).wait_send()
            for d in hops:
                px(1, s, d).wait_send()
        area_sum.drain()
        stat_sum.drain()
        for chunk in self.chunks:
            chunk.drain()

    def __call__(self, count, x, tgt, area, node, snd, rcv, *states):
        vm, hbm = pl.BlockSpec(memory_space=pltpu.VMEM), pl.BlockSpec(memory_space=pl.ANY)
        D, SH = self.D, self.SH
        outs = [(states[0].shape, f32), (states[2].shape, f32), ((SH, D), f32), ((SH, 2 * D), bf16), ((SH, 2 * D), bf16), ((SH, D), bf16), ((8, 128), f32)]
        return pl.pallas_call(
            self.kernel,
            out_shape=[jax.ShapeDtypeStruct(*o) for o in outs],
            in_specs=[pl.BlockSpec(memory_space=pltpu.SMEM)] + [vm] * 6 + [vm, hbm, vm] * 3,
            out_specs=[vm] * 7,
            scratch_shapes=self.scratch(),
            name="train_step",
            compiler_params=pltpu.CompilerParams(collective_id=0, has_side_effects=True, vmem_limit_bytes=67043328),
        )(count, x, tgt, area, node, snd, rcv, *states)


def update_kernel(g_in, g_out, g_skip, g_two, g_three, g_four, stats, wi, wl, wo, mi, mal, mo, si, sal, so, *refs):
    loss, *outs, norms = refs[:17]
    in_buf, out_buf, low_buf, in_sem, out_sem = refs[17:]
    SH, D = g_skip.shape
    loads = [[pltpu.make_async_copy(a.at[m], in_buf.at[j, m], in_sem.at[j, m]) for j, a in enumerate((wl, mal, sal))] for m in range(6)]
    order = (5, 4, 3, 2, 1, 0)
    for m in order:
        for load in loads[m]:
            load.start()
    root = jnp.sqrt(stats[...])
    norms[...] = root[0:2, 0:8]
    loss[...] = stats[2:3, 0:1]

    def step(j, weight, gradient, mean, square):
        first, second, update = adam_parts(weight, gradient, mean, square)
        ratio = root[0:1, j : j + 1] / (root[1:2, j : j + 1] + trust_epsilon)
        master = weight - learn_rate * ratio * update
        return gradient, first, second, master, master.astype(bf16)

    grads = {5: (g_skip, 0), 4: (g_two, 0), 3: (g_two, D), 2: (g_three, D), 1: (g_three, 0), 0: (g_four, 0)}
    stores = []
    for m in order:
        for load in loads[m]:
            load.wait()
        ref, at = grads[m]
        results = step(1 + m, in_buf[0, m], ref[:, at : at + D].astype(f32), in_buf[1, m], in_buf[2, m])
        for j, result in enumerate(results):
            buf = low_buf.at[m] if j == 4 else out_buf.at[j, m]
            buf[...] = result
            stores.append(pltpu.make_async_copy(buf, outs[3 * j + 1].at[m], out_sem.at[j, m]))
            stores[-1].start()
    for j, result in enumerate(step(0, wi[...], g_in[...], mi[...], si[...])):
        outs[3 * j][...] = result
    for j, result in enumerate(step(7, wo[...], g_out[...], mo[...], so[...])):
        outs[3 * j + 2][...] = result
    for store in stores:
        store.wait()


def update_all(grads, states):
    vm, hbm = pl.BlockSpec(memory_space=pltpu.VMEM), pl.BlockSpec(memory_space=pl.ANY)
    kinds = [f32] * 4 + [bf16]
    shapes = [states[0].shape, states[1].shape, states[2].shape]
    n, SH, D = states[1].shape
    return pl.pallas_call(
        update_kernel,
        out_shape=[jax.ShapeDtypeStruct((1, 1), f32)]
        + [jax.ShapeDtypeStruct(s, k) for k in kinds for s in shapes]
        + [jax.ShapeDtypeStruct((2, 8), f32)],
        in_specs=[vm] * 7 + [vm, hbm, vm] * 3,
        out_specs=[vm] + [vm, hbm, vm] * 5 + [vm],
        scratch_shapes=[
            pltpu.VMEM((3, n, SH, D), f32),
            pltpu.VMEM((4, n, SH, D), f32),
            pltpu.VMEM((n, SH, D), bf16),
            pltpu.SemaphoreType.DMA((3, n)),
            pltpu.SemaphoreType.DMA((5, n)),
        ],
        name="lamb",
        compiler_params=pltpu.CompilerParams(vmem_limit_bytes=67043328),
    )(*grads, *states)


def kernel_body(mesh, step, inputs, targets, cell_area, cell_count, cell_node, edge_senders, edge_receivers, *states):
    states = [a.T if i % 3 == 2 else a for i, a in enumerate(states)]
    inputs, targets = (a.transpose(2, 0, 1) for a in (inputs, targets))
    grads = step(cell_count, inputs, targets, cell_area, cell_node, edge_senders[None, :], edge_receivers[None, :], *states)
    loss, *outs, norms = update_all(grads, states)
    outs = [a.T if i % 3 == 2 else a for i, a in enumerate(outs)]
    return (loss[0, 0], *outs, norms)


def native_gradients(
    inputs,
    targets,
    cell_area,
    cell_count,
    cell_node,
    edge_senders,
    edge_receivers,
    weight_input,
    weight_latent,
    weight_output,
):
    full_input, complete_latent, full_output = (
        lax.all_gather(weight_input.astype(jnp.bfloat16), "col", axis=1, tiled=True),
        lax.all_gather(weight_latent.astype(jnp.bfloat16), "col", axis=1, tiled=True),
        lax.all_gather(weight_output.astype(jnp.bfloat16), "col", axis=0, tiled=True),
    )
    samples = inputs.shape[0]
    slots = inputs.shape[1]
    valid = (jnp.arange(slots, dtype=jnp.int32) < cell_count[0]).astype(jnp.float32)
    cell_weight = cell_area * valid
    area_total = lax.psum(jnp.sum(cell_weight), ("row", "col"))
    first_pre = reduced_matmul("sci,id->scd", inputs, full_input)
    grid_latent = jax.nn.silu(first_pre).astype(jnp.bfloat16)
    node_match = (cell_node[None, :] == jnp.arange(MESH_DEV, dtype=jnp.int32)[:, None]).astype(
        jnp.float32
    )
    node_match_low = node_match.astype(jnp.bfloat16)
    cell_match = node_match_low.T
    node_valid = node_match * valid[None, :]
    node_sum = reduced_matmul("nc,scd->snd", node_valid.astype(jnp.bfloat16), grid_latent)
    node_lower_limit = jnp.maximum(jnp.sum(node_valid, axis=1), 1.0)
    node_average = node_sum / node_lower_limit[None, :, None]
    average_reduced = node_average.astype(jnp.bfloat16)
    second_activation_input = reduced_matmul("kaj,jz->kaz", average_reduced, complete_latent[0])
    mesh_latent = jax.nn.silu(second_activation_input)
    mesh_state_reduced = mesh_latent.astype(jnp.bfloat16)
    receiver_local_part = reduced_matmul("kaj,jz->kaz", mesh_state_reduced, complete_latent[2])
    receiver_block = lax.all_gather(receiver_local_part, "col", axis=1, tiled=True)
    sender_block = reduced_matmul(
        "kaj,jz->kaz",
        lax.all_gather(mesh_state_reduced, "row", axis=1, tiled=True),
        complete_latent[1],
    )
    receiver_rows = receiver_block.shape[1]
    sender_rows = sender_block.shape[1]
    sender_match = one_hot_table(edge_senders, sender_rows)
    receiver_match = one_hot_table(edge_receivers, receiver_rows)
    edge_pre = pick_rows(sender_match, sender_block) + pick_rows(receiver_match, receiver_block)
    partial_sums = add_into_rows(receiver_match, jax.nn.silu(edge_pre))
    message_total = lax.psum_scatter(partial_sums, "col", scatter_dimension=1, tiled=True) / DEG
    message_total_reduced = message_total.astype(jnp.bfloat16)
    residual_branch = reduced_matmul("kaj,jz->kaz", message_total_reduced, complete_latent[3])
    mesh_next = mesh_latent + residual_branch
    decode_rows = reduced_matmul("cn,snd->scd", cell_match, mesh_next.astype(jnp.bfloat16)).astype(
        jnp.bfloat16
    )
    third_pre = reduced_matmul("scd,de->sce", decode_rows, complete_latent[4]) + reduced_matmul(
        "scd,de->sce", grid_latent, complete_latent[5]
    )
    grid_out = jax.nn.silu(third_pre).astype(jnp.bfloat16)
    predict = reduced_matmul("scd,do->sco", grid_out, full_output)
    error = predict - targets.astype(jnp.float32)
    denominator = C_OUT * samples * area_total
    weighted = cell_weight[None, :, None] * error
    loss_value = lax.psum(jnp.sum(weighted * error), ("row", "col")) / denominator
    d_predict = (2.0 * weighted / denominator).astype(jnp.bfloat16)
    grad_output_local = reduced_matmul("scd,sco->do", grid_out, d_predict)
    d_grid_out = reduced_matmul("sco,do->scd", d_predict, full_output)
    d_third = silu_grad(third_pre, d_grid_out).astype(jnp.bfloat16)
    grad_decode = reduced_matmul("scd,sce->de", decode_rows, d_third)
    grad_skip = reduced_matmul("scd,sce->de", grid_latent, d_third)
    d_decode = reduced_matmul("sce,de->scd", d_third, complete_latent[4])
    d_skip = reduced_matmul("sce,de->scd", d_third, complete_latent[5])
    d_mesh_next = jnp.einsum("nc,scd->snd", node_match, d_decode, precision=highest)
    residual_branch_gradient = d_mesh_next.astype(jnp.bfloat16)
    branch_gradient_sum = reduced_matmul(
        "lhg,lhj->gj", message_total_reduced, residual_branch_gradient
    )
    message_total_gradient = reduced_matmul(
        "pyk,ck->pyc", residual_branch_gradient, complete_latent[3]
    ).astype(jnp.bfloat16)
    d_block = lax.all_gather(message_total_gradient, "col", axis=1, tiled=True)
    d_edge_message = reduced_matmul("es,ksd->ked", receiver_match, d_block)
    d_edge_pre = silu_grad(edge_pre, d_edge_message / DEG)
    d_sender_part = add_into_rows(sender_match, d_edge_pre)
    d_receiver_part = add_into_rows(receiver_match, d_edge_pre)
    sender_gradient = lax.psum_scatter(
        d_sender_part.astype(jnp.bfloat16), "row", scatter_dimension=1, tiled=True
    )
    receiver_gradient = lax.psum_scatter(
        d_receiver_part.astype(jnp.bfloat16), "col", scatter_dimension=1, tiled=True
    )
    sender_weight_gradient = reduced_matmul("lhg,lhj->gj", mesh_state_reduced, sender_gradient)
    receiver_weight_gradient = reduced_matmul("lhg,lhj->gj", mesh_state_reduced, receiver_gradient)
    d_mesh = (
        d_mesh_next
        + reduced_matmul("pyk,ck->pyc", sender_gradient, complete_latent[1])
        + reduced_matmul("pyk,ck->pyc", receiver_gradient, complete_latent[2])
    )
    hidden_second_gradient = silu_grad(second_activation_input, d_mesh).astype(jnp.bfloat16)
    encoder_gradient = reduced_matmul("lhg,lhj->gj", average_reduced, hidden_second_gradient)
    node_average_gradient = (
        reduced_matmul("pyk,ck->pyc", hidden_second_gradient, complete_latent[0])
        / node_lower_limit[None, :, None]
    )
    d_grid = d_skip + valid[None, :, None] * pick_rows(cell_match, node_average_gradient)
    d_first = silu_grad(first_pre, d_grid).astype(jnp.bfloat16)
    grad_input_local = reduced_matmul("sci,scd->id", inputs, d_first)
    grad_latent_local = jnp.stack(
        [
            encoder_gradient,
            sender_weight_gradient,
            receiver_weight_gradient,
            branch_gradient_sum,
            grad_decode,
            grad_skip,
        ]
    )
    local_terms = (grad_input_local, grad_latent_local, grad_output_local)
    whole_input, whole_latent, whole_output = lax.psum(
        (local_terms[0], local_terms[1], local_terms[2]), ("row", "col")
    )
    column = lax.axis_index("col")
    width_input = weight_input.shape[1]
    width_latent = weight_latent.shape[1]
    width_output = weight_output.shape[0]
    gradient_input = lax.dynamic_slice_in_dim(whole_input, column * width_input, width_input, 1)
    gradient_latent = lax.dynamic_slice_in_dim(whole_latent, column * width_latent, width_latent, 1)
    gradient_output = lax.dynamic_slice_in_dim(whole_output, column * width_output, width_output, 0)
    return loss_value, gradient_input, gradient_latent, gradient_output


def body(
    mesh,
    inputs,
    targets,
    cell_area,
    cell_count,
    cell_node,
    edge_senders,
    edge_receivers,
    weight_input,
    weight_latent,
    weight_output,
    mean_input,
    mean_latent,
    mean_output,
    square_input,
    square_latent,
    square_output,
):
    given = (inputs, targets, cell_area, cell_count, cell_node, edge_senders, edge_receivers, weight_input, weight_latent, weight_output)
    states = (mean_input, mean_latent, mean_output, square_input, square_latent, square_output)
    step = Step(mesh, inputs.shape[0], inputs.shape[1], weight_latent.shape[2], edge_senders.shape[0], inputs.shape[2])
    if step.fits():
        return kernel_body(mesh, step, *given, *states)
    loss_value, gradient_input, gradient_latent, gradient_output = native_gradients(*given)
    first_input, second_input, update_input = adam_parts(
        weight_input, gradient_input, mean_input, square_input
    )
    first_latent, second_latent, update_latent = adam_parts(
        weight_latent, gradient_latent, mean_latent, square_latent
    )
    first_output, second_output, update_output = adam_parts(
        weight_output, gradient_output, mean_output, square_output
    )
    weight_sums = jnp.concatenate(
        [
            jnp.sum(weight_input * weight_input)[None],
            jnp.sum(weight_latent * weight_latent, axis=(1, 2)),
            jnp.sum(weight_output * weight_output)[None],
        ]
    )
    update_sums = jnp.concatenate(
        [
            jnp.sum(update_input * update_input)[None],
            jnp.sum(update_latent * update_latent, axis=(1, 2)),
            jnp.sum(update_output * update_output)[None],
        ]
    )
    norm_sums = lax.psum(jnp.stack([weight_sums, update_sums]), "col")
    trust_norms = jnp.sqrt(norm_sums)
    ratio = trust_norms[0] / (trust_norms[1] + trust_epsilon)
    master_input = weight_input - learn_rate * ratio[0] * update_input
    master_latent = weight_latent - learn_rate * ratio[1:7][:, None, None] * update_latent
    master_output = weight_output - learn_rate * ratio[7] * update_output
    return (
        loss_value,
        gradient_input,
        gradient_latent,
        gradient_output,
        first_input,
        first_latent,
        first_output,
        second_input,
        second_latent,
        second_output,
        master_input,
        master_latent,
        master_output,
        master_input.astype(jnp.bfloat16),
        master_latent.astype(jnp.bfloat16),
        master_output.astype(jnp.bfloat16),
        trust_norms,
    )


def solution(mesh):
    placed = (
        P(None, ("row", "col"), None),
        P(None, ("row", "col"), None),
        P(("row", "col")),
        P(("row", "col")),
        P(("row", "col")),
        P(("row", "col")),
        P(("row", "col")),
        P(None, "col"),
        P(None, "col", None),
        P("col", None),
        P(None, "col"),
        P(None, "col", None),
        P("col", None),
        P(None, "col"),
        P(None, "col", None),
        P("col", None),
    )
    return jax.shard_map(
        functools.partial(body, mesh),
        mesh=mesh,
        in_specs=placed,
        out_specs=(
            P(),
            P(None, "col"),
            P(None, "col", None),
            P("col", None),
            P(None, "col"),
            P(None, "col", None),
            P("col", None),
            P(None, "col"),
            P(None, "col", None),
            P("col", None),
            P(None, "col"),
            P(None, "col", None),
            P("col", None),
            P(None, "col"),
            P(None, "col", None),
            P("col", None),
            P(),
        ),
        check_vma=False,
    )
```

```python
import functools
import types

import jax
import jax.numpy as jnp
from jax import lax
from jax.experimental import pallas as pl
from jax.experimental.pallas import tpu as pltpu
from jax.sharding import PartitionSpec as P

C_OUT = 83
DEG = 16
MESH_DEV = 64


highest = lax.Precision.HIGHEST
beta_first = 0.5
beta_second = 0.5
adam_epsilon = 1e-08
trust_epsilon = 1e-06
weight_decay = 0.01
learn_rate = 0.1


def silu_grad(pre_act, grad_out):
    sigma = jax.nn.sigmoid(pre_act)
    return grad_out * sigma * (1.0 + pre_act * (1.0 - sigma))


def reduced_matmul(form, left, right):
    return jnp.einsum(form, left, right, preferred_element_type=jnp.float32)


def split_parts(values):
    upper = values.astype(jnp.bfloat16)
    rest = values - upper.astype(jnp.float32)
    middle = rest.astype(jnp.bfloat16)
    lower = (rest - middle.astype(jnp.float32)).astype(jnp.bfloat16)
    return (upper, middle, lower)


def pick_rows(match, values):
    upper, middle, lower = split_parts(values)
    total = reduced_matmul("es,ksd->ked", match, upper)
    total = total + reduced_matmul("es,ksd->ked", match, middle)
    return total + reduced_matmul("es,ksd->ked", match, lower)


def add_into_rows(match, values):
    upper, middle, lower = split_parts(values)
    total = reduced_matmul("es,ked->ksd", match, upper)
    total = total + reduced_matmul("es,ked->ksd", match, middle)
    return total + reduced_matmul("es,ked->ksd", match, lower)


def one_hot_table(indices, count):
    return (indices[:, None] == jnp.arange(count, dtype=jnp.int32)[None, :]).astype(jnp.bfloat16)


def adam_parts(weight, gradient, first, second):
    new_first = beta_first * first + (1.0 - beta_first) * gradient
    new_second = beta_second * second + (1.0 - beta_second) * gradient * gradient
    update = new_first / (jnp.sqrt(new_second) + adam_epsilon) + weight_decay * weight
    return (new_first, new_second, update)


MESH = pl.DeviceIdType.MESH
bf16 = jnp.bfloat16
f32 = jnp.float32
VMEM_ROOM = 63 * 2**20
N_IN = 256
N_OUT = 128
WIRE = ("in", 0, 1, 2, 5, 3, 4, "out")


def sizes_of(n_row, n_col):
    X = n_col // 2
    Y = X if n_row % X == 0 else 1
    return X, Y, n_row // Y


class Place:
    def __init__(self, n_row, n_col):
        self.K = 2
        self.X, self.Y, self.Z = sizes_of(n_row, n_col)
        self.row, self.col = lax.axis_index("row"), lax.axis_index("col")
        self.z, self.y = self.row // self.Y, self.row % self.Y
        self.x, self.k = self.col // 2, self.col % 2

    def to(self, axis, d):
        n = getattr(self, axis.upper())
        return (getattr(self, axis) + d) % n

    def peer(self, axis, d):
        at = {a: getattr(self, a) for a in "zyxk"}
        at[axis] = self.to(axis, d)
        return (at["z"] * self.Y + at["y"], at["x"] * 2 + at["k"])

    def greet(self):
        sem = pltpu.get_barrier_semaphore()
        peers = [self.peer(a, d) for a in "kxyz" for d in range(1, getattr(self, a.upper()))]
        for peer in peers:
            pl.semaphore_signal(sem, inc=1, device_id=peer, device_id_type=MESH)
        return sem, len(peers)


def remote(src, dst, send_sem, recv_sem, device):
    return pltpu.make_async_remote_copy(
        src_ref=src,
        dst_ref=dst,
        send_sem=send_sem,
        recv_sem=recv_sem,
        device_id=device,
        device_id_type=MESH,
    )


def ds(start, size):
    if isinstance(start, int):
        return pl.ds(start, size)
    return pl.ds(pl.multiple_of(start, size if size % 128 else 128), size)


def by_rows(count, step, todo):
    def one(i, carry):
        todo(pl.multiple_of(i * step, step))
        return carry

    lax.fori_loop(0, count // step, one, 0)


def mm(a, b):
    return jnp.dot(a, b, preferred_element_type=f32)


def mm_nt(a, b):
    return lax.dot_general(a, b, (((1,), (1,)), ((), ())), preferred_element_type=f32)


def mm_tn(a, b):
    return lax.dot_general(a, b, (((0,), (0,)), ((), ())), preferred_element_type=f32)


def sigmoid(v):
    return 0.5 * jnp.tanh(0.5 * v) + 0.5


def silu(v):
    return v * sigmoid(v)


def silu_slope(v):
    s = sigmoid(v)
    return s * (1.0 + v * (1.0 - s))


def high_low(v):
    high = v.astype(bf16)
    return high, (v - high.astype(f32)).astype(bf16)


class Total:
    AXES = "kxyz"

    @staticmethod
    def scratch(X, Y, Z):
        many = 1 + X - 1 + Y - 1 + Z - 1
        return [pltpu.VMEM((n, 8, 128), f32) for n in (2, X, Y, Z)] + [
            pltpu.VMEM((8, 128), f32),
            pltpu.SemaphoreType.DMA((many,)),
            pltpu.SemaphoreType.DMA((many,)),
        ]

    def __init__(self, place, refs):
        self.p, self.bufs, (self.value, self.ss, self.rs) = place, dict(zip("kxyz", refs[:4])), refs[4:]

    def _copies(self, axis):
        p, buf = self.p, self.bufs[axis]
        base = sum(getattr(p, a.upper()) - 1 for a in self.AXES[: self.AXES.index(axis)])
        here = buf.at[getattr(p, axis)]
        for d in range(1, getattr(p, axis.upper())):
            i = base + d - 1
            yield remote(here, here, self.ss.at[i], self.rs.at[i], p.peer(axis, d))

    def start(self, axis):
        self.bufs[axis][getattr(self.p, axis)] = self.value[...]
        for copy in self._copies(axis):
            copy.start()

    def finish(self, axis):
        for copy in self._copies(axis):
            copy.wait_recv()
        buf = self.bufs[axis]
        value = buf[0]
        for i in range(1, getattr(self.p, axis.upper())):
            value = value + buf[i]
        self.value[...] = value

    def drain(self, axes):
        for axis in axes:
            for copy in self._copies(axis):
                copy.wait_send()


class Reduce:
    def __init__(self, grid, dim, n_col, width, late, order, lender=None, lanes=0):
        self.X, self.Y, self.Z = grid
        self.dim, self.shard, self.late, self.order = dim, dim // n_col, late, order
        self.ry = self.shard // self.Y
        self.rz = self.ry // self.Z
        self.w = width
        self.lender, self.lanes, self.lent = lender, lanes, False

    def scratch(self):
        X, Y, Z, w = self.X, self.Y, self.Z, self.w
        many = X + (X - 1) + 2 * (Y - 1) + 2 * (Z - 1)
        along_x = (X - 1, 1, self.shard, w) if self.order == "xy" else (X - 1, 1, self.ry, w)
        along_y = (Y - 1, 1, self.ry, w) if self.order == "xy" else (Y - 1, X, self.ry, w)
        return [
            *([] if self.lender else [pltpu.VMEM((self.dim, w), f32)]),
            pltpu.VMEM((X, self.shard, w), f32),
            pltpu.VMEM(along_x, bf16),
            pltpu.VMEM(along_x, bf16),
            pltpu.VMEM(along_y, bf16),
            pltpu.VMEM(along_y, bf16),
            pltpu.VMEM((Z - 1, self.rz, w), self.late),
            pltpu.VMEM((Z - 1, self.rz, w), self.late),
            pltpu.VMEM((self.rz, w), f32),
            pltpu.VMEM((self.shard, w), self.late),
            pltpu.SemaphoreType.DMA((many,)),
            pltpu.SemaphoreType.DMA((many,)),
        ]

    def bind(self, place, refs):
        if self.lender:
            refs = (self.lender.full.at[:, self.lanes : self.lanes + self.w], *refs)
        (self.full, self.cr, self.xs, self.xr, self.ys, self.yr, self.zs, self.zin, self.piece, self.out, self.ss, self.rs) = refs
        self.p = place

    def lend(self):
        for copy in self.copies(0):
            copy.wait_send()

    def rows_of(self, x, k):
        return (2 * x + k) * self.shard

    def place_z(self):
        return pl.ds(pl.multiple_of(self.p.y * self.ry + self.p.z * self.rz, 16), self.rz)

    def copies(self, stage):
        p, X, Y, Z = self.p, self.X, self.Y, self.Z
        first_x = self.order == "xy"
        x_base, y_base = (X, 2 * X - 1) if first_x else (X + Y - 1, X)
        base = (0, x_base if first_x else y_base, y_base if first_x else x_base, 2 * X + Y - 2, 2 * X + Y + Z - 3, 2 * X + Y + 2 * Z - 4)[stage]
        if stage == 0:
            many = [(self.full.at[ds(self.rows_of(x, 1 - p.k), self.shard), :], self.cr.at[x], p.peer("k", 1)) for x in range(X)]
        elif stage == (1 if first_x else 2):
            many = [(self.xs.at[d - 1], self.xr.at[d - 1], p.peer("x", d)) for d in range(1, X)]
        elif stage == (2 if first_x else 1):
            many = [(self.ys.at[d - 1], self.yr.at[d - 1], p.peer("y", d)) for d in range(1, Y)]
        elif stage == 3:
            many = [(self.zs.at[d - 1], self.zin.at[d - 1], p.peer("z", d)) for d in range(1, Z)]
        elif stage == 4:
            here = self.out.at[self.place_z(), :]
            many = [(here, here, p.peer("z", d)) for d in range(1, Z)]
        else:
            here = self.out.at[pl.ds(pl.multiple_of(p.y * self.ry, 16), self.ry), :]
            many = [(here, here, p.peer("y", d)) for d in range(1, Y)]
        return [remote(src, dst, self.ss.at[base + i], self.rs.at[base + i], to) for i, (src, dst, to) in enumerate(many)]

    def sum_core(self, x, at, n=16):
        mine = self.full[pl.ds(pl.multiple_of(self.rows_of(x, self.p.k) + at, 16), n), :]
        return mine + self.cr[x, pl.ds(at, n), :]

    def sum_first(self, x, y, at):
        rows = pl.multiple_of(y * self.ry + at, 16)
        value = self.sum_core(x, rows)
        if self.order == "xy":
            for d in range(1, self.X):
                value = value + self.xr[d - 1, 0, pl.ds(rows, 16), :].astype(f32)
        else:
            for d in range(1, self.Y):
                value = value + self.yr[d - 1, x, pl.ds(at, 16), :].astype(f32)
        return value

    def stage(self, s):
        p, X, Y, Z = self.p, self.X, self.Y, self.Z
        if s:
            for copy in self.copies(s - 1):
                copy.wait_recv()
        if s == 1 and self.order == "xy":
            for d in range(1, X):
                to = p.to("x", d)

                def one(at, to=to, d=d):
                    self.xs[d - 1, 0, pl.ds(at, 16), :] = self.sum_core(to, at).astype(bf16)

                by_rows(self.shard, 16, one)
        elif s == 1:
            for d in range(1, Y):
                base = p.to("y", d) * self.ry

                def one(at, base=base, d=d):
                    for x in range(X):
                        self.ys[d - 1, x, pl.ds(at, 16), :] = self.sum_core(x, pl.multiple_of(base + at, 16)).astype(bf16)

                by_rows(self.ry, 16, one)
        elif s == 2:
            if self.order == "xy":
                for d in range(1, Y):

                    def one(at, to=p.to("y", d), d=d):
                        self.ys[d - 1, 0, pl.ds(at, 16), :] = self.sum_first(p.x, to, at).astype(bf16)

                    by_rows(self.ry, 16, one)
            else:
                for d in range(1, X):

                    def one(at, to=p.to("x", d), d=d):
                        self.xs[d - 1, 0, pl.ds(at, 16), :] = self.sum_first(to, p.y, at).astype(bf16)

                    by_rows(self.ry, 16, one)

            def mine(at):
                self.cr[p.x, pl.ds(pl.multiple_of(p.y * self.ry + at, 16), 16), :] = self.sum_first(p.x, p.y, at)

            by_rows(self.ry, 16, mine)
        elif s == 3:

            def total(z):
                rows = pl.multiple_of(z * self.rz, 16)
                value = self.cr[p.x, pl.ds(pl.multiple_of(p.y * self.ry + rows, 16), self.rz), :]
                arrived = self.yr if self.order == "xy" else self.xr
                for d in range(1, Y if self.order == "xy" else X):
                    value = value + arrived[d - 1, 0, pl.ds(rows, self.rz), :].astype(f32)
                return value

            for d in range(1, Z):
                self.zs[d - 1] = total(p.to("z", d)).astype(self.late)
            self.piece[...] = total(p.z)
        elif s == 4:
            value = self.piece[...]
            for d in range(1, Z):
                value = value + self.zin[d - 1].astype(f32)
            self.piece[...] = value
            self.out[self.place_z(), :] = value.astype(self.late)
        if s < STAGES - 1:
            for copy in self.copies(s):
                copy.start()

    def drain(self):
        for s in range(1 if self.lent else 0, STAGES - 1):
            for copy in self.copies(s):
                copy.wait_send()


STAGES = 7


class Step:
    def __init__(self, mesh, samples, slots, dim, edges, c_in):
        self.n_row, self.n_col = mesh.shape["row"], mesh.shape["col"]
        self.grid = sizes_of(self.n_row, self.n_col)
        self.S, self.C, self.D, self.E, self.c_in = samples, slots, dim, edges, c_in
        self.N = MESH_DEV
        self.SH = dim // self.n_col
        self.R, self.Q = self.n_row * self.N, self.n_col * self.N
        chunk = functools.partial(Reduce, self.grid, dim, self.n_col)
        skips, decoders = chunk(dim + N_OUT, f32, "xy"), chunk(2 * dim, bf16, "xy")
        skips.lent = decoders.lent = True
        self.chunks = [
            skips,
            decoders,
            chunk(dim, bf16, "xy", decoders, 0),
            chunk(dim, bf16, "xy", decoders, dim),
            chunk(dim, bf16, "yx", skips, 0),
            chunk(N_IN, f32, "yx"),
        ]
        X, Y, Z = self.grid
        S, C, D, E, N, R, Q = self.S, self.C, self.D, self.E, self.N, self.R, self.Q
        vm = pltpu.VMEM
        dma = lambda *shape: pltpu.SemaphoreType.DMA(shape)
        self.shapes = dict(
            wib=vm((D, N_IN), bf16),
            wlb=vm((6, D, D), bf16),
            wob=vm((D, N_OUT), bf16),
            nm=vm((N, C), bf16),
            nv=vm((N, C), bf16),
            cm=vm((C, N), bf16),
            cmv=vm((C, N), bf16),
            cw=vm((C, 128), f32),
            cnt=vm((N, 128), f32),
            fx=vm((N_IN, S, C), f32),
            xb=vm((S * C, N_IN), bf16),
            tb=vm((S * C, N_OUT), bf16),
            fp=vm((S * C, D), f32),
            gl=vm((S * C, D), bf16),
            tp=vm((S * C, D), f32),
            go=vm((S * C, D), bf16),
            dp=vm((S * C, N_OUT), bf16),
            dt=vm((S * C, D), bf16),
            av=vm((S * N, D), bf16),
            sp=vm((S * N, D), f32),
            mlb=vm((S * N, D), bf16),
            agb=vm((S * N, D), bf16),
            mnb=vm((S * N, D), bf16),
            sg=vm((S * N, D), f32),
            dmn=vm((S * N, D), f32),
            dsb=vm((S * N, D), bf16),
            drb=vm((S * N, D), bf16),
            d2b=vm((S * N, D), bf16),
            sr=vm((S, R + Q, D), bf16),
            oh=vm((E, R + Q), bf16),
            oht=vm((R + Q, E), bf16),
            ep=vm((S, E, D), f32),
            ac=vm((E, D), bf16),
            tmp=vm((R + Q, D), f32),
            part=vm((S, Q, D), f32),
            pcr=vm((S, X, N, D), f32),
            pxs=vm((S, X - 1, N, D), bf16),
            pxr=vm((S, X - 1, N, D), bf16),
            da=vm((S, Q, D), bf16),
            down=vm((S, Z, N, D), f32),
            dys=vm((S, Y - 1, Z, N, D), bf16),
            dyr=vm((S, Y - 1, Z, N, D), bf16),
            dzs=vm((S, Z - 1, N, D), bf16),
            dzr=vm((S, Z - 1, N, D), bf16),
            loss=vm((8, 128), f32),
            l_sem=dma(24),
            w_ss=dma(8, 1 + 2 * (X - 1)),
            w_rs=dma(8, 1 + 2 * (X - 1)),
            mz_ss=dma(S, Z - 1),
            mz_rs=dma(S, Z - 1),
            my_ss=dma(S, Y - 1, Z),
            my_rs=dma(S, Y - 1, Z),
            mr_ss=dma(S, 1 + 2 * (X - 1)),
            mr_rs=dma(S, 1 + 2 * (X - 1)),
            pk_ss=dma(2, S, X),
            pk_rs=dma(2, S, X),
            px_ss=dma(2, S, X - 1),
            px_rs=dma(2, S, X - 1),
            a_ss=dma(S, 1 + 2 * (X - 1)),
            a_rs=dma(S, 1 + 2 * (X - 1)),
            dy_ss=dma(S, Y - 1, Z),
            dy_rs=dma(S, Y - 1, Z),
            dz_ss=dma(S, Z - 1),
            dz_rs=dma(S, Z - 1),
        )

    def fits(self):
        X, Y, Z = self.grid
        return self.SH % (16 * Y * Z) == 0 and self.SH % 128 == 0 and self.vmem_bytes() < VMEM_ROOM

    def vmem_bytes(self):
        total = 0
        for s in [*self.shapes.values(), *[s for c in self.chunks for s in c.scratch()]]:
            dtype = getattr(s, "dtype", None)
            if dtype in (jnp.dtype(f32), jnp.dtype(bf16)):
                size = jnp.dtype(dtype).itemsize
                for n in s.shape[:-1]:
                    size *= n
                total += size * -(-s.shape[-1] // 128) * 128
        return total

    def scratch(self):
        total = Total.scratch(*self.grid)
        return [*self.shapes.values(), *total * 2, *[s for c in self.chunks for s in c.scratch()]]

    def kernel(self, count, x, tgt, area, node, snd, rcv, wi, wl, wo, mi, mal, mo, si, sal, so, *refs):
        S, C, D, E, N, R, Q, SH = self.S, self.C, self.D, self.E, self.N, self.R, self.Q, self.SH
        X, Y, Z = self.grid
        (g_in, g_out, g_skip, g_two, g_three, g_four, stats), refs = refs[:7], refs[7:]
        v = types.SimpleNamespace(**dict(zip(self.shapes, refs)))
        refs = refs[len(self.shapes) :]
        p = Place(self.n_row, self.n_col)
        area_sum, stat_sum = Total(p, refs[:7]), Total(p, refs[7:14])
        refs = refs[14:]
        for chunk in self.chunks:
            many = len(chunk.scratch())
            chunk.bind(p, refs[:many])
            refs = refs[many:]

        def weight_rows(i, col):
            which = WIRE[i]
            whole = v.wib if which == "in" else v.wob if which == "out" else v.wlb.at[which]
            return whole.at[ds(col * SH, SH), :]

        def w_copy(i, j, d=0):
            rows = weight_rows(i, 2 * p.to("x", -d) + p.k if j == 2 else p.col)
            at = (0, d, X - 1 + d)[j]
            device = p.peer("x", d) if j == 1 else p.peer("k", 1)
            return remote(rows, rows, v.w_ss.at[i, at], v.w_rs.at[i, at], device)

        hops = range(1, X)

        def w_forward(i):
            for d in hops:
                w_copy(i, 1, d).wait_recv()
                w_copy(i, 2, d).start()

        def w_get(i):
            w_copy(i, 0).wait_recv()
            for d in hops:
                w_copy(i, 2, d).wait_recv()

        W = lambda which: v.wlb[which]
        barrier = p.greet()
        own = ds(p.col * SH, SH)
        latents = [w for w in WIRE if isinstance(w, int)]
        loads = {m: pltpu.make_async_copy(wl.at[m], v.fp.at[m * SH : (m + 1) * SH, :], v.l_sem.at[m]) for m in latents}
        for load in loads.values():
            load.start()

        def turned(ref, n):
            v.tmp[0:n, 0:SH] = jnp.zeros((n, SH), f32)
            v.tmp[0 : ref.shape[0], 0:SH] = ref[...]
            return jnp.transpose(v.tmp[0:n, 0:SH])

        def w_ready(i):
            m = WIRE[i]
            if m == "in":
                v.wib[own, :] = turned(wi, N_IN).astype(bf16)
            elif m == "out":
                v.wob[own, :] = turned(wo, N_OUT).astype(bf16)
            else:
                loads[m].wait()
                v.wlb[m, own, :] = v.fp[m * SH : (m + 1) * SH, :].astype(bf16)

        def w_depart(*items):
            for i in items:
                w_copy(i, 0).start()
                for d in hops:
                    w_copy(i, 1, d).start()

        w_ready(0)
        w_ready(1)
        pl.semaphore_wait(*barrier)
        w_depart(0, 1)
        for i in range(2, 8):
            w_ready(i)
            if i < 4:
                w_depart(i)
        used = count[0]
        area_row = area[...].reshape(1, C) * (lax.broadcasted_iota(jnp.int32, (1, C), 1) < used).astype(f32)
        area_sum.value[...] = jnp.broadcast_to(jnp.sum(area_row), (8, 128))
        area_sum.start("y")

        def by_cell(ref, n, out):
            have = ref.shape[0]
            v.fx[0:have] = ref[...].astype(f32)
            v.fx[have:n] = jnp.zeros((n - have, S, C), f32)
            for s in range(S):
                out[s * C : (s + 1) * C, :] = jnp.transpose(v.fx[0:n, s, :]).astype(bf16)

        by_cell(x, N_IN, v.xb)

        node_row = node[...].reshape(1, C)
        match = (lax.broadcasted_iota(jnp.int32, (N, C), 0) == node_row).astype(f32)
        v.nm[...] = match.astype(bf16)
        match = match * (lax.broadcasted_iota(jnp.int32, (N, C), 1) < used).astype(f32)
        v.nv[...] = match.astype(bf16)
        v.cnt[...] = jnp.broadcast_to(jnp.maximum(jnp.sum(match, axis=1, keepdims=True), 1.0), (N, 128))
        node_col = jnp.transpose(jnp.broadcast_to(node_row, (128, C)))
        v.cw[...] = jnp.transpose(jnp.broadcast_to(area_row, (128, C)))
        match = (lax.broadcasted_iota(jnp.int32, (C, 128), 1) == node_col).astype(f32)
        v.cm[...] = match[:, :N].astype(bf16)
        match = match * (lax.broadcasted_iota(jnp.int32, (C, 128), 0) < used).astype(f32)
        v.cmv[...] = match[:, :N].astype(bf16)

        def table(index, base, rows):
            def down(at):
                hit = lax.broadcasted_iota(jnp.int32, (128, E), 0) + at == index
                v.oht[pl.ds(pl.multiple_of(base + at, 128), 128), :] = hit.astype(f32).astype(bf16)

            by_rows(rows, 128, down)
            column = jnp.transpose(jnp.broadcast_to(index, (128, E)))
            for at in range(0, rows, 128):
                hit = lax.broadcasted_iota(jnp.int32, (E, 128), 1) + at == column
                v.oh[:, base + at : base + at + 128] = hit.astype(f32).astype(bf16)

        v.dp[...] = jnp.zeros((S * C, N_OUT), bf16)
        v.loss[...] = jnp.zeros((8, 128), f32)

        def encode(xx, s):
            at, here, lanes = ds(s * C, C), ds(s * N, N), ds(xx * 2 * SH, 2 * SH)
            pre = mm_nt(v.xb[at, :], v.wib[lanes, :])
            v.fp[at, lanes] = pre
            v.gl[at, lanes] = silu(pre).astype(bf16)
            v.av[here, lanes] = (mm(v.nv[...], v.gl[at, lanes]) / v.cnt[:, 0:1]).astype(bf16)

        def encode_all(xx):
            def one(s, carry):
                encode(xx, s)
                return carry

            lax.fori_loop(0, S, one, 0)

        w_copy(0, 0).wait_recv()
        encode_all(p.x)
        w_forward(0)
        by_cell(tgt, N_OUT, v.tb)
        table(snd[...], 0, R)
        table(rcv[...], R, Q)
        for d in hops:
            w_copy(0, 2, d).wait_recv()
            encode_all(p.to("x", -d))
        w_forward(1)
        w_get(1)
        area_sum.finish("y")
        area_sum.start("z")
        pre = mm(v.av[...], W(0))
        v.sp[...] = pre
        v.mlb[...] = silu(pre).astype(bf16)

        def mz(s, d):
            rows = v.sr.at[s, ds(p.row * N, N), :]
            return remote(rows, rows, v.mz_ss.at[s, d - 1], v.mz_rs.at[s, d - 1], p.peer("z", d))

        def my(s, d, e):
            rows = v.sr.at[s, ds((p.to("z", -e) * Y + p.y) * N, N), :]
            return remote(rows, rows, v.my_ss.at[s, d - 1, e], v.my_rs.at[s, d - 1, e], p.peer("y", d))

        def mr(s, j, d=0):
            col = 2 * p.to("x", -d) + p.k if j == 2 else p.col
            rows = v.sr.at[s, ds(R + col * N, N), :]
            at = (0, d, X - 1 + d)[j]
            return remote(rows, rows, v.mr_ss.at[s, at], v.mr_rs.at[s, at], p.peer("x", d) if j == 1 else p.peer("k", 1))

        for s in range(S):
            v.sr[s, ds(p.row * N, N), :] = v.mlb[s * N : (s + 1) * N, :]
            v.sr[s, ds(R + p.col * N, N), :] = v.mlb[s * N : (s + 1) * N, :]

        def depart(s):
            for d in range(1, Z):
                mz(s, d).start()

        depart(0)
        for s in range(S):
            for d in range(1, Y):
                my(s, d, 0).start()
            mr(s, 0).start()
            for d in hops:
                mr(s, 1, d).start()
            if s == 1:
                w_depart(4)
        w_depart(5, 6, 7)
        w_forward(2)
        w_forward(3)
        depart(1)
        area_sum.finish("z")
        area_sum.start("k")
        w_get(2)
        w_get(3)

        def skip(at):
            v.tp[pl.ds(at, 512), :] = mm(v.gl[pl.ds(at, 512), :], W(5))

        def pk(t, s, xx):
            rows = v.part.at[s, ds((2 * xx + 1 - p.k) * N, N), :]
            return remote(rows, v.pcr.at[s, xx], v.pk_ss.at[t, s, xx], v.pk_rs.at[t, s, xx], p.peer("k", 1))

        def px(t, s, d):
            return remote(v.pxs.at[s, d - 1], v.pxr.at[s, d - 1], v.px_ss.at[t, s, d - 1], v.px_rs.at[t, s, d - 1], p.peer("x", d))

        def col_second(t, s):
            for xx in range(X):
                pk(t, s, xx).wait_recv()
            for d in hops:
                px_to = p.to("x", d)
                mine = v.part[s, ds((2 * px_to + p.k) * N, N), :]
                v.pxs[s, d - 1] = (mine + v.pcr[s, px_to]).astype(bf16)
                px(t, s, d).start()

        def col_last(t, s):
            total = v.part[s, ds(p.col * N, N), :] + v.pcr[s, p.x]
            for d in hops:
                px(t, s, d).wait_recv()
                total = total + v.pxr[s, d - 1].astype(f32)
            return total

        def nearest(j):
            steps = [(n + 1) // 2 * (1 if n % 2 else -1) for n in range(1, 2 * Z - 1)]
            taken, found = jnp.int32(0), jnp.int32(0)
            for step in steps:
                inside = ((p.z - step >= 0) & (p.z - step < Z)).astype(jnp.int32)
                found = found + jnp.where((taken == j) & (inside == 1), step, 0)
                taken = taken + inside
            return (found + Z) % Z

        def arrive(s):
            for j in range(Z - 1):
                d = nearest(j)
                mz(s, d).wait_recv()
                for b in range(1, Y):
                    my(s, b, d).start()
            for d in hops:
                mr(s, 1, d).wait_recv()
                mr(s, 2, d).start()

        def edges(s):
            for b in range(1, Y):
                for e in range(Z):
                    my(s, b, e).wait_recv()
            mr(s, 0).wait_recv()
            for d in hops:
                mr(s, 2, d).wait_recv()
            for d in range(1, Z):
                mz(s, d).wait_send()
            for b in range(1, Y):
                for e in range(Z):
                    my(s, b, e).wait_send()
            mr(s, 0).wait_send()
            for d in hops:
                mr(s, 1, d).wait_send()
                mr(s, 2, d).wait_send()
            v.sr[s, 0:R, :] = mm(v.sr[s, 0:R, :], W(1)).astype(bf16)
            v.sr[s, R : R + Q, :] = mm(v.sr[s, R : R + Q, :], W(2)).astype(bf16)

            def pick(at):
                pre = mm(v.oh[pl.ds(at, 512), :], v.sr[s])
                v.ep[s, pl.ds(at, 512), :] = pre
                v.ac[pl.ds(at, 512), :] = silu(pre).astype(bf16)

            by_rows(E, 512, pick)
            v.part[s] = mm(v.oht[R:, :], v.ac[...])
            for xx in range(X):
                pk(0, s, xx).start()

        def ac(s, j, d=0):
            col = 2 * p.to("x", -d) + p.k if j == 2 else p.col
            rows = v.da.at[s, ds(col * N, N), :]
            at = (0, d, X - 1 + d)[j]
            return remote(rows, rows, v.a_ss.at[s, at], v.a_rs.at[s, at], p.peer("x", d) if j == 1 else p.peer("k", 1))

        def decode(s):
            at, here = ds(s * C, C), ds(s * N, N)
            v.agb[here, :] = (col_last(0, s) * (1.0 / DEG)).astype(bf16)
            v.mnb[here, :] = (silu(v.sp[here, :]) + mm(v.agb[here, :], W(3))).astype(bf16)
            scale = 1.0 / (C_OUT * S * area_sum.value[0:1, 0:1])
            rows = mm(v.cm[...], v.mnb[here, :]).astype(bf16)
            pre = mm(rows, W(4)) + v.tp[at, :]
            v.tp[at, :] = pre
            v.go[at, :] = silu(pre).astype(bf16)
            error = mm(v.go[at, :], v.wob[...])[:, :C_OUT] - v.tb[at, 0:C_OUT].astype(f32)
            weighted = v.cw[:, :C_OUT] * error
            v.loss[0:1, 0:C_OUT] = v.loss[0:1, 0:C_OUT] + jnp.sum(weighted * error, axis=0, keepdims=True)
            v.dp[at, 0:C_OUT] = (2.0 * weighted * scale).astype(bf16)
            v.dt[at, :] = (silu_slope(v.tp[at, :]) * mm_nt(v.dp[at, :], v.wob[...])).astype(bf16)
            grad = mm(v.nm[...], v.dt[at, :])
            v.sg[here, :] = grad
            grad = mm_nt(jnp.concatenate(high_low(grad), axis=0), W(4))
            grad = grad[:N] + grad[N:]
            v.dmn[here, :] = grad
            v.da[s, ds(p.col * N, N), :] = mm_nt(grad.astype(bf16), W(3)).astype(bf16)
            ac(s, 0).start()
            for d in hops:
                ac(s, 1, d).start()

        def dy(s, d, e):
            return remote(v.dys.at[s, d - 1, e], v.dyr.at[s, d - 1, e], v.dy_ss.at[s, d - 1, e], v.dy_rs.at[s, d - 1, e], p.peer("y", d))

        def dz(s, d):
            return remote(v.dzs.at[s, d - 1], v.dzr.at[s, d - 1], v.dz_ss.at[s, d - 1], v.dz_rs.at[s, d - 1], p.peer("z", d))

        def pass_on(s):
            for d in hops:
                ac(s, 1, d).wait_recv()
                ac(s, 2, d).start()

        def edges_back(s):
            ac(s, 0).wait_recv()
            for d in hops:
                ac(s, 2, d).wait_recv()
            for xx in range(X):
                pk(0, s, xx).wait_send()
            for d in hops:
                px(0, s, d).wait_send()

            def pick(at):
                grad = mm(v.oh[pl.ds(at, 512), R:], v.da[s])
                v.ac[pl.ds(at, 512), :] = (silu_slope(v.ep[s, pl.ds(at, 512), :]) * grad * (1.0 / DEG)).astype(bf16)

            by_rows(E, 512, pick)
            v.tmp[...] = mm(v.oht[...], v.ac[...])
            for e in (*range(1, Z), 0):
                to = p.to("z", e)
                for d in range(1, Y):
                    v.dys[s, d - 1, e] = v.tmp[ds((to * Y + p.to("y", d)) * N, N), :].astype(bf16)
                    dy(s, d, e).start()
                v.down[s, e] = v.tmp[ds((to * Y + p.y) * N, N), :]
            v.part[s] = v.tmp[R:, :]
            for xx in range(X):
                pk(1, s, xx).start()

        def row_sum(s, e):
            total = v.down[s, e]
            for d in range(1, Y):
                dy(s, d, e).wait_recv()
                total = total + v.dyr[s, d - 1, e].astype(f32)
            return total

        def row_second(s):
            for e in range(1, Z):
                v.dzs[s, e - 1] = row_sum(s, e).astype(bf16)
                dz(s, e).start()

        def encode_back(s):
            at, here = ds(s * C, C), ds(s * N, N)
            v.drb[here, :] = col_last(1, s).astype(bf16)
            total = row_sum(s, 0)
            for d in range(1, Z):
                dz(s, d).wait_recv()
                total = total + v.dzr[s, d - 1].astype(f32)
            v.dsb[here, :] = total.astype(bf16)
            whole = v.dmn[here, :] + mm_nt(v.dsb[here, :], W(1)) + mm_nt(v.drb[here, :], W(2))
            v.d2b[here, :] = (silu_slope(v.sp[here, :]) * whole).astype(bf16)
            high, low = high_low(mm_nt(v.d2b[here, :], W(0)) / v.cnt[:, 0:1])
            grad = v.tp[at, :] + mm(v.cmv[...], high) + mm(v.cmv[...], low)
            v.dt[at, :] = (silu_slope(v.fp[at, :]) * grad).astype(bf16)

        skips, decoders, senders, receivers, encoders, inputs = self.chunks

        def decoder_gradients():
            skips.full[:, 0:D] = mm_tn(v.gl[...], v.dt[...])
            skips.full[:, D : D + N_OUT] = mm_tn(v.go[...], v.dp[...])
            skips.stage(0)
            high, low = high_low(v.sg[...])
            decoders.full[:, 0:D] = mm_tn(v.mnb[...], high) + mm_tn(v.mnb[...], low)
            decoders.full[:, D : 2 * D] = mm_tn(v.agb[...], v.dmn[...].astype(bf16))
            decoders.stage(0)

        def skip_back():
            def one(at):
                v.tp[pl.ds(at, 512), :] = mm_nt(v.dt[pl.ds(at, 512), :], W(5))

            by_rows(S * C, 512, one)

        def weights_rest():
            for i in (5, 6, 7):
                w_forward(i)
            area_sum.finish("x")
            for i in (5, 6, 7):
                w_get(i)

        def partials_back(s):
            col_second(1, s)
            row_second(s)

        stage = lambda chunk, n: functools.partial(chunk.stage, n)
        line = [
            (edges, 0),
            (edges_back, 3),
            (stage(skips, 1), S + 2, None),
            (stage(decoders, 1), S + 2, None),
            (arrive, -2),
            (functools.partial(col_second, 0), 0),
            (weights_rest, 1, None),
            (lambda s: pl.when(s < S // 2)(functools.partial(pass_on, s)), 2),
            (decode, 1),
            (lambda s: pl.when(s >= S // 2)(functools.partial(pass_on, s)), 2),
            (decoder_gradients, S + 1, None),
            (partials_back, 4),
            (skip_back, S + 2, None),
            (stage(skips, 3), S + 5, None),
            (encode_back, 6),
            (stage(skips, 2), S + 3, None),
            (stage(decoders, 2), S + 3, None),
        ]
        arrive(0)
        depart(2)
        w_forward(4)
        w_get(4)
        by_rows(S * C, 512, skip)
        arrive(1)
        depart(3)
        area_sum.finish("k")
        area_sum.start("x")

        def turn(i, carry):
            for todo, behind, *once in line:
                if once:
                    pl.when(i == behind)(todo)
                else:
                    pl.when((i >= max(behind, 0)) & (i < S + behind))(functools.partial(todo, i - behind))
            return carry

        lax.fori_loop(0, S + 6, turn, 0)
        states = [
            pltpu.make_async_copy(a.at[m], v.ep.at[j, m * SH : (m + 1) * SH, :], v.l_sem.at[6 + 6 * j + m])
            for j, a in enumerate((wl, mal, sal))
            for m in range(6)
        ]
        for load in states:
            load.start()
        decoders.lend()
        skips.lend()
        senders.full[...] = mm_tn(v.mlb[...], v.dsb[...])
        senders.stage(0)
        receivers.full[...] = mm_tn(v.mlb[...], v.drb[...])
        receivers.stage(0)
        decoders.stage(3)
        encoders.full[...] = mm_tn(v.av[...], v.d2b[...])
        encoders.stage(0)
        inputs.full[...] = mm_tn(v.dt[...], v.xb[...])
        inputs.stage(0)
        senders.stage(1)
        encoders.stage(1)
        receivers.stage(1)
        inputs.stage(1)

        for load in states:
            load.wait()
        spare = v.ep.at[3]
        for j, (a, b) in enumerate(((wi, wo), (mi, mo), (si, so))):
            spare[j * SH : (j + 1) * SH, 0:N_IN] = turned(a, N_IN)
            spare[j * SH : (j + 1) * SH, N_IN : N_IN + N_OUT] = turned(b, N_OUT)
        lane = lax.broadcasted_iota(jnp.int32, (8, 128), 1)
        row = lax.broadcasted_iota(jnp.int32, (8, 128), 0)
        stat_sum.value[...] = jnp.where(row == 2, jnp.sum(v.loss[...]), 0.0)

        def note(j, gradient, at, lanes):
            held = [buf[pl.ds(pl.multiple_of(start + p.y * (SH // Y) + p.z * (SH // Y // Z), 16), SH // Y // Z), lanes] for buf, start in at]
            _, _, update = adam_parts(held[0], gradient, held[1], held[2])
            for i, what in enumerate((held[0], update)):
                stat_sum.value[...] += jnp.where((row == i) & (lane == j), jnp.sum(what * what), 0.0)

        def note_latent(m, gradient):
            note(1 + m, gradient, [(v.ep.at[j], m * SH) for j in range(3)], slice(None))

        edge = [(spare, j * SH) for j in range(3)]
        skips.stage(4)
        note_latent(5, skips.piece[:, 0:D])
        note(7, skips.piece[:, D : D + N_OUT], edge, slice(N_IN, N_IN + N_OUT))
        decoders.stage(4)
        note_latent(4, decoders.piece[:, 0:D])
        note_latent(3, decoders.piece[:, D : 2 * D])
        senders.stage(2)
        encoders.stage(2)
        receivers.stage(2)
        inputs.stage(2)
        senders.stage(3)
        encoders.stage(3)
        inputs.stage(3)
        receivers.stage(3)
        skips.stage(5)
        senders.stage(4)
        note_latent(1, senders.piece[...])
        encoders.stage(4)
        note_latent(0, encoders.piece[...])
        inputs.stage(4)
        note(0, inputs.piece[...], edge, slice(0, N_IN))
        receivers.stage(4)
        note_latent(2, receivers.piece[...])
        stat_sum.start("k")
        decoders.stage(5)
        stat_sum.finish("k")
        stat_sum.start("x")
        skips.stage(6)
        g_skip[...] = skips.out[:, :D]
        g_out[...] = jnp.transpose(skips.out[:, D : D + N_OUT])[: g_out.shape[0], :]
        senders.stage(5)
        encoders.stage(5)
        stat_sum.finish("x")
        stat_sum.start("z")
        inputs.stage(5)
        receivers.stage(5)
        decoders.stage(6)
        g_two[...] = decoders.out[...]
        senders.stage(6)
        g_three[:, 0:D] = senders.out[...]
        encoders.stage(6)
        g_four[...] = encoders.out[...]
        stat_sum.finish("z")
        stat_sum.start("y")
        inputs.stage(6)
        g_in[...] = jnp.transpose(inputs.out[...])[: g_in.shape[0], :]
        receivers.stage(6)
        g_three[:, D : 2 * D] = receivers.out[...]
        stat_sum.finish("y")
        stats[...] = jnp.where(row < 2, stat_sum.value[...], stat_sum.value[...] / (C_OUT * S * area_sum.value[...]))

        for i in range(8):
            w_copy(i, 0).wait_send()
            for d in hops:
                w_copy(i, 1, d).wait_send()
                w_copy(i, 2, d).wait_send()
        for s in range(S):
            for d in range(1, Z):
                dz(s, d).wait_send()
            for d in range(1, Y):
                for e in range(Z):
                    dy(s, d, e).wait_send()
            ac(s, 0).wait_send()
            for d in hops:
                ac(s, 1, d).wait_send()
                ac(s, 2, d).wait_send()
            for xx in range(X):
                pk(1, s, xx).wait_send()
            for d in hops:
                px(1, s, d).wait_send()
        area_sum.drain("kxyz")
        stat_sum.drain("kxyz")
        for chunk in self.chunks:
            chunk.drain()

    def __call__(self, count, x, tgt, area, node, snd, rcv, *states):
        vm, hbm = pl.BlockSpec(memory_space=pltpu.VMEM), pl.BlockSpec(memory_space=pl.ANY)
        D, SH = self.D, self.SH
        outs = [(states[0].shape, f32), (states[2].shape, f32), ((SH, D), f32), ((SH, 2 * D), bf16), ((SH, 2 * D), bf16), ((SH, D), bf16), ((8, 128), f32)]
        return pl.pallas_call(
            self.kernel,
            out_shape=[jax.ShapeDtypeStruct(*o) for o in outs],
            in_specs=[pl.BlockSpec(memory_space=pltpu.SMEM)] + [vm] * 6 + [vm, hbm, vm] * 3,
            out_specs=[vm] * 7,
            scratch_shapes=self.scratch(),
            name="train_step",
            compiler_params=pltpu.CompilerParams(collective_id=0, has_side_effects=True, vmem_limit_bytes=67043328),
        )(count, x, tgt, area, node, snd, rcv, *states)


def update_kernel(g_in, g_out, g_skip, g_two, g_three, g_four, stats, wi, wl, wo, mi, mal, mo, si, sal, so, *refs):
    loss, *outs, norms = refs[:17]
    in_buf, out_buf, low_buf, in_sem, out_sem = refs[17:]
    SH, D = g_skip.shape
    loads = [[pltpu.make_async_copy(a.at[m], in_buf.at[j, m], in_sem.at[j, m]) for j, a in enumerate((wl, mal, sal))] for m in range(6)]
    order = (5, 4, 3, 2, 1, 0)
    for m in order:
        for load in loads[m]:
            load.start()
    root = jnp.sqrt(stats[...])
    norms[...] = root[0:2, 0:8]
    loss[...] = stats[2:3, 0:1]

    def step(j, weight, gradient, mean, square):
        first, second, update = adam_parts(weight, gradient, mean, square)
        ratio = root[0:1, j : j + 1] / (root[1:2, j : j + 1] + trust_epsilon)
        master = weight - learn_rate * ratio * update
        return gradient, first, second, master, master.astype(bf16)

    grads = {5: (g_skip, 0), 4: (g_two, 0), 3: (g_two, D), 2: (g_three, D), 1: (g_three, 0), 0: (g_four, 0)}
    stores = []
    for m in order:
        for load in loads[m]:
            load.wait()
        ref, at = grads[m]
        results = step(1 + m, in_buf[0, m], ref[:, at : at + D].astype(f32), in_buf[1, m], in_buf[2, m])
        for j, result in enumerate(results):
            buf = low_buf.at[m] if j == 4 else out_buf.at[j, m]
            buf[...] = result
            stores.append(pltpu.make_async_copy(buf, outs[3 * j + 1].at[m], out_sem.at[j, m]))
            stores[-1].start()
    for j, result in enumerate(step(0, wi[...], g_in[...], mi[...], si[...])):
        outs[3 * j][...] = result
    for j, result in enumerate(step(7, wo[...], g_out[...], mo[...], so[...])):
        outs[3 * j + 2][...] = result
    for store in stores:
        store.wait()


def update_all(grads, states):
    vm, hbm = pl.BlockSpec(memory_space=pltpu.VMEM), pl.BlockSpec(memory_space=pl.ANY)
    kinds = [f32] * 4 + [bf16]
    shapes = [states[0].shape, states[1].shape, states[2].shape]
    n, SH, D = states[1].shape
    return pl.pallas_call(
        update_kernel,
        out_shape=[jax.ShapeDtypeStruct((1, 1), f32)]
        + [jax.ShapeDtypeStruct(s, k) for k in kinds for s in shapes]
        + [jax.ShapeDtypeStruct((2, 8), f32)],
        in_specs=[vm] * 7 + [vm, hbm, vm] * 3,
        out_specs=[vm] + [vm, hbm, vm] * 5 + [vm],
        scratch_shapes=[
            pltpu.VMEM((3, n, SH, D), f32),
            pltpu.VMEM((4, n, SH, D), f32),
            pltpu.VMEM((n, SH, D), bf16),
            pltpu.SemaphoreType.DMA((3, n)),
            pltpu.SemaphoreType.DMA((5, n)),
        ],
        name="lamb",
        compiler_params=pltpu.CompilerParams(vmem_limit_bytes=67043328),
    )(*grads, *states)


def kernel_body(mesh, step, inputs, targets, cell_area, cell_count, cell_node, edge_senders, edge_receivers, *states):
    states = [a.T if i % 3 == 2 else a for i, a in enumerate(states)]
    inputs, targets = (a.transpose(2, 0, 1) for a in (inputs, targets))
    grads = step(cell_count, inputs, targets, cell_area, cell_node, edge_senders[None, :], edge_receivers[None, :], *states)
    loss, *outs, norms = update_all(grads, states)
    outs = [a.T if i % 3 == 2 else a for i, a in enumerate(outs)]
    return (loss[0, 0], *outs, norms)


def native_gradients(
    inputs,
    targets,
    cell_area,
    cell_count,
    cell_node,
    edge_senders,
    edge_receivers,
    weight_input,
    weight_latent,
    weight_output,
):
    full_input, complete_latent, full_output = (
        lax.all_gather(weight_input.astype(jnp.bfloat16), "col", axis=1, tiled=True),
        lax.all_gather(weight_latent.astype(jnp.bfloat16), "col", axis=1, tiled=True),
        lax.all_gather(weight_output.astype(jnp.bfloat16), "col", axis=0, tiled=True),
    )
    samples = inputs.shape[0]
    slots = inputs.shape[1]
    valid = (jnp.arange(slots, dtype=jnp.int32) < cell_count[0]).astype(jnp.float32)
    cell_weight = cell_area * valid
    area_total = lax.psum(jnp.sum(cell_weight), ("row", "col"))
    first_pre = reduced_matmul("sci,id->scd", inputs, full_input)
    grid_latent = jax.nn.silu(first_pre).astype(jnp.bfloat16)
    node_match = (cell_node[None, :] == jnp.arange(MESH_DEV, dtype=jnp.int32)[:, None]).astype(
        jnp.float32
    )
    node_match_low = node_match.astype(jnp.bfloat16)
    cell_match = node_match_low.T
    node_valid = node_match * valid[None, :]
    node_sum = reduced_matmul("nc,scd->snd", node_valid.astype(jnp.bfloat16), grid_latent)
    node_lower_limit = jnp.maximum(jnp.sum(node_valid, axis=1), 1.0)
    node_average = node_sum / node_lower_limit[None, :, None]
    average_reduced = node_average.astype(jnp.bfloat16)
    second_activation_input = reduced_matmul("kaj,jz->kaz", average_reduced, complete_latent[0])
    mesh_latent = jax.nn.silu(second_activation_input)
    mesh_state_reduced = mesh_latent.astype(jnp.bfloat16)
    receiver_local_part = reduced_matmul("kaj,jz->kaz", mesh_state_reduced, complete_latent[2])
    receiver_block = lax.all_gather(receiver_local_part, "col", axis=1, tiled=True)
    sender_block = reduced_matmul(
        "kaj,jz->kaz",
        lax.all_gather(mesh_state_reduced, "row", axis=1, tiled=True),
        complete_latent[1],
    )
    receiver_rows = receiver_block.shape[1]
    sender_rows = sender_block.shape[1]
    sender_match = one_hot_table(edge_senders, sender_rows)
    receiver_match = one_hot_table(edge_receivers, receiver_rows)
    edge_pre = pick_rows(sender_match, sender_block) + pick_rows(receiver_match, receiver_block)
    partial_sums = add_into_rows(receiver_match, jax.nn.silu(edge_pre))
    message_total = lax.psum_scatter(partial_sums, "col", scatter_dimension=1, tiled=True) / DEG
    message_total_reduced = message_total.astype(jnp.bfloat16)
    residual_branch = reduced_matmul("kaj,jz->kaz", message_total_reduced, complete_latent[3])
    mesh_next = mesh_latent + residual_branch
    decode_rows = reduced_matmul("cn,snd->scd", cell_match, mesh_next.astype(jnp.bfloat16)).astype(
        jnp.bfloat16
    )
    third_pre = reduced_matmul("scd,de->sce", decode_rows, complete_latent[4]) + reduced_matmul(
        "scd,de->sce", grid_latent, complete_latent[5]
    )
    grid_out = jax.nn.silu(third_pre).astype(jnp.bfloat16)
    predict = reduced_matmul("scd,do->sco", grid_out, full_output)
    error = predict - targets.astype(jnp.float32)
    denominator = C_OUT * samples * area_total
    weighted = cell_weight[None, :, None] * error
    loss_value = lax.psum(jnp.sum(weighted * error), ("row", "col")) / denominator
    d_predict = (2.0 * weighted / denominator).astype(jnp.bfloat16)
    grad_output_local = reduced_matmul("scd,sco->do", grid_out, d_predict)
    d_grid_out = reduced_matmul("sco,do->scd", d_predict, full_output)
    d_third = silu_grad(third_pre, d_grid_out).astype(jnp.bfloat16)
    grad_decode = reduced_matmul("scd,sce->de", decode_rows, d_third)
    grad_skip = reduced_matmul("scd,sce->de", grid_latent, d_third)
    d_decode = reduced_matmul("sce,de->scd", d_third, complete_latent[4])
    d_skip = reduced_matmul("sce,de->scd", d_third, complete_latent[5])
    d_mesh_next = jnp.einsum("nc,scd->snd", node_match, d_decode, precision=highest)
    residual_branch_gradient = d_mesh_next.astype(jnp.bfloat16)
    branch_gradient_sum = reduced_matmul(
        "lhg,lhj->gj", message_total_reduced, residual_branch_gradient
    )
    message_total_gradient = reduced_matmul(
        "pyk,ck->pyc", residual_branch_gradient, complete_latent[3]
    ).astype(jnp.bfloat16)
    d_block = lax.all_gather(message_total_gradient, "col", axis=1, tiled=True)
    d_edge_message = reduced_matmul("es,ksd->ked", receiver_match, d_block)
    d_edge_pre = silu_grad(edge_pre, d_edge_message / DEG)
    d_sender_part = add_into_rows(sender_match, d_edge_pre)
    d_receiver_part = add_into_rows(receiver_match, d_edge_pre)
    sender_gradient = lax.psum_scatter(
        d_sender_part.astype(jnp.bfloat16), "row", scatter_dimension=1, tiled=True
    )
    receiver_gradient = lax.psum_scatter(
        d_receiver_part.astype(jnp.bfloat16), "col", scatter_dimension=1, tiled=True
    )
    sender_weight_gradient = reduced_matmul("lhg,lhj->gj", mesh_state_reduced, sender_gradient)
    receiver_weight_gradient = reduced_matmul("lhg,lhj->gj", mesh_state_reduced, receiver_gradient)
    d_mesh = (
        d_mesh_next
        + reduced_matmul("pyk,ck->pyc", sender_gradient, complete_latent[1])
        + reduced_matmul("pyk,ck->pyc", receiver_gradient, complete_latent[2])
    )
    hidden_second_gradient = silu_grad(second_activation_input, d_mesh).astype(jnp.bfloat16)
    encoder_gradient = reduced_matmul("lhg,lhj->gj", average_reduced, hidden_second_gradient)
    node_average_gradient = (
        reduced_matmul("pyk,ck->pyc", hidden_second_gradient, complete_latent[0])
        / node_lower_limit[None, :, None]
    )
    d_grid = d_skip + valid[None, :, None] * pick_rows(cell_match, node_average_gradient)
    d_first = silu_grad(first_pre, d_grid).astype(jnp.bfloat16)
    grad_input_local = reduced_matmul("sci,scd->id", inputs, d_first)
    grad_latent_local = jnp.stack(
        [
            encoder_gradient,
            sender_weight_gradient,
            receiver_weight_gradient,
            branch_gradient_sum,
            grad_decode,
            grad_skip,
        ]
    )
    local_terms = (grad_input_local, grad_latent_local, grad_output_local)
    whole_input, whole_latent, whole_output = lax.psum(
        (local_terms[0], local_terms[1], local_terms[2]), ("row", "col")
    )
    column = lax.axis_index("col")
    width_input = weight_input.shape[1]
    width_latent = weight_latent.shape[1]
    width_output = weight_output.shape[0]
    gradient_input = lax.dynamic_slice_in_dim(whole_input, column * width_input, width_input, 1)
    gradient_latent = lax.dynamic_slice_in_dim(whole_latent, column * width_latent, width_latent, 1)
    gradient_output = lax.dynamic_slice_in_dim(whole_output, column * width_output, width_output, 0)
    return loss_value, gradient_input, gradient_latent, gradient_output


def body(
    mesh,
    inputs,
    targets,
    cell_area,
    cell_count,
    cell_node,
    edge_senders,
    edge_receivers,
    weight_input,
    weight_latent,
    weight_output,
    mean_input,
    mean_latent,
    mean_output,
    square_input,
    square_latent,
    square_output,
):
    given = (inputs, targets, cell_area, cell_count, cell_node, edge_senders, edge_receivers, weight_input, weight_latent, weight_output)
    states = (mean_input, mean_latent, mean_output, square_input, square_latent, square_output)
    step = Step(mesh, inputs.shape[0], inputs.shape[1], weight_latent.shape[2], edge_senders.shape[0], inputs.shape[2])
    if step.fits():
        return kernel_body(mesh, step, *given, *states)
    loss_value, gradient_input, gradient_latent, gradient_output = native_gradients(*given)
    first_input, second_input, update_input = adam_parts(
        weight_input, gradient_input, mean_input, square_input
    )
    first_latent, second_latent, update_latent = adam_parts(
        weight_latent, gradient_latent, mean_latent, square_latent
    )
    first_output, second_output, update_output = adam_parts(
        weight_output, gradient_output, mean_output, square_output
    )
    weight_sums = jnp.concatenate(
        [
            jnp.sum(weight_input * weight_input)[None],
            jnp.sum(weight_latent * weight_latent, axis=(1, 2)),
            jnp.sum(weight_output * weight_output)[None],
        ]
    )
    update_sums = jnp.concatenate(
        [
            jnp.sum(update_input * update_input)[None],
            jnp.sum(update_latent * update_latent, axis=(1, 2)),
            jnp.sum(update_output * update_output)[None],
        ]
    )
    norm_sums = lax.psum(jnp.stack([weight_sums, update_sums]), "col")
    trust_norms = jnp.sqrt(norm_sums)
    ratio = trust_norms[0] / (trust_norms[1] + trust_epsilon)
    master_input = weight_input - learn_rate * ratio[0] * update_input
    master_latent = weight_latent - learn_rate * ratio[1:7][:, None, None] * update_latent
    master_output = weight_output - learn_rate * ratio[7] * update_output
    return (
        loss_value,
        gradient_input,
        gradient_latent,
        gradient_output,
        first_input,
        first_latent,
        first_output,
        second_input,
        second_latent,
        second_output,
        master_input,
        master_latent,
        master_output,
        master_input.astype(jnp.bfloat16),
        master_latent.astype(jnp.bfloat16),
        master_output.astype(jnp.bfloat16),
        trust_norms,
    )


def solution(mesh):
    placed = (
        P(None, ("row", "col"), None),
        P(None, ("row", "col"), None),
        P(("row", "col")),
        P(("row", "col")),
        P(("row", "col")),
        P(("row", "col")),
        P(("row", "col")),
        P(None, "col"),
        P(None, "col", None),
        P("col", None),
        P(None, "col"),
        P(None, "col", None),
        P("col", None),
        P(None, "col"),
        P(None, "col", None),
        P("col", None),
    )
    return jax.shard_map(
        functools.partial(body, mesh),
        mesh=mesh,
        in_specs=placed,
        out_specs=(
            P(),
            P(None, "col"),
            P(None, "col", None),
            P("col", None),
            P(None, "col"),
            P(None, "col", None),
            P("col", None),
            P(None, "col"),
            P(None, "col", None),
            P("col", None),
            P(None, "col"),
            P(None, "col", None),
            P("col", None),
            P(None, "col"),
            P(None, "col", None),
            P("col", None),
            P(),
        ),
        check_vma=False,
    )
```

```python
import functools
import types

import jax
import jax.numpy as jnp
from jax import lax
from jax.experimental import pallas as pl
from jax.experimental.pallas import tpu as pltpu
from jax.sharding import PartitionSpec as P

C_OUT = 83
DEG = 16
MESH_DEV = 64


highest = lax.Precision.HIGHEST
beta_first = 0.5
beta_second = 0.5
adam_epsilon = 1e-08
trust_epsilon = 1e-06
weight_decay = 0.01
learn_rate = 0.1


def silu_grad(pre_act, grad_out):
    sigma = jax.nn.sigmoid(pre_act)
    return grad_out * sigma * (1.0 + pre_act * (1.0 - sigma))


def reduced_matmul(form, left, right):
    return jnp.einsum(form, left, right, preferred_element_type=jnp.float32)


def split_parts(values):
    upper = values.astype(jnp.bfloat16)
    rest = values - upper.astype(jnp.float32)
    middle = rest.astype(jnp.bfloat16)
    lower = (rest - middle.astype(jnp.float32)).astype(jnp.bfloat16)
    return (upper, middle, lower)


def pick_rows(match, values):
    upper, middle, lower = split_parts(values)
    total = reduced_matmul("es,ksd->ked", match, upper)
    total = total + reduced_matmul("es,ksd->ked", match, middle)
    return total + reduced_matmul("es,ksd->ked", match, lower)


def add_into_rows(match, values):
    upper, middle, lower = split_parts(values)
    total = reduced_matmul("es,ked->ksd", match, upper)
    total = total + reduced_matmul("es,ked->ksd", match, middle)
    return total + reduced_matmul("es,ked->ksd", match, lower)


def one_hot_table(indices, count):
    return (indices[:, None] == jnp.arange(count, dtype=jnp.int32)[None, :]).astype(jnp.bfloat16)


def adam_parts(weight, gradient, first, second):
    new_first = beta_first * first + (1.0 - beta_first) * gradient
    new_second = beta_second * second + (1.0 - beta_second) * gradient * gradient
    update = new_first / (jnp.sqrt(new_second) + adam_epsilon) + weight_decay * weight
    return (new_first, new_second, update)


MESH = pl.DeviceIdType.MESH
bf16 = jnp.bfloat16
f32 = jnp.float32
VMEM_ROOM = 63 * 2**20
N_IN = 256
N_OUT = 128
WIRE = ("in", 0, 1, 2, 5, 3, 4, "out")


def sizes_of(n_row, n_col):
    X = n_col // 2
    Y = X if n_row % X == 0 else 1
    return X, Y, n_row // Y


class Place:
    def __init__(self, n_row, n_col):
        self.K = 2
        self.X, self.Y, self.Z = sizes_of(n_row, n_col)
        self.row, self.col = lax.axis_index("row"), lax.axis_index("col")
        self.z, self.y = self.row // self.Y, self.row % self.Y
        self.x, self.k = self.col // 2, self.col % 2

    def to(self, axis, d):
        n = getattr(self, axis.upper())
        return (getattr(self, axis) + d) % n

    def peer(self, axis, d):
        at = {a: getattr(self, a) for a in "zyxk"}
        at[axis] = self.to(axis, d)
        return (at["z"] * self.Y + at["y"], at["x"] * 2 + at["k"])

    def greet(self):
        sem = pltpu.get_barrier_semaphore()
        peers = [self.peer(a, d) for a in "kxyz" for d in range(1, getattr(self, a.upper()))]
        for peer in peers:
            pl.semaphore_signal(sem, inc=1, device_id=peer, device_id_type=MESH)
        return sem, len(peers)


def remote(src, dst, send_sem, recv_sem, device):
    return pltpu.make_async_remote_copy(
        src_ref=src,
        dst_ref=dst,
        send_sem=send_sem,
        recv_sem=recv_sem,
        device_id=device,
        device_id_type=MESH,
    )


def ds(start, size):
    if isinstance(start, int):
        return pl.ds(start, size)
    return pl.ds(pl.multiple_of(start, size if size % 128 else 128), size)


def by_rows(count, step, todo):
    def one(i, carry):
        todo(pl.multiple_of(i * step, step))
        return carry

    lax.fori_loop(0, count // step, one, 0)


def mm(a, b):
    return jnp.dot(a, b, preferred_element_type=f32)


def mm_nt(a, b):
    return lax.dot_general(a, b, (((1,), (1,)), ((), ())), preferred_element_type=f32)


def mm_tn(a, b):
    return lax.dot_general(a, b, (((0,), (0,)), ((), ())), preferred_element_type=f32)


def sigmoid(v):
    return 0.5 * jnp.tanh(0.5 * v) + 0.5


def silu(v):
    return v * sigmoid(v)


def silu_slope(v):
    s = sigmoid(v)
    return s * (1.0 + v * (1.0 - s))


def high_low(v):
    high = v.astype(bf16)
    return high, (v - high.astype(f32)).astype(bf16)


class Total:
    AXES = "kxyz"

    @staticmethod
    def scratch(X, Y, Z):
        many = 1 + X - 1 + Y - 1 + Z - 1
        return [pltpu.VMEM((n, 8, 128), f32) for n in (2, X, Y, Z)] + [
            pltpu.VMEM((8, 128), f32),
            pltpu.SemaphoreType.DMA((many,)),
            pltpu.SemaphoreType.DMA((many,)),
        ]

    def __init__(self, place, refs):
        self.p, self.bufs, (self.value, self.ss, self.rs) = place, dict(zip("kxyz", refs[:4])), refs[4:]

    def _copies(self, axis):
        p, buf = self.p, self.bufs[axis]
        base = sum(getattr(p, a.upper()) - 1 for a in self.AXES[: self.AXES.index(axis)])
        here = buf.at[getattr(p, axis)]
        for d in range(1, getattr(p, axis.upper())):
            i = base + d - 1
            yield remote(here, here, self.ss.at[i], self.rs.at[i], p.peer(axis, d))

    def start(self, axis):
        self.bufs[axis][getattr(self.p, axis)] = self.value[...]
        for copy in self._copies(axis):
            copy.start()

    def finish(self, axis):
        for copy in self._copies(axis):
            copy.wait_recv()
        buf = self.bufs[axis]
        value = buf[0]
        for i in range(1, getattr(self.p, axis.upper())):
            value = value + buf[i]
        self.value[...] = value

    def drain(self, axes):
        for axis in axes:
            for copy in self._copies(axis):
                copy.wait_send()


class Reduce:
    def __init__(self, grid, dim, n_col, width, late, order, lender=None, lanes=0):
        self.X, self.Y, self.Z = grid
        self.dim, self.shard, self.late, self.order = dim, dim // n_col, late, order
        self.ry = self.shard // self.Y
        self.rz = self.ry // self.Z
        self.w = width
        self.lender, self.lanes, self.lent = lender, lanes, False

    def scratch(self):
        X, Y, Z, w = self.X, self.Y, self.Z, self.w
        many = X + (X - 1) + 2 * (Y - 1) + 2 * (Z - 1)
        along_x = (X - 1, 1, self.shard, w) if self.order == "xy" else (X - 1, 1, self.ry, w)
        along_y = (Y - 1, 1, self.ry, w) if self.order == "xy" else (Y - 1, X, self.ry, w)
        return [
            *([] if self.lender else [pltpu.VMEM((self.dim, w), f32)]),
            pltpu.VMEM((X, self.shard, w), f32),
            pltpu.VMEM(along_x, bf16),
            pltpu.VMEM(along_x, bf16),
            pltpu.VMEM(along_y, bf16),
            pltpu.VMEM(along_y, bf16),
            pltpu.VMEM((Z - 1, self.rz, w), self.late),
            pltpu.VMEM((Z - 1, self.rz, w), self.late),
            pltpu.VMEM((self.rz, w), f32),
            pltpu.VMEM((self.shard, w), self.late),
            pltpu.SemaphoreType.DMA((many,)),
            pltpu.SemaphoreType.DMA((many,)),
        ]

    def bind(self, place, refs):
        if self.lender:
            refs = (self.lender.full.at[:, self.lanes : self.lanes + self.w], *refs)
        (self.full, self.cr, self.xs, self.xr, self.ys, self.yr, self.zs, self.zin, self.piece, self.out, self.ss, self.rs) = refs
        self.p = place

    def lend(self):
        for copy in self.copies(0):
            copy.wait_send()

    def rows_of(self, x, k):
        return (2 * x + k) * self.shard

    def place_z(self):
        return pl.ds(pl.multiple_of(self.p.y * self.ry + self.p.z * self.rz, 16), self.rz)

    def copies(self, stage):
        p, X, Y, Z = self.p, self.X, self.Y, self.Z
        first_x = self.order == "xy"
        x_base, y_base = (X, 2 * X - 1) if first_x else (X + Y - 1, X)
        base = (0, x_base if first_x else y_base, y_base if first_x else x_base, 2 * X + Y - 2, 2 * X + Y + Z - 3, 2 * X + Y + 2 * Z - 4)[stage]
        if stage == 0:
            many = [(self.full.at[ds(self.rows_of(x, 1 - p.k), self.shard), :], self.cr.at[x], p.peer("k", 1)) for x in range(X)]
        elif stage == (1 if first_x else 2):
            many = [(self.xs.at[d - 1], self.xr.at[d - 1], p.peer("x", d)) for d in range(1, X)]
        elif stage == (2 if first_x else 1):
            many = [(self.ys.at[d - 1], self.yr.at[d - 1], p.peer("y", d)) for d in range(1, Y)]
        elif stage == 3:
            many = [(self.zs.at[d - 1], self.zin.at[d - 1], p.peer("z", d)) for d in range(1, Z)]
        elif stage == 4:
            here = self.out.at[self.place_z(), :]
            many = [(here, here, p.peer("z", d)) for d in range(1, Z)]
        else:
            here = self.out.at[pl.ds(pl.multiple_of(p.y * self.ry, 16), self.ry), :]
            many = [(here, here, p.peer("y", d)) for d in range(1, Y)]
        return [remote(src, dst, self.ss.at[base + i], self.rs.at[base + i], to) for i, (src, dst, to) in enumerate(many)]

    def sum_core(self, x, at, n=16):
        mine = self.full[pl.ds(pl.multiple_of(self.rows_of(x, self.p.k) + at, 16), n), :]
        return mine + self.cr[x, pl.ds(at, n), :]

    def sum_first(self, x, y, at):
        rows = pl.multiple_of(y * self.ry + at, 16)
        value = self.sum_core(x, rows)
        if self.order == "xy":
            for d in range(1, self.X):
                value = value + self.xr[d - 1, 0, pl.ds(rows, 16), :].astype(f32)
        else:
            for d in range(1, self.Y):
                value = value + self.yr[d - 1, x, pl.ds(at, 16), :].astype(f32)
        return value

    def stage(self, s):
        p, X, Y, Z = self.p, self.X, self.Y, self.Z
        if s:
            for copy in self.copies(s - 1):
                copy.wait_recv()
        if s == 1 and self.order == "xy":
            for d in range(1, X):
                to = p.to("x", d)

                def one(at, to=to, d=d):
                    self.xs[d - 1, 0, pl.ds(at, 16), :] = self.sum_core(to, at).astype(bf16)

                by_rows(self.shard, 16, one)
        elif s == 1:
            for d in range(1, Y):
                base = p.to("y", d) * self.ry

                def one(at, base=base, d=d):
                    for x in range(X):
                        self.ys[d - 1, x, pl.ds(at, 16), :] = self.sum_core(x, pl.multiple_of(base + at, 16)).astype(bf16)

                by_rows(self.ry, 16, one)
        elif s == 2:
            if self.order == "xy":
                for d in range(1, Y):

                    def one(at, to=p.to("y", d), d=d):
                        self.ys[d - 1, 0, pl.ds(at, 16), :] = self.sum_first(p.x, to, at).astype(bf16)

                    by_rows(self.ry, 16, one)
            else:
                for d in range(1, X):

                    def one(at, to=p.to("x", d), d=d):
                        self.xs[d - 1, 0, pl.ds(at, 16), :] = self.sum_first(to, p.y, at).astype(bf16)

                    by_rows(self.ry, 16, one)

            def mine(at):
                self.cr[p.x, pl.ds(pl.multiple_of(p.y * self.ry + at, 16), 16), :] = self.sum_first(p.x, p.y, at)

            by_rows(self.ry, 16, mine)
        elif s == 3:

            def total(z):
                rows = pl.multiple_of(z * self.rz, 16)
                value = self.cr[p.x, pl.ds(pl.multiple_of(p.y * self.ry + rows, 16), self.rz), :]
                arrived = self.yr if self.order == "xy" else self.xr
                for d in range(1, Y if self.order == "xy" else X):
                    value = value + arrived[d - 1, 0, pl.ds(rows, self.rz), :].astype(f32)
                return value

            for d in range(1, Z):
                self.zs[d - 1] = total(p.to("z", d)).astype(self.late)
            self.piece[...] = total(p.z)
        elif s == 4:
            value = self.piece[...]
            for d in range(1, Z):
                value = value + self.zin[d - 1].astype(f32)
            self.piece[...] = value
            self.out[self.place_z(), :] = value.astype(self.late)
        if s < STAGES - 1:
            for copy in self.copies(s):
                copy.start()

    def drain(self):
        for s in range(1 if self.lent else 0, STAGES - 1):
            for copy in self.copies(s):
                copy.wait_send()


STAGES = 7


class Step:
    def __init__(self, mesh, samples, slots, dim, edges, c_in):
        self.n_row, self.n_col = mesh.shape["row"], mesh.shape["col"]
        self.grid = sizes_of(self.n_row, self.n_col)
        self.S, self.C, self.D, self.E, self.c_in = samples, slots, dim, edges, c_in
        self.N = MESH_DEV
        self.SH = dim // self.n_col
        self.R, self.Q = self.n_row * self.N, self.n_col * self.N
        chunk = functools.partial(Reduce, self.grid, dim, self.n_col)
        skips, decoders = chunk(dim + N_OUT, f32, "xy"), chunk(2 * dim, bf16, "xy")
        skips.lent = decoders.lent = True
        self.chunks = [
            skips,
            decoders,
            chunk(dim, bf16, "xy", decoders, 0),
            chunk(dim, bf16, "xy", decoders, dim),
            chunk(dim, bf16, "yx", skips, 0),
            chunk(N_IN, f32, "yx"),
        ]
        X, Y, Z = self.grid
        S, C, D, E, N, R, Q = self.S, self.C, self.D, self.E, self.N, self.R, self.Q
        vm = pltpu.VMEM
        dma = lambda *shape: pltpu.SemaphoreType.DMA(shape)
        self.shapes = dict(
            wib=vm((D, N_IN), bf16),
            wlb=vm((6, D, D), bf16),
            wob=vm((D, N_OUT), bf16),
            nm=vm((N, C), bf16),
            nv=vm((N, C), bf16),
            cm=vm((C, N), bf16),
            cmv=vm((C, N), bf16),
            cw=vm((C, 128), f32),
            cnt=vm((N, 128), f32),
            fx=vm((N_IN, S, C), f32),
            xb=vm((S * C, N_IN), bf16),
            tb=vm((S * C, N_OUT), bf16),
            fp=vm((S * C, D), f32),
            gl=vm((S * C, D), bf16),
            tp=vm((S * C, D), f32),
            go=vm((S * C, D), bf16),
            dp=vm((S * C, N_OUT), bf16),
            dt=vm((S * C, D), bf16),
            av=vm((S * N, D), bf16),
            sp=vm((S * N, D), f32),
            mlb=vm((S * N, D), bf16),
            agb=vm((S * N, D), bf16),
            mnb=vm((S * N, D), bf16),
            sg=vm((S * N, D), f32),
            dmn=vm((S * N, D), f32),
            dsb=vm((S * N, D), bf16),
            drb=vm((S * N, D), bf16),
            d2b=vm((S * N, D), bf16),
            sr=vm((S, R + Q, D), bf16),
            oh=vm((E, R + Q), bf16),
            oht=vm((R + Q, E), bf16),
            ep=vm((S, E, D), f32),
            ac=vm((E, D), bf16),
            tmp=vm((R + Q, D), f32),
            part=vm((S, Q, D), f32),
            pcr=vm((S, X, N, D), f32),
            pxs=vm((S, X - 1, N, D), bf16),
            pxr=vm((S, X - 1, N, D), bf16),
            da=vm((S, Q, D), bf16),
            down=vm((S, Z, N, D), f32),
            dys=vm((S, Y - 1, Z, N, D), bf16),
            dyr=vm((S, Y - 1, Z, N, D), bf16),
            dzs=vm((S, Z - 1, N, D), bf16),
            dzr=vm((S, Z - 1, N, D), bf16),
            loss=vm((8, 128), f32),
            l_sem=dma(24),
            w_ss=dma(8, 1 + 2 * (X - 1)),
            w_rs=dma(8, 1 + 2 * (X - 1)),
            mz_ss=dma(S, Z - 1),
            mz_rs=dma(S, Z - 1),
            my_ss=dma(S, Y - 1, Z),
            my_rs=dma(S, Y - 1, Z),
            mr_ss=dma(S, 1 + 2 * (X - 1)),
            mr_rs=dma(S, 1 + 2 * (X - 1)),
            pk_ss=dma(2, S, X),
            pk_rs=dma(2, S, X),
            px_ss=dma(2, S, X - 1),
            px_rs=dma(2, S, X - 1),
            a_ss=dma(S, 1 + 2 * (X - 1)),
            a_rs=dma(S, 1 + 2 * (X - 1)),
            dy_ss=dma(S, Y - 1, Z),
            dy_rs=dma(S, Y - 1, Z),
            dz_ss=dma(S, Z - 1),
            dz_rs=dma(S, Z - 1),
        )

    def fits(self):
        X, Y, Z = self.grid
        return self.SH % (16 * Y * Z) == 0 and self.SH % 128 == 0 and self.vmem_bytes() < VMEM_ROOM

    def vmem_bytes(self):
        total = 0
        for s in [*self.shapes.values(), *[s for c in self.chunks for s in c.scratch()]]:
            dtype = getattr(s, "dtype", None)
            if dtype in (jnp.dtype(f32), jnp.dtype(bf16)):
                size = jnp.dtype(dtype).itemsize
                for n in s.shape[:-1]:
                    size *= n
                total += size * -(-s.shape[-1] // 128) * 128
        return total

    def scratch(self):
        total = Total.scratch(*self.grid)
        return [*self.shapes.values(), *total * 2, *[s for c in self.chunks for s in c.scratch()]]

    def kernel(self, count, x, tgt, area, node, snd, rcv, wi, wl, wo, mi, mal, mo, si, sal, so, *refs):
        S, C, D, E, N, R, Q, SH = self.S, self.C, self.D, self.E, self.N, self.R, self.Q, self.SH
        X, Y, Z = self.grid
        (g_in, g_out, g_skip, g_two, g_three, g_four, stats), refs = refs[:7], refs[7:]
        v = types.SimpleNamespace(**dict(zip(self.shapes, refs)))
        refs = refs[len(self.shapes) :]
        p = Place(self.n_row, self.n_col)
        area_sum, stat_sum = Total(p, refs[:7]), Total(p, refs[7:14])
        refs = refs[14:]
        for chunk in self.chunks:
            many = len(chunk.scratch())
            chunk.bind(p, refs[:many])
            refs = refs[many:]

        def weight_rows(i, col):
            which = WIRE[i]
            whole = v.wib if which == "in" else v.wob if which == "out" else v.wlb.at[which]
            return whole.at[ds(col * SH, SH), :]

        def w_copy(i, j, d=0):
            rows = weight_rows(i, 2 * p.to("x", -d) + p.k if j == 2 else p.col)
            at = (0, d, X - 1 + d)[j]
            device = p.peer("x", d) if j == 1 else p.peer("k", 1)
            return remote(rows, rows, v.w_ss.at[i, at], v.w_rs.at[i, at], device)

        hops = range(1, X)

        def w_forward(i):
            for d in hops:
                w_copy(i, 1, d).wait_recv()
                w_copy(i, 2, d).start()

        def w_get(i):
            w_copy(i, 0).wait_recv()
            for d in hops:
                w_copy(i, 2, d).wait_recv()

        W = lambda which: v.wlb[which]
        barrier = p.greet()
        own = ds(p.col * SH, SH)
        latents = [w for w in WIRE if isinstance(w, int)]
        loads = {m: pltpu.make_async_copy(wl.at[m], v.fp.at[m * SH : (m + 1) * SH, :], v.l_sem.at[m]) for m in latents}
        for load in loads.values():
            load.start()

        def turned(ref, n):
            v.tmp[0:n, 0:SH] = jnp.zeros((n, SH), f32)
            v.tmp[0 : ref.shape[0], 0:SH] = ref[...]
            return jnp.transpose(v.tmp[0:n, 0:SH])

        def w_ready(i):
            m = WIRE[i]
            if m == "in":
                v.wib[own, :] = turned(wi, N_IN).astype(bf16)
            elif m == "out":
                v.wob[own, :] = turned(wo, N_OUT).astype(bf16)
            else:
                loads[m].wait()
                v.wlb[m, own, :] = v.fp[m * SH : (m + 1) * SH, :].astype(bf16)

        def w_depart(*items):
            for i in items:
                w_copy(i, 0).start()
                for d in hops:
                    w_copy(i, 1, d).start()

        w_ready(0)
        w_ready(1)
        pl.semaphore_wait(*barrier)
        w_depart(0, 1)
        for i in range(2, 8):
            w_ready(i)
            if i < 4:
                w_depart(i)
        used = count[0]
        area_row = area[...].reshape(1, C) * (lax.broadcasted_iota(jnp.int32, (1, C), 1) < used).astype(f32)
        area_sum.value[...] = jnp.broadcast_to(jnp.sum(area_row), (8, 128))
        area_sum.start("y")

        def by_cell(ref, n, out):
            have = ref.shape[0]
            v.fx[0:have] = ref[...].astype(f32)
            v.fx[have:n] = jnp.zeros((n - have, S, C), f32)
            for s in range(S):
                out[s * C : (s + 1) * C, :] = jnp.transpose(v.fx[0:n, s, :]).astype(bf16)

        by_cell(x, N_IN, v.xb)

        node_row = node[...].reshape(1, C)
        match = (lax.broadcasted_iota(jnp.int32, (N, C), 0) == node_row).astype(f32)
        v.nm[...] = match.astype(bf16)
        match = match * (lax.broadcasted_iota(jnp.int32, (N, C), 1) < used).astype(f32)
        v.nv[...] = match.astype(bf16)
        v.cnt[...] = jnp.broadcast_to(jnp.maximum(jnp.sum(match, axis=1, keepdims=True), 1.0), (N, 128))
        node_col = jnp.transpose(jnp.broadcast_to(node_row, (128, C)))
        v.cw[...] = jnp.transpose(jnp.broadcast_to(area_row, (128, C)))
        match = (lax.broadcasted_iota(jnp.int32, (C, 128), 1) == node_col).astype(f32)
        v.cm[...] = match[:, :N].astype(bf16)
        match = match * (lax.broadcasted_iota(jnp.int32, (C, 128), 0) < used).astype(f32)
        v.cmv[...] = match[:, :N].astype(bf16)

        def table(index, base, rows):
            def down(at):
                hit = lax.broadcasted_iota(jnp.int32, (128, E), 0) + at == index
                v.oht[pl.ds(pl.multiple_of(base + at, 128), 128), :] = hit.astype(f32).astype(bf16)

            by_rows(rows, 128, down)
            column = jnp.transpose(jnp.broadcast_to(index, (128, E)))
            for at in range(0, rows, 128):
                hit = lax.broadcasted_iota(jnp.int32, (E, 128), 1) + at == column
                v.oh[:, base + at : base + at + 128] = hit.astype(f32).astype(bf16)

        v.dp[...] = jnp.zeros((S * C, N_OUT), bf16)
        v.loss[...] = jnp.zeros((8, 128), f32)

        def encode(xx, s):
            at, here, lanes = ds(s * C, C), ds(s * N, N), ds(xx * 2 * SH, 2 * SH)
            pre = mm_nt(v.xb[at, :], v.wib[lanes, :])
            v.fp[at, lanes] = pre
            v.gl[at, lanes] = silu(pre).astype(bf16)
            v.av[here, lanes] = (mm(v.nv[...], v.gl[at, lanes]) / v.cnt[:, 0:1]).astype(bf16)

        def encode_all(xx):
            def one(s, carry):
                encode(xx, s)
                return carry

            lax.fori_loop(0, S, one, 0)

        w_copy(0, 0).wait_recv()
        encode_all(p.x)
        w_forward(0)
        by_cell(tgt, N_OUT, v.tb)
        table(snd[...], 0, R)
        table(rcv[...], R, Q)
        for d in hops:
            w_copy(0, 2, d).wait_recv()
            encode_all(p.to("x", -d))
        w_forward(1)
        w_get(1)
        area_sum.finish("y")
        area_sum.start("z")
        pre = mm(v.av[...], W(0))
        v.sp[...] = pre
        v.mlb[...] = silu(pre).astype(bf16)

        def mz(s, d):
            rows = v.sr.at[s, ds(p.row * N, N), :]
            return remote(rows, rows, v.mz_ss.at[s, d - 1], v.mz_rs.at[s, d - 1], p.peer("z", d))

        def my(s, d, e):
            rows = v.sr.at[s, ds((p.to("z", -e) * Y + p.y) * N, N), :]
            return remote(rows, rows, v.my_ss.at[s, d - 1, e], v.my_rs.at[s, d - 1, e], p.peer("y", d))

        def mr(s, j, d=0):
            col = 2 * p.to("x", -d) + p.k if j == 2 else p.col
            rows = v.sr.at[s, ds(R + col * N, N), :]
            at = (0, d, X - 1 + d)[j]
            return remote(rows, rows, v.mr_ss.at[s, at], v.mr_rs.at[s, at], p.peer("x", d) if j == 1 else p.peer("k", 1))

        for s in range(S):
            v.sr[s, ds(p.row * N, N), :] = v.mlb[s * N : (s + 1) * N, :]
            v.sr[s, ds(R + p.col * N, N), :] = v.mlb[s * N : (s + 1) * N, :]

        def depart(s):
            for d in range(1, Z):
                mz(s, d).start()

        depart(0)
        for s in range(S):
            for d in range(1, Y):
                my(s, d, 0).start()
            mr(s, 0).start()
            for d in hops:
                mr(s, 1, d).start()
            if s == 1:
                w_depart(4)
        w_depart(5, 6, 7)
        w_forward(2)
        w_forward(3)
        depart(1)
        area_sum.finish("z")
        area_sum.start("k")
        w_get(2)
        w_get(3)

        def skip(at):
            v.tp[pl.ds(at, 512), :] = mm(v.gl[pl.ds(at, 512), :], W(5))

        def pk(t, s, xx):
            rows = v.part.at[s, ds((2 * xx + 1 - p.k) * N, N), :]
            return remote(rows, v.pcr.at[s, xx], v.pk_ss.at[t, s, xx], v.pk_rs.at[t, s, xx], p.peer("k", 1))

        def px(t, s, d):
            return remote(v.pxs.at[s, d - 1], v.pxr.at[s, d - 1], v.px_ss.at[t, s, d - 1], v.px_rs.at[t, s, d - 1], p.peer("x", d))

        def col_second(t, s):
            for xx in range(X):
                pk(t, s, xx).wait_recv()
            for d in hops:
                px_to = p.to("x", d)
                mine = v.part[s, ds((2 * px_to + p.k) * N, N), :]
                v.pxs[s, d - 1] = (mine + v.pcr[s, px_to]).astype(bf16)
                px(t, s, d).start()

        def col_last(t, s):
            total = v.part[s, ds(p.col * N, N), :] + v.pcr[s, p.x]
            for d in hops:
                px(t, s, d).wait_recv()
                total = total + v.pxr[s, d - 1].astype(f32)
            return total

        def nearest(j):
            steps = [(n + 1) // 2 * (1 if n % 2 else -1) for n in range(1, 2 * Z - 1)]
            taken, found = jnp.int32(0), jnp.int32(0)
            for step in steps:
                inside = ((p.z - step >= 0) & (p.z - step < Z)).astype(jnp.int32)
                found = found + jnp.where((taken == j) & (inside == 1), step, 0)
                taken = taken + inside
            return (found + Z) % Z

        def arrive(s):
            for j in range(Z - 1):
                d = nearest(j)
                mz(s, d).wait_recv()
                for b in range(1, Y):
                    my(s, b, d).start()
            for d in hops:
                mr(s, 1, d).wait_recv()
                mr(s, 2, d).start()

        def edges(s):
            for b in range(1, Y):
                for e in range(Z):
                    my(s, b, e).wait_recv()
            mr(s, 0).wait_recv()
            for d in hops:
                mr(s, 2, d).wait_recv()
            for d in range(1, Z):
                mz(s, d).wait_send()
            for b in range(1, Y):
                for e in range(Z):
                    my(s, b, e).wait_send()
            mr(s, 0).wait_send()
            for d in hops:
                mr(s, 1, d).wait_send()
                mr(s, 2, d).wait_send()
            v.sr[s, 0:R, :] = mm(v.sr[s, 0:R, :], W(1)).astype(bf16)
            v.sr[s, R : R + Q, :] = mm(v.sr[s, R : R + Q, :], W(2)).astype(bf16)

            def pick(at):
                pre = mm(v.oh[pl.ds(at, 512), :], v.sr[s])
                v.ep[s, pl.ds(at, 512), :] = pre
                v.ac[pl.ds(at, 512), :] = silu(pre).astype(bf16)

            by_rows(E, 512, pick)
            v.part[s] = mm(v.oht[R:, :], v.ac[...])
            for xx in range(X):
                pk(0, s, xx).start()

        def ac(s, j, d=0):
            col = 2 * p.to("x", -d) + p.k if j == 2 else p.col
            rows = v.da.at[s, ds(col * N, N), :]
            at = (0, d, X - 1 + d)[j]
            return remote(rows, rows, v.a_ss.at[s, at], v.a_rs.at[s, at], p.peer("x", d) if j == 1 else p.peer("k", 1))

        def decode(s):
            at, here = ds(s * C, C), ds(s * N, N)
            v.agb[here, :] = (col_last(0, s) * (1.0 / DEG)).astype(bf16)
            v.mnb[here, :] = (silu(v.sp[here, :]) + mm(v.agb[here, :], W(3))).astype(bf16)
            scale = 1.0 / (C_OUT * S * area_sum.value[0:1, 0:1])
            rows = mm(v.cm[...], v.mnb[here, :]).astype(bf16)
            pre = mm(rows, W(4)) + v.tp[at, :]
            v.tp[at, :] = pre
            v.go[at, :] = silu(pre).astype(bf16)
            error = mm(v.go[at, :], v.wob[...])[:, :C_OUT] - v.tb[at, 0:C_OUT].astype(f32)
            weighted = v.cw[:, :C_OUT] * error
            v.loss[0:1, 0:C_OUT] = v.loss[0:1, 0:C_OUT] + jnp.sum(weighted * error, axis=0, keepdims=True)
            v.dp[at, 0:C_OUT] = (2.0 * weighted * scale).astype(bf16)
            v.dt[at, :] = (silu_slope(v.tp[at, :]) * mm_nt(v.dp[at, :], v.wob[...])).astype(bf16)
            grad = mm(v.nm[...], v.dt[at, :])
            v.sg[here, :] = grad
            grad = mm_nt(jnp.concatenate(high_low(grad), axis=0), W(4))
            grad = grad[:N] + grad[N:]
            v.dmn[here, :] = grad
            v.da[s, ds(p.col * N, N), :] = mm_nt(grad.astype(bf16), W(3)).astype(bf16)
            ac(s, 0).start()
            for d in hops:
                ac(s, 1, d).start()

        def dy(s, d, e):
            return remote(v.dys.at[s, d - 1, e], v.dyr.at[s, d - 1, e], v.dy_ss.at[s, d - 1, e], v.dy_rs.at[s, d - 1, e], p.peer("y", d))

        def dz(s, d):
            return remote(v.dzs.at[s, d - 1], v.dzr.at[s, d - 1], v.dz_ss.at[s, d - 1], v.dz_rs.at[s, d - 1], p.peer("z", d))

        def pass_on(s):
            for d in hops:
                ac(s, 1, d).wait_recv()
                ac(s, 2, d).start()

        def edges_back(s):
            ac(s, 0).wait_recv()
            for d in hops:
                ac(s, 2, d).wait_recv()
            for xx in range(X):
                pk(0, s, xx).wait_send()
            for d in hops:
                px(0, s, d).wait_send()

            def pick(at):
                grad = mm(v.oh[pl.ds(at, 512), R:], v.da[s])
                v.ac[pl.ds(at, 512), :] = (silu_slope(v.ep[s, pl.ds(at, 512), :]) * grad * (1.0 / DEG)).astype(bf16)

            by_rows(E, 512, pick)
            v.tmp[...] = mm(v.oht[...], v.ac[...])
            for e in (*range(1, Z), 0):
                to = p.to("z", e)
                for d in range(1, Y):
                    v.dys[s, d - 1, e] = v.tmp[ds((to * Y + p.to("y", d)) * N, N), :].astype(bf16)
                    dy(s, d, e).start()
                v.down[s, e] = v.tmp[ds((to * Y + p.y) * N, N), :]
            v.part[s] = v.tmp[R:, :]
            for xx in range(X):
                pk(1, s, xx).start()

        def row_sum(s, e):
            total = v.down[s, e]
            for d in range(1, Y):
                dy(s, d, e).wait_recv()
                total = total + v.dyr[s, d - 1, e].astype(f32)
            return total

        def row_second(s):
            for e in range(1, Z):
                v.dzs[s, e - 1] = row_sum(s, e).astype(bf16)
                dz(s, e).start()

        def encode_back(s):
            at, here = ds(s * C, C), ds(s * N, N)
            v.drb[here, :] = col_last(1, s).astype(bf16)
            total = row_sum(s, 0)
            for d in range(1, Z):
                dz(s, d).wait_recv()
                total = total + v.dzr[s, d - 1].astype(f32)
            v.dsb[here, :] = total.astype(bf16)
            whole = v.dmn[here, :] + mm_nt(v.dsb[here, :], W(1)) + mm_nt(v.drb[here, :], W(2))
            v.d2b[here, :] = (silu_slope(v.sp[here, :]) * whole).astype(bf16)
            high, low = high_low(mm_nt(v.d2b[here, :], W(0)) / v.cnt[:, 0:1])
            grad = v.tp[at, :] + mm(v.cmv[...], high) + mm(v.cmv[...], low)
            v.dt[at, :] = (silu_slope(v.fp[at, :]) * grad).astype(bf16)

        skips, decoders, senders, receivers, encoders, inputs = self.chunks

        def decoder_gradients():
            skips.full[:, 0:D] = mm_tn(v.gl[...], v.dt[...])
            skips.full[:, D : D + N_OUT] = mm_tn(v.go[...], v.dp[...])
            skips.stage(0)
            high, low = high_low(v.sg[...])
            decoders.full[:, 0:D] = mm_tn(v.mnb[...], high) + mm_tn(v.mnb[...], low)
            decoders.full[:, D : 2 * D] = mm_tn(v.agb[...], v.dmn[...].astype(bf16))
            decoders.stage(0)

        def skip_back():
            def one(at):
                v.tp[pl.ds(at, 512), :] = mm_nt(v.dt[pl.ds(at, 512), :], W(5))

            by_rows(S * C, 512, one)

        def weights_rest():
            for i in (5, 6, 7):
                w_forward(i)
            area_sum.finish("x")
            for i in (5, 6, 7):
                w_get(i)

        def partials_back(s):
            col_second(1, s)
            row_second(s)

        stage = lambda chunk, n: functools.partial(chunk.stage, n)
        line = [
            (edges, 0),
            (edges_back, 3),
            (stage(skips, 1), S + 2, None),
            (stage(decoders, 1), S + 2, None),
            (arrive, -2),
            (functools.partial(col_second, 0), 0),
            (weights_rest, 1, None),
            (lambda s: pl.when(s < S // 2)(functools.partial(pass_on, s)), 2),
            (decode, 1),
            (lambda s: pl.when(s >= S // 2)(functools.partial(pass_on, s)), 2),
            (decoder_gradients, S + 1, None),
            (partials_back, 4),
            (skip_back, S + 2, None),
            (stage(skips, 3), S + 5, None),
            (encode_back, 6),
            (stage(skips, 2), S + 3, None),
            (stage(decoders, 2), S + 3, None),
        ]
        arrive(0)
        depart(2)
        w_forward(4)
        w_get(4)
        by_rows(S * C, 512, skip)
        arrive(1)
        depart(3)
        area_sum.finish("k")
        area_sum.start("x")

        def turn(i, carry):
            for todo, behind, *once in line:
                if once:
                    pl.when(i == behind)(todo)
                else:
                    pl.when((i >= max(behind, 0)) & (i < S + behind))(functools.partial(todo, i - behind))
            return carry

        lax.fori_loop(0, S + 6, turn, 0)
        states = [
            pltpu.make_async_copy(a.at[m], v.ep.at[j, m * SH : (m + 1) * SH, :], v.l_sem.at[6 + 6 * j + m])
            for j, a in enumerate((wl, mal, sal))
            for m in range(6)
        ]
        for load in states:
            load.start()
        decoders.lend()
        skips.lend()
        senders.full[...] = mm_tn(v.mlb[...], v.dsb[...])
        senders.stage(0)
        receivers.full[...] = mm_tn(v.mlb[...], v.drb[...])
        receivers.stage(0)
        decoders.stage(3)
        encoders.full[...] = mm_tn(v.av[...], v.d2b[...])
        encoders.stage(0)
        inputs.full[...] = mm_tn(v.dt[...], v.xb[...])
        inputs.stage(0)
        senders.stage(1)
        encoders.stage(1)
        receivers.stage(1)
        inputs.stage(1)

        for load in states:
            load.wait()
        spare = v.ep.at[3]
        for j, (a, b) in enumerate(((wi, wo), (mi, mo), (si, so))):
            spare[j * SH : (j + 1) * SH, 0:N_IN] = turned(a, N_IN)
            spare[j * SH : (j + 1) * SH, N_IN : N_IN + N_OUT] = turned(b, N_OUT)
        lane = lax.broadcasted_iota(jnp.int32, (8, 128), 1)
        row = lax.broadcasted_iota(jnp.int32, (8, 128), 0)
        stat_sum.value[...] = jnp.where(row == 2, jnp.sum(v.loss[...]), 0.0)

        def note(j, gradient, at, lanes):
            held = [buf[pl.ds(pl.multiple_of(start + p.y * (SH // Y) + p.z * (SH // Y // Z), 16), SH // Y // Z), lanes] for buf, start in at]
            _, _, update = adam_parts(held[0], gradient, held[1], held[2])
            for i, what in enumerate((held[0], update)):
                stat_sum.value[...] += jnp.where((row == i) & (lane == j), jnp.sum(what * what), 0.0)

        def note_latent(m, gradient):
            note(1 + m, gradient, [(v.ep.at[j], m * SH) for j in range(3)], slice(None))

        edge = [(spare, j * SH) for j in range(3)]
        skips.stage(4)
        note_latent(5, skips.piece[:, 0:D])
        note(7, skips.piece[:, D : D + N_OUT], edge, slice(N_IN, N_IN + N_OUT))
        decoders.stage(4)
        note_latent(4, decoders.piece[:, 0:D])
        note_latent(3, decoders.piece[:, D : 2 * D])
        senders.stage(2)
        encoders.stage(2)
        receivers.stage(2)
        inputs.stage(2)
        senders.stage(3)
        encoders.stage(3)
        inputs.stage(3)
        receivers.stage(3)
        skips.stage(5)
        senders.stage(4)
        note_latent(1, senders.piece[...])
        encoders.stage(4)
        note_latent(0, encoders.piece[...])
        inputs.stage(4)
        note(0, inputs.piece[...], edge, slice(0, N_IN))
        receivers.stage(4)
        note_latent(2, receivers.piece[...])
        stat_sum.start("k")
        decoders.stage(5)
        stat_sum.finish("k")
        stat_sum.start("x")
        skips.stage(6)
        g_skip[...] = skips.out[:, :D]
        g_out[...] = jnp.transpose(skips.out[:, D : D + N_OUT])[: g_out.shape[0], :]
        senders.stage(5)
        encoders.stage(5)
        stat_sum.finish("x")
        stat_sum.start("z")
        inputs.stage(5)
        receivers.stage(5)
        decoders.stage(6)
        g_two[...] = decoders.out[...]
        senders.stage(6)
        g_three[:, 0:D] = senders.out[...]
        encoders.stage(6)
        g_four[...] = encoders.out[...]
        stat_sum.finish("z")
        stat_sum.start("y")
        inputs.stage(6)
        g_in[...] = jnp.transpose(inputs.out[...])[: g_in.shape[0], :]
        receivers.stage(6)
        g_three[:, D : 2 * D] = receivers.out[...]
        stat_sum.finish("y")
        stats[...] = jnp.where(row < 2, stat_sum.value[...], stat_sum.value[...] / (C_OUT * S * area_sum.value[...]))

        for i in range(8):
            w_copy(i, 0).wait_send()
            for d in hops:
                w_copy(i, 1, d).wait_send()
                w_copy(i, 2, d).wait_send()
        for s in range(S):
            for d in range(1, Z):
                dz(s, d).wait_send()
            for d in range(1, Y):
                for e in range(Z):
                    dy(s, d, e).wait_send()
            ac(s, 0).wait_send()
            for d in hops:
                ac(s, 1, d).wait_send()
                ac(s, 2, d).wait_send()
            for xx in range(X):
                pk(1, s, xx).wait_send()
            for d in hops:
                px(1, s, d).wait_send()
        area_sum.drain("kxyz")
        stat_sum.drain("kxyz")
        for chunk in self.chunks:
            chunk.drain()

    def __call__(self, count, x, tgt, area, node, snd, rcv, *states):
        vm, hbm = pl.BlockSpec(memory_space=pltpu.VMEM), pl.BlockSpec(memory_space=pl.ANY)
        D, SH = self.D, self.SH
        outs = [(states[0].shape, f32), (states[2].shape, f32), ((SH, D), f32), ((SH, 2 * D), bf16), ((SH, 2 * D), bf16), ((SH, D), bf16), ((8, 128), f32)]
        return pl.pallas_call(
            self.kernel,
            out_shape=[jax.ShapeDtypeStruct(*o) for o in outs],
            in_specs=[pl.BlockSpec(memory_space=pltpu.SMEM)] + [vm] * 6 + [vm, hbm, vm] * 3,
            out_specs=[vm] * 7,
            scratch_shapes=self.scratch(),
            name="train_step",
            compiler_params=pltpu.CompilerParams(collective_id=0, has_side_effects=True, vmem_limit_bytes=67043328),
        )(count, x, tgt, area, node, snd, rcv, *states)


def update_kernel(g_in, g_out, g_skip, g_two, g_three, g_four, stats, wi, wl, wo, mi, mal, mo, si, sal, so, *refs):
    loss, *outs, norms = refs[:17]
    in_buf, out_buf, low_buf, skip_buf, two_buf, three_buf, four_buf, in_sem, out_sem, g_sem = refs[17:]
    SH, D = g_skip.shape
    loads = [[pltpu.make_async_copy(a.at[m], in_buf.at[j, m], in_sem.at[j, m]) for j, a in enumerate((wl, mal, sal))] for m in range(6)]
    order = (5, 4, 3, 2, 1, 0)
    pairs = ((g_skip, skip_buf), (g_two, two_buf), (g_three, three_buf), (g_four, four_buf))
    takes = [pltpu.make_async_copy(ref, buf, g_sem.at[i]) for i, (ref, buf) in enumerate(pairs)]
    first_use = {5: 0, 4: 1, 2: 2, 0: 3}
    for m in order:
        if m in first_use:
            takes[first_use[m]].start()
        for load in loads[m]:
            load.start()
    root = jnp.sqrt(stats[...])
    norms[...] = root[0:2, 0:8]
    loss[...] = stats[2:3, 0:1]

    def step(j, weight, gradient, mean, square):
        first, second, update = adam_parts(weight, gradient, mean, square)
        ratio = root[0:1, j : j + 1] / (root[1:2, j : j + 1] + trust_epsilon)
        master = weight - learn_rate * ratio * update
        return gradient, first, second, master, master.astype(bf16)

    for j, result in enumerate(step(0, wi[...], g_in[...], mi[...], si[...])):
        outs[3 * j][...] = result
    for j, result in enumerate(step(7, wo[...], g_out[...], mo[...], so[...])):
        outs[3 * j + 2][...] = result
    grads = {5: (skip_buf, 0), 4: (two_buf, 0), 3: (two_buf, D), 2: (three_buf, D), 1: (three_buf, 0), 0: (four_buf, 0)}
    stores = []
    for m in order:
        if m in first_use:
            takes[first_use[m]].wait()
        for load in loads[m]:
            load.wait()
        ref, at = grads[m]
        results = step(1 + m, in_buf[0, m], ref[:, at : at + D].astype(f32), in_buf[1, m], in_buf[2, m])
        for j, result in enumerate(results):
            buf = low_buf.at[m] if j == 4 else out_buf.at[j, m]
            buf[...] = result
            stores.append(pltpu.make_async_copy(buf, outs[3 * j + 1].at[m], out_sem.at[j, m]))
            stores[-1].start()
    for store in stores:
        store.wait()


def update_all(grads, states):
    vm, hbm = pl.BlockSpec(memory_space=pltpu.VMEM), pl.BlockSpec(memory_space=pl.ANY)
    kinds = [f32] * 4 + [bf16]
    shapes = [states[0].shape, states[1].shape, states[2].shape]
    n, SH, D = states[1].shape
    return pl.pallas_call(
        update_kernel,
        out_shape=[jax.ShapeDtypeStruct((1, 1), f32)]
        + [jax.ShapeDtypeStruct(s, k) for k in kinds for s in shapes]
        + [jax.ShapeDtypeStruct((2, 8), f32)],
        in_specs=[vm, vm, hbm, hbm, hbm, hbm, vm] + [vm, hbm, vm] * 3,
        out_specs=[vm] + [vm, hbm, vm] * 5 + [vm],
        scratch_shapes=[
            pltpu.VMEM((3, n, SH, D), f32),
            pltpu.VMEM((4, n, SH, D), f32),
            pltpu.VMEM((n, SH, D), bf16),
            pltpu.VMEM((SH, D), f32),
            pltpu.VMEM((SH, 2 * D), bf16),
            pltpu.VMEM((SH, 2 * D), bf16),
            pltpu.VMEM((SH, D), bf16),
            pltpu.SemaphoreType.DMA((3, n)),
            pltpu.SemaphoreType.DMA((5, n)),
            pltpu.SemaphoreType.DMA((4,)),
        ],
        name="lamb",
        compiler_params=pltpu.CompilerParams(vmem_limit_bytes=67043328),
    )(*grads, *states)


def kernel_body(mesh, step, inputs, targets, cell_area, cell_count, cell_node, edge_senders, edge_receivers, *states):
    states = [a.T if i % 3 == 2 else a for i, a in enumerate(states)]
    inputs, targets = (a.transpose(2, 0, 1) for a in (inputs, targets))
    grads = step(cell_count, inputs, targets, cell_area, cell_node, edge_senders[None, :], edge_receivers[None, :], *states)
    loss, *outs, norms = update_all(grads, states)
    outs = [a.T if i % 3 == 2 else a for i, a in enumerate(outs)]
    return (loss[0, 0], *outs, norms)


def native_gradients(
    inputs,
    targets,
    cell_area,
    cell_count,
    cell_node,
    edge_senders,
    edge_receivers,
    weight_input,
    weight_latent,
    weight_output,
):
    full_input, complete_latent, full_output = (
        lax.all_gather(weight_input.astype(jnp.bfloat16), "col", axis=1, tiled=True),
        lax.all_gather(weight_latent.astype(jnp.bfloat16), "col", axis=1, tiled=True),
        lax.all_gather(weight_output.astype(jnp.bfloat16), "col", axis=0, tiled=True),
    )
    samples = inputs.shape[0]
    slots = inputs.shape[1]
    valid = (jnp.arange(slots, dtype=jnp.int32) < cell_count[0]).astype(jnp.float32)
    cell_weight = cell_area * valid
    area_total = lax.psum(jnp.sum(cell_weight), ("row", "col"))
    first_pre = reduced_matmul("sci,id->scd", inputs, full_input)
    grid_latent = jax.nn.silu(first_pre).astype(jnp.bfloat16)
    node_match = (cell_node[None, :] == jnp.arange(MESH_DEV, dtype=jnp.int32)[:, None]).astype(
        jnp.float32
    )
    node_match_low = node_match.astype(jnp.bfloat16)
    cell_match = node_match_low.T
    node_valid = node_match * valid[None, :]
    node_sum = reduced_matmul("nc,scd->snd", node_valid.astype(jnp.bfloat16), grid_latent)
    node_lower_limit = jnp.maximum(jnp.sum(node_valid, axis=1), 1.0)
    node_average = node_sum / node_lower_limit[None, :, None]
    average_reduced = node_average.astype(jnp.bfloat16)
    second_activation_input = reduced_matmul("kaj,jz->kaz", average_reduced, complete_latent[0])
    mesh_latent = jax.nn.silu(second_activation_input)
    mesh_state_reduced = mesh_latent.astype(jnp.bfloat16)
    receiver_local_part = reduced_matmul("kaj,jz->kaz", mesh_state_reduced, complete_latent[2])
    receiver_block = lax.all_gather(receiver_local_part, "col", axis=1, tiled=True)
    sender_block = reduced_matmul(
        "kaj,jz->kaz",
        lax.all_gather(mesh_state_reduced, "row", axis=1, tiled=True),
        complete_latent[1],
    )
    receiver_rows = receiver_block.shape[1]
    sender_rows = sender_block.shape[1]
    sender_match = one_hot_table(edge_senders, sender_rows)
    receiver_match = one_hot_table(edge_receivers, receiver_rows)
    edge_pre = pick_rows(sender_match, sender_block) + pick_rows(receiver_match, receiver_block)
    partial_sums = add_into_rows(receiver_match, jax.nn.silu(edge_pre))
    message_total = lax.psum_scatter(partial_sums, "col", scatter_dimension=1, tiled=True) / DEG
    message_total_reduced = message_total.astype(jnp.bfloat16)
    residual_branch = reduced_matmul("kaj,jz->kaz", message_total_reduced, complete_latent[3])
    mesh_next = mesh_latent + residual_branch
    decode_rows = reduced_matmul("cn,snd->scd", cell_match, mesh_next.astype(jnp.bfloat16)).astype(
        jnp.bfloat16
    )
    third_pre = reduced_matmul("scd,de->sce", decode_rows, complete_latent[4]) + reduced_matmul(
        "scd,de->sce", grid_latent, complete_latent[5]
    )
    grid_out = jax.nn.silu(third_pre).astype(jnp.bfloat16)
    predict = reduced_matmul("scd,do->sco", grid_out, full_output)
    error = predict - targets.astype(jnp.float32)
    denominator = C_OUT * samples * area_total
    weighted = cell_weight[None, :, None] * error
    loss_value = lax.psum(jnp.sum(weighted * error), ("row", "col")) / denominator
    d_predict = (2.0 * weighted / denominator).astype(jnp.bfloat16)
    grad_output_local = reduced_matmul("scd,sco->do", grid_out, d_predict)
    d_grid_out = reduced_matmul("sco,do->scd", d_predict, full_output)
    d_third = silu_grad(third_pre, d_grid_out).astype(jnp.bfloat16)
    grad_decode = reduced_matmul("scd,sce->de", decode_rows, d_third)
    grad_skip = reduced_matmul("scd,sce->de", grid_latent, d_third)
    d_decode = reduced_matmul("sce,de->scd", d_third, complete_latent[4])
    d_skip = reduced_matmul("sce,de->scd", d_third, complete_latent[5])
    d_mesh_next = jnp.einsum("nc,scd->snd", node_match, d_decode, precision=highest)
    residual_branch_gradient = d_mesh_next.astype(jnp.bfloat16)
    branch_gradient_sum = reduced_matmul(
        "lhg,lhj->gj", message_total_reduced, residual_branch_gradient
    )
    message_total_gradient = reduced_matmul(
        "pyk,ck->pyc", residual_branch_gradient, complete_latent[3]
    ).astype(jnp.bfloat16)
    d_block = lax.all_gather(message_total_gradient, "col", axis=1, tiled=True)
    d_edge_message = reduced_matmul("es,ksd->ked", receiver_match, d_block)
    d_edge_pre = silu_grad(edge_pre, d_edge_message / DEG)
    d_sender_part = add_into_rows(sender_match, d_edge_pre)
    d_receiver_part = add_into_rows(receiver_match, d_edge_pre)
    sender_gradient = lax.psum_scatter(
        d_sender_part.astype(jnp.bfloat16), "row", scatter_dimension=1, tiled=True
    )
    receiver_gradient = lax.psum_scatter(
        d_receiver_part.astype(jnp.bfloat16), "col", scatter_dimension=1, tiled=True
    )
    sender_weight_gradient = reduced_matmul("lhg,lhj->gj", mesh_state_reduced, sender_gradient)
    receiver_weight_gradient = reduced_matmul("lhg,lhj->gj", mesh_state_reduced, receiver_gradient)
    d_mesh = (
        d_mesh_next
        + reduced_matmul("pyk,ck->pyc", sender_gradient, complete_latent[1])
        + reduced_matmul("pyk,ck->pyc", receiver_gradient, complete_latent[2])
    )
    hidden_second_gradient = silu_grad(second_activation_input, d_mesh).astype(jnp.bfloat16)
    encoder_gradient = reduced_matmul("lhg,lhj->gj", average_reduced, hidden_second_gradient)
    node_average_gradient = (
        reduced_matmul("pyk,ck->pyc", hidden_second_gradient, complete_latent[0])
        / node_lower_limit[None, :, None]
    )
    d_grid = d_skip + valid[None, :, None] * pick_rows(cell_match, node_average_gradient)
    d_first = silu_grad(first_pre, d_grid).astype(jnp.bfloat16)
    grad_input_local = reduced_matmul("sci,scd->id", inputs, d_first)
    grad_latent_local = jnp.stack(
        [
            encoder_gradient,
            sender_weight_gradient,
            receiver_weight_gradient,
            branch_gradient_sum,
            grad_decode,
            grad_skip,
        ]
    )
    local_terms = (grad_input_local, grad_latent_local, grad_output_local)
    whole_input, whole_latent, whole_output = lax.psum(
        (local_terms[0], local_terms[1], local_terms[2]), ("row", "col")
    )
    column = lax.axis_index("col")
    width_input = weight_input.shape[1]
    width_latent = weight_latent.shape[1]
    width_output = weight_output.shape[0]
    gradient_input = lax.dynamic_slice_in_dim(whole_input, column * width_input, width_input, 1)
    gradient_latent = lax.dynamic_slice_in_dim(whole_latent, column * width_latent, width_latent, 1)
    gradient_output = lax.dynamic_slice_in_dim(whole_output, column * width_output, width_output, 0)
    return loss_value, gradient_input, gradient_latent, gradient_output


def body(
    mesh,
    inputs,
    targets,
    cell_area,
    cell_count,
    cell_node,
    edge_senders,
    edge_receivers,
    weight_input,
    weight_latent,
    weight_output,
    mean_input,
    mean_latent,
    mean_output,
    square_input,
    square_latent,
    square_output,
):
    given = (inputs, targets, cell_area, cell_count, cell_node, edge_senders, edge_receivers, weight_input, weight_latent, weight_output)
    states = (mean_input, mean_latent, mean_output, square_input, square_latent, square_output)
    step = Step(mesh, inputs.shape[0], inputs.shape[1], weight_latent.shape[2], edge_senders.shape[0], inputs.shape[2])
    if step.fits():
        return kernel_body(mesh, step, *given, *states)
    loss_value, gradient_input, gradient_latent, gradient_output = native_gradients(*given)
    first_input, second_input, update_input = adam_parts(
        weight_input, gradient_input, mean_input, square_input
    )
    first_latent, second_latent, update_latent = adam_parts(
        weight_latent, gradient_latent, mean_latent, square_latent
    )
    first_output, second_output, update_output = adam_parts(
        weight_output, gradient_output, mean_output, square_output
    )
    weight_sums = jnp.concatenate(
        [
            jnp.sum(weight_input * weight_input)[None],
            jnp.sum(weight_latent * weight_latent, axis=(1, 2)),
            jnp.sum(weight_output * weight_output)[None],
        ]
    )
    update_sums = jnp.concatenate(
        [
            jnp.sum(update_input * update_input)[None],
            jnp.sum(update_latent * update_latent, axis=(1, 2)),
            jnp.sum(update_output * update_output)[None],
        ]
    )
    norm_sums = lax.psum(jnp.stack([weight_sums, update_sums]), "col")
    trust_norms = jnp.sqrt(norm_sums)
    ratio = trust_norms[0] / (trust_norms[1] + trust_epsilon)
    master_input = weight_input - learn_rate * ratio[0] * update_input
    master_latent = weight_latent - learn_rate * ratio[1:7][:, None, None] * update_latent
    master_output = weight_output - learn_rate * ratio[7] * update_output
    return (
        loss_value,
        gradient_input,
        gradient_latent,
        gradient_output,
        first_input,
        first_latent,
        first_output,
        second_input,
        second_latent,
        second_output,
        master_input,
        master_latent,
        master_output,
        master_input.astype(jnp.bfloat16),
        master_latent.astype(jnp.bfloat16),
        master_output.astype(jnp.bfloat16),
        trust_norms,
    )


def solution(mesh):
    placed = (
        P(None, ("row", "col"), None),
        P(None, ("row", "col"), None),
        P(("row", "col")),
        P(("row", "col")),
        P(("row", "col")),
        P(("row", "col")),
        P(("row", "col")),
        P(None, "col"),
        P(None, "col", None),
        P("col", None),
        P(None, "col"),
        P(None, "col", None),
        P("col", None),
        P(None, "col"),
        P(None, "col", None),
        P("col", None),
    )
    return jax.shard_map(
        functools.partial(body, mesh),
        mesh=mesh,
        in_specs=placed,
        out_specs=(
            P(),
            P(None, "col"),
            P(None, "col", None),
            P("col", None),
            P(None, "col"),
            P(None, "col", None),
            P("col", None),
            P(None, "col"),
            P(None, "col", None),
            P("col", None),
            P(None, "col"),
            P(None, "col", None),
            P("col", None),
            P(None, "col"),
            P(None, "col", None),
            P("col", None),
            P(),
        ),
        check_vma=False,
    )
```
